32 devices in a mesh: gx: 8 (over z, x), gy: 4 (over y, core).
Axes of the slice: x: 2, y: 2, z: 4, core: 2. Of those that a mesh axis runs over, the one named last changes fastest.
Arguments:
- density: float32 [512, 128, 128], P('gx', 'gy'), may hold values from -6 to 6
- slowness: float32 [512, 128, 128], P('gx', 'gy'), may hold values from -6 to 6
- pressure_obs: float32 [512, 128, 128], P('gx', 'gy'), may hold values from -6 to 6
- time_obs: float32 [512, 128, 128], P('gx', 'gy'), may hold values from -6 to 6
- zone_map: int32 [512, 128, 128], P('gx', 'gy'), may hold values from 0 to 7
- zone_low: float32 [8], replicated, may hold values from -2.5 to -0.5
- zone_high: float32 [8], replicated, may hold values from 0.5 to 2.5
Outputs:
- density_out: float32 [512, 128, 128], P('gx', 'gy')
- slowness_out: float32 [512, 128, 128], P('gx', 'gy')
- objective: float32 [3], replicated
The draws below stay inside these ranges and needn't reach their ends.
All inputs are finite; a program needn't handle non-finite values.
Results may differ from the reference program's by a relative error of at most 0.00013.
Values sent between devices are 32-bit elements; how exact they have to be, the bound alone decides.
No kernel may reach another device: no remote copies, remote signals or barrier semaphores. Data moves between devices by JAX's collectives and lax.ppermute only.
A program may use at most 128 MiB of HBM per device.

```python
import jax
import jax.numpy as jnp
from jax import lax

ITERS = 3
ZONES = 8
NX = 512
NY = 128
NZ = 128


def with_ends(array, own_key, low, top_value):
    shape = array.shape
    spot = [jax.random.randint(jax.random.fold_in(own_key, axis), (), 0, shape[axis]) for axis in range(len(shape))]
    array = array.at[tuple(spot)].set(low)
    longest = shape.index(max(shape))
    spot[longest] = (spot[longest] + 1) % shape[longest]
    return array.at[tuple(spot)].set(top_value)


def block_scale(stream_key, shape, split, least, top_value):
    level = 1.0
    for axis_at, parts in split:
        draws = jax.random.uniform(jax.random.fold_in(jax.random.fold_in(stream_key, 6), axis_at), (parts,), jnp.float32, least / len(split), top_value / len(split))
        level = level * jnp.repeat(jnp.exp(draws), shape[axis_at] // parts).reshape((-1,) + (1,) * (len(shape) - 1 - axis_at))
    return level


def normal_values(stream_key, dims, spread, bound, pieces=(), held_as=jnp.bfloat16):
    entries = jax.random.normal(stream_key, dims, jnp.float32) * spread
    if len(pieces) > 0:
        entries = block_scale(stream_key, dims, pieces, -0.22, 0.18) * entries
    return jnp.clip(entries, min=-bound, max=bound).astype(held_as)


def setup_inputs(seed: int = 0) -> dict:
    splits = jax.random.split(jax.random.key(seed), 8)
    return {
        "density": normal_values(splits[0], (NX, NY, NZ), 1.0, 6.0, ((0, 8), (1, 4)), jnp.float32),
        "slowness": normal_values(splits[1], (NX, NY, NZ), 1.0, 6.0, ((0, 8), (1, 4)), jnp.float32),
        "pressure_obs": normal_values(splits[2], (NX, NY, NZ), 1.0, 6.0, ((0, 8), (1, 4)), jnp.float32),
        "time_obs": normal_values(splits[3], (NX, NY, NZ), 1.0, 6.0, ((0, 8), (1, 4)), jnp.float32),
        "zone_map": with_ends(jax.random.randint(splits[4], (NX, NY, NZ), 0, ZONES), jax.random.fold_in(splits[4], 1), 0, ZONES - 1).astype(jnp.int32),
        "zone_low": jnp.clip(jax.random.uniform(splits[5], (ZONES,), jnp.float32, -2.5, -0.5), -2.5, -0.5),
        "zone_high": jnp.clip(jax.random.uniform(splits[6], (ZONES,), jnp.float32, 0.5, 2.5), 0.5, 2.5),
    }


BETA = 1.0
ETA = 0.5
EPSILON = 1e-06

def slopes(field):
    padded = jnp.pad(field, 1)
    along_x = (padded[2:, 1:-1, 1:-1] - padded[:-2, 1:-1, 1:-1]) * 0.5
    along_y = (padded[1:-1, 2:, 1:-1] - padded[1:-1, :-2, 1:-1]) * 0.5
    along_z = (padded[1:-1, 1:-1, 2:] - padded[1:-1, 1:-1, :-2]) * 0.5
    return (along_x, along_y, along_z)

def slopes_adjoint(values):
    first = jnp.pad(values[0], 1)
    second = jnp.pad(values[1], 1)
    third = jnp.pad(values[2], 1)
    total = (first[:-2, 1:-1, 1:-1] - first[2:, 1:-1, 1:-1]) * 0.5
    total = total + (second[1:-1, :-2, 1:-1] - second[1:-1, 2:, 1:-1]) * 0.5
    total = total + (third[1:-1, 1:-1, :-2] - third[1:-1, 1:-1, 2:]) * 0.5
    return total

def cross_product(first_vec, second_vec):
    return (first_vec[1] * second_vec[2] - first_vec[2] * second_vec[1], first_vec[2] * second_vec[0] - first_vec[0] * second_vec[2], first_vec[0] * second_vec[1] - first_vec[1] * second_vec[0])

def reverse_cumsum(values, axis_number):
    return jnp.flip(jnp.cumsum(jnp.flip(values, axis_number), axis_number), axis_number)

def reference(density, slowness, pressure_obs, time_obs, zone_map, zone_low, zone_high):
    lower_bound = zone_low[zone_map]
    upper_bound = zone_high[zone_map]
    cells = float(NX * NY * NZ)
    zscale = 1.0 / float(NZ) ** 0.5
    xscale = 1.0 / float(NX) ** 0.5
    density_now = density
    slowness_now = slowness
    history = []
    for iteration in range(ITERS):
        first_vec = slopes(density_now)
        second_vec = slopes(slowness_now)
        crossed = cross_product(first_vec, second_vec)
        pressure_miss = jnp.cumsum(density_now, axis=2) * zscale - pressure_obs
        time_miss = jnp.cumsum(slowness_now, axis=0) * xscale - time_obs
        crossed_sq = jnp.sum(crossed[0] * crossed[0]) + jnp.sum(crossed[1] * crossed[1]) + jnp.sum(crossed[2] * crossed[2])
        history.append(0.5 * (jnp.sum(pressure_miss * pressure_miss) + jnp.sum(time_miss * time_miss) + BETA * crossed_sq) / cells)
        toward_density = cross_product(second_vec, crossed)
        toward_slowness = cross_product(crossed, first_vec)
        grad_density = reverse_cumsum(pressure_miss, 2) * zscale + BETA * slopes_adjoint(toward_density)
        grad_slowness = reverse_cumsum(time_miss, 0) * xscale + BETA * slopes_adjoint(toward_slowness)
        norm_density = jnp.sum(grad_density * grad_density)
        norm_slowness = jnp.sum(grad_slowness * grad_slowness)
        moved = density_now - ETA * grad_density * lax.rsqrt(norm_density / cells + EPSILON)
        density_now = jnp.minimum(jnp.maximum(moved, lower_bound), upper_bound)
        slowness_now = slowness_now - ETA * grad_slowness * lax.rsqrt(norm_slowness / cells + EPSILON)
    return (density_now, slowness_now, jnp.stack(history))
```

```python
import functools
import math

import jax
import jax.numpy as jnp
from jax import lax
from jax.experimental import pallas as pl
from jax.experimental.pallas import tpu as pltpu
from jax.sharding import PartitionSpec as P

ITERS = 3
BETA = 1.0
ETA = 0.5
EPSILON = 1e-06

XO = 2
YO = 4
F32 = jnp.float32
BF16 = jnp.bfloat16


class Geo:
    def __init__(self, nx, ny, nz, px, py):
        self.nx, self.ny, self.nz, self.px, self.py = nx, ny, nz, px, py
        self.pl = ny + 2 * YO
        self.planes = nx + 2 * XO
        self.ext = (nx + 8) * self.pl
        self.xp = nx + 8
        self.cells = float(nx * px * ny * py * nz)
        self.zs = 1.0 / math.sqrt(nz)
        self.xs = 1.0 / math.sqrt(nx * px)
        self.win = (nx + 2) * self.pl + 8

    def own(self, x):
        return (x + XO) * self.pl + YO


def fold8(v):
    total = v[0:8]
    for i in range(8, v.shape[0], 8):
        total = total + v[i : i + 8]
    return total


def pick_sides(even, first, last, a, b):
    low = jnp.where(even, b, a)
    high = jnp.where(even, a, b)
    return jnp.where(first, 0.0, low), jnp.where(last, 0.0, high)


def put_pair(even, low, high, a_ref, b_ref, at):
    n = low.shape[0]
    a_ref[at : at + n, :] = jnp.where(even, high, low)
    b_ref[at : at + n, :] = jnp.where(even, low, high)


def flags_of(g, flags):
    ix, iy = flags[0], flags[1]
    return ((ix % 2) == 0, ix == 0, ix == g.px - 1), ((iy % 2) == 0, iy == 0, iy == g.py - 1)


def split2(v):
    high = v.astype(BF16)
    low = (v - high.astype(F32)).astype(BF16)
    return jnp.concatenate([high, low], axis=1)


def first_kernel(g, flags, rho, sigma, zone, t, tr, xa, xb):
    (even, _, _), _ = flags_of(g, flags)

    def body(x, carry):
        run, total, seen = carry
        run = run + sigma[x]
        return run, total + run, seen + t[x]

    zero = jnp.zeros((g.ny, g.nz), F32)
    run, total, seen = lax.fori_loop(0, g.nx, body, (zero, zero, zero), unroll=4)
    rest = total * g.xs - seen
    for s in range(g.px):
        tr[s, 0 : g.ny, :] = run
        tr[s, g.ny : 2 * g.ny, :] = rest
    at = 0
    for f, ref in enumerate((rho, sigma, zone)):
        for r in range(2):
            low = ref[r].astype(F32)
            high = ref[g.nx - 2 + r].astype(F32)
            put_pair(even, low, high, xa, xb, at)
            at += g.ny


def spread_kernel(g, zones, zlow, zhigh, rho, sigma, zone, p, rho_e, sig_e, low_e, high_e, q, table):
    nz = g.nz
    row = lax.broadcasted_iota(jnp.int32, (2 * nz, 2 * nz), 0) % nz
    col = lax.broadcasted_iota(jnp.int32, (2 * nz, 2 * nz), 1)
    first = (row <= col).astype(F32)
    second = (nz - jnp.maximum(row, col - nz)).astype(F32)
    table[...] = jnp.where(col < nz, first, second).astype(BF16)
    r2 = lax.broadcasted_iota(jnp.int32, (2 * nz, nz), 0) % nz
    c2 = lax.broadcasted_iota(jnp.int32, (2 * nz, nz), 1)
    back = (r2 >= c2).astype(F32).astype(BF16)
    step = 8

    def body(c, carry):
        for k in range(step):
            x = c * step + k
            at = pl.ds(g.own(x), g.ny)
            rho_e[at, :] = rho[x]
            sig_e[at, :] = sigma[x]
            z = zone[x]
            low = jnp.full((g.ny, nz), zlow[0], F32)
            high = jnp.full((g.ny, nz), zhigh[0], F32)
            for i in range(1, zones):
                hit = z == i
                low = jnp.where(hit, zlow[i], low)
                high = jnp.where(hit, zhigh[i], high)
            low_e[at, :] = low
            high_e[at, :] = high
        rows = p[pl.ds(c * step, step)].reshape(step * g.ny, nz)
        out = jnp.dot(split2(rows), back, preferred_element_type=F32) * g.zs
        q[pl.ds(c * step, step)] = out.reshape(step, g.ny, nz)
        return carry

    lax.fori_loop(0, g.nx // step, body, 0)


def sides_kernel(g, fields, flags, xa, xb, *refs):
    exts, (ya, yb) = refs[:fields], refs[fields:]
    (xeven, xfirst, xlast), (yeven, _, _) = flags_of(g, flags)
    n = g.xp
    for f in range(fields):
        ext = exts[f]
        for r in range(2):
            low = ext[pl.ds(YO + r, n, stride=g.pl), :]
            high = ext[pl.ds(YO + g.ny - 2 + r, n, stride=g.pl), :]
            put_pair(yeven, low, high, ya, yb, (f * 2 + r) * n)
    for f in range(fields):
        for px in range(2):
            base = (f * 2 + px) * g.ny
            for r in range(2):
                for side in range(2):
                    at = base + (r if side == 0 else g.ny - 2 + r)
                    left, right = pick_sides(xeven, xfirst, xlast, xa[at : at + 1, :], xb[at : at + 1, :])
                    for plane, value in ((px, left), (XO + g.nx + px, right)):
                        spot = (f * 2 + r) * n + plane

                        @pl.when(yeven if side == 1 else jnp.logical_not(yeven))
                        def _():
                            ya[spot : spot + 1, :] = value

                        @pl.when(jnp.logical_not(yeven) if side == 1 else yeven)
                        def _():
                            yb[spot : spot + 1, :] = value


def halos(g, flags, fields, xa, xb, ya, yb):
    (xeven, xfirst, xlast), (yeven, yfirst, ylast) = flags_of(g, flags)
    out = []
    for f in range(fields):
        for r in range(2):
            at = (f * 2 + r) * g.ny
            low, high = pick_sides(xeven, xfirst, xlast, xa[at : at + g.ny, :], xb[at : at + g.ny, :])
            out.append((f, pl.ds(r * g.pl + YO, g.ny), low))
            out.append((f, pl.ds((XO + g.nx + r) * g.pl + YO, g.ny), high))
    n = g.xp
    for f in range(fields):
        for r in range(2):
            at = (f * 2 + r) * n
            low, high = pick_sides(yeven, yfirst, ylast, ya[at : at + n, :], yb[at : at + n, :])
            out.append((f, pl.ds(YO - 2 + r, n, stride=g.pl), low))
            out.append((f, pl.ds(YO + g.ny + r, n, stride=g.pl), high))
    return out


def lane_value(row, lane):
    ids = lax.broadcasted_iota(jnp.int32, row.shape, 1)
    return jnp.sum(jnp.where(ids == lane, row, 0.0), axis=1, keepdims=True)


def alphas(g, sums):
    row = jnp.sum(sums[...], axis=0, keepdims=True)
    return tuple(ETA * lax.rsqrt(lane_value(row, k) / g.cells + EPSILON) for k in range(2))


def copy_rows(g, pairs, fn):
    def body(i, carry):
        at = pl.ds(pl.multiple_of(i * g.pl, 8), g.pl)
        fn(at)
        return carry

    lax.fori_loop(0, g.planes, body, 0, unroll=4)


def step_core(g, flags, rho_e, sig_e, trs, p, q, t, table, outs, scratch):
    grho_e, gsig_e, sums, tr, xa, xb = outs
    vxr, vxs, vyr, vys, gyr, gys, dr, rt_s, yu, ym = scratch
    nx, ny, nz = g.nx, g.ny, g.nz
    (even, _, _), _ = flags_of(g, flags)
    ix = flags[0]
    zero = jnp.zeros((ny, nz), F32)
    zero8 = jnp.zeros((8, nz), F32)
    run = zero
    before = zero
    after = zero
    for s in range(g.px):
        total = trs[s, 0:ny, :]
        after = after + jnp.where(s > ix, trs[s, ny : 2 * ny, :] + run * (nx * g.xs), 0.0)
        before = before + jnp.where(s < ix, total, 0.0)
        run = run + total

    def rays(x, carry):
        run, acc = carry
        run = run + sig_e[pl.ds(g.own(x), ny), :]
        miss = run * g.xs - t[x]
        rt_s[pl.ds(x * ny, ny), :] = miss
        return run, acc + fold8(miss * miss)

    _, acc_t = lax.fori_loop(0, nx, rays, (before, zero8), unroll=4)

    step = 8
    rows = step * g.pl

    def columns(c, acc):
        x = rho_e[pl.ds((c * step + XO) * g.pl, rows), :]
        y = jnp.dot(split2(x), table[...], preferred_element_type=F32)
        yu[...] = y[:, :nz]
        ym[...] = y[:, nz:]
        for k in range(step):
            plane = c * step + k
            at = pl.ds(k * g.pl + YO, ny)
            miss = yu[at, :] * g.zs - p[plane]
            acc = acc + fold8(miss * miss)
            dr[pl.ds(plane * ny, ny), :] = ym[at, :] * (g.zs * g.zs) - q[plane]
        return acc

    acc_p = lax.fori_loop(0, nx // step, columns, zero8)

    lanes = lax.broadcasted_iota(jnp.int32, (g.pl, nz), 1)
    below = lanes > 0
    above = lanes < nz - 1
    rowid = lax.broadcasted_iota(jnp.int32, (g.pl, nz), 0)
    mine = jnp.logical_and(rowid >= 1, rowid <= ny)

    def slopes(ref, base):
        w = g.pl
        c = ref[pl.ds(base, w), :]
        sx = ref[pl.ds(base + g.pl, w), :] - ref[pl.ds(base - g.pl, w), :]
        sy = ref[pl.ds(base + 1, w), :] - ref[pl.ds(base - 1, w), :]
        sz = jnp.where(above, pltpu.roll(c, nz - 1, 1), 0.0) - jnp.where(below, pltpu.roll(c, 1, 1), 0.0)
        return sx, sy, sz

    def adjoint_z(v):
        return jnp.where(below, pltpu.roll(v, 1, 1), 0.0) - jnp.where(above, pltpu.roll(v, nz - 1, 1), 0.0)

    def cross_plane(xi, acc, inside):
        base = (xi + XO - 1) * g.pl + YO - 1
        w = g.pl
        a0, a1, a2 = slopes(rho_e, base)
        b0, b1, b2 = slopes(sig_e, base)
        c0 = a1 * b2 - a2 * b1
        c1 = a2 * b0 - a0 * b2
        c2 = a0 * b1 - a1 * b0
        at = xi * w
        vxr[pl.ds(at, w), :] = b1 * c2 - b2 * c1
        vxs[pl.ds(at, w), :] = c1 * a2 - c2 * a1
        if not inside:
            return acc
        acc = acc + fold8(jnp.where(mine, c0 * c0 + c1 * c1 + c2 * c2, 0.0))
        vyr[pl.ds(at, w), :] = b2 * c0 - b0 * c2
        vys[pl.ds(at, w), :] = c2 * a0 - c0 * a2
        zr = adjoint_z(b0 * c1 - b1 * c0)
        zs = adjoint_z(c0 * a1 - c1 * a0)
        gyr[pl.ds(at, w), :] = zr + (vyr[pl.ds(at - 1, w), :] - vyr[pl.ds(at + 1, w), :])
        gys[pl.ds(at, w), :] = zs + (vys[pl.ds(at - 1, w), :] - vys[pl.ds(at + 1, w), :])
        return acc

    cross_plane(0, None, False)
    acc_c = lax.fori_loop(1, nx + 1, lambda xi, acc: cross_plane(xi, acc, True), zero8)
    cross_plane(nx + 1, None, False)

    def gradients(i, carry):
        back, sum_t, sum_r, nr, ns = carry
        x = nx - 1 - i
        w = g.pl
        lower = pl.ds(x * w + 1, ny)
        here = pl.ds((x + 1) * w + 1, ny)
        upper = pl.ds((x + 2) * w + 1, ny)
        cr = (vxr[lower, :] - vxr[upper, :] + gyr[here, :]) * (BETA / 16.0)
        cs = (vxs[lower, :] - vxs[upper, :] + gys[here, :]) * (BETA / 16.0)
        back = back + rt_s[pl.ds(x * ny, ny), :]
        gr = dr[pl.ds(x * ny, ny), :] + cr
        gs = back * g.xs + cs
        at = pl.ds(g.own(x), ny)
        grho_e[at, :] = gr
        gsig_e[at, :] = gs
        weight = (i + 1).astype(F32)
        return back, sum_t + gs, sum_r + gs * weight, nr + fold8(gr * gr), ns + fold8(gs * gs)

    _, sum_t, sum_r, nr, ns = lax.fori_loop(0, nx, gradients, (after, zero, zero, zero8, zero8), unroll=2)

    total = lambda v: jnp.sum(jnp.sum(v, axis=0, keepdims=True), axis=1, keepdims=True)
    lane = lax.broadcasted_iota(jnp.int32, sums.shape, 1)
    obj = acc_t + acc_p + acc_c * (BETA / 16.0)
    sums[...] = jnp.where(lane == 0, total(nr), jnp.where(lane == 1, total(ns), jnp.where(lane == 2, total(obj), 0.0)))
    if tr is not None:
        rest = sum_r * g.xs
        for s in range(g.px):
            tr[s, 0:ny, :] = sum_t
            tr[s, ny : 2 * ny, :] = rest
        pos = 0
        for ext in (grho_e, gsig_e):
            for r in range(2):
                put_pair(even, ext[pl.ds(g.own(r), ny), :], ext[pl.ds(g.own(nx - 2 + r), ny), :], xa, xb, pos)
                pos += ny


def opening_step(g, zones, flags, zlow, zhigh, xa, xb, ya, yb, rho_i, sig_i, low_i, high_i, trs, p, q, t, table,
                 rho_e, sig_e, low_e, high_e, *rest):
    def move(at):
        rho_e[at, :] = rho_i[at, :]
        sig_e[at, :] = sig_i[at, :]
        low_e[at, :] = low_i[at, :]
        high_e[at, :] = high_i[at, :]

    copy_rows(g, None, move)
    for f, at, value in halos(g, flags, 3, xa, xb, ya, yb):
        if f == 0:
            rho_e[at, :] = value
        elif f == 1:
            sig_e[at, :] = value
        else:
            low = jnp.full(value.shape, zlow[0], F32)
            high = jnp.full(value.shape, zhigh[0], F32)
            for i in range(1, zones):
                hit = value == float(i)
                low = jnp.where(hit, zlow[i], low)
                high = jnp.where(hit, zhigh[i], high)
            low_e[at, :] = low
            high_e[at, :] = high
    step_core(g, flags, rho_e, sig_e, trs, p, q, t, table, rest[:6], rest[6:])


def later_step(g, last, flags, xa, xb, ya, yb, sums_i, grho_i, gsig_i, tr_i, rho_i, sig_i, low_e, high_e, trs_i,
               p, q, t, table, rho_e, sig_e, trs, *rest):
    ar, asig = alphas(g, sums_i)

    def move(at):
        rho_e[at, :] = jnp.minimum(jnp.maximum(rho_i[at, :] - ar * grho_i[at, :], low_e[at, :]), high_e[at, :])
        sig_e[at, :] = sig_i[at, :] - asig * gsig_i[at, :]

    copy_rows(g, None, move)
    for f, at, value in halos(g, flags, 2, xa, xb, ya, yb):
        if f == 0:
            rho_e[at, :] = jnp.minimum(jnp.maximum(rho_i[at, :] - ar * value, low_e[at, :]), high_e[at, :])
        else:
            sig_e[at, :] = sig_i[at, :] - asig * value
    for s in range(g.px):
        trs[s] = trs_i[s] - asig * tr_i[s]
    if last:
        outs, scratch = (rest[0], rest[1], rest[2], None, None, None), rest[3:]
    else:
        outs, scratch = rest[:6], rest[6:]
    step_core(g, flags, rho_e, sig_e, trs, p, q, t, table, outs, scratch)


def closing_kernel(g, sums0, sums1, sums2, grho_e, gsig_e, rho_e, sig_e, low_e, high_e, rho_o, sig_o, obj):
    ar, asig = alphas(g, sums2)

    def body(x, carry):
        at = pl.ds(g.own(x), g.ny)
        rho_o[x] = jnp.minimum(jnp.maximum(rho_e[at, :] - ar * grho_e[at, :], low_e[at, :]), high_e[at, :])
        sig_o[x] = sig_e[at, :] - asig * gsig_e[at, :]
        return carry

    lax.fori_loop(0, g.nx, body, 0, unroll=4)
    lane = lax.broadcasted_iota(jnp.int32, obj.shape, 1)
    total = jnp.zeros(obj.shape, F32)
    for k, sums in enumerate((sums0, sums1, sums2)):
        row = jnp.sum(sums[...], axis=0, keepdims=True)
        total = jnp.where(lane == k, lane_value(row, 2) * (0.5 / g.cells), total)
    obj[...] = total


def pairs_of(size):
    a = [(i, i ^ 1) for i in range(size)]
    b = [(i, i if i in (0, size - 1) else ((i + 1) ^ 1) - 1) for i in range(size)]
    return a, b


def exchange(axis, a, b):
    pa, pb = pairs_of(lax.axis_size(axis))
    return lax.ppermute(a, axis, pa), lax.ppermute(b, axis, pb)


SMEM = pl.BlockSpec(memory_space=pltpu.SMEM)
VMEM = pl.BlockSpec(memory_space=pltpu.VMEM)


def call(body, name, shapes, specs, args, scratch=(), limit=24):
    return pl.pallas_call(
        body,
        name=name,
        out_shape=[jax.ShapeDtypeStruct(s, d) for s, d in shapes],
        in_specs=specs,
        out_specs=[VMEM] * len(shapes),
        scratch_shapes=list(scratch),
        compiler_params=pltpu.CompilerParams(vmem_limit_bytes=limit * 1024 * 1024),
    )(*args)


def local(density, slowness, pressure_obs, time_obs, zone_map, zone_low, zone_high):
    nx, ny, nz = density.shape
    px, py = lax.axis_size("gx"), lax.axis_size("gy")
    g = Geo(nx, ny, nz, px, py)
    zones = zone_low.shape[0]
    both = ("gx", "gy")
    flags = jnp.stack([lax.axis_index("gx"), lax.axis_index("gy")]).astype(jnp.int32)

    ext = ((g.ext, nz), F32)
    tr_shape = ((px, 2 * ny, nz), F32)
    sums_shape = ((px * py, nz), F32)
    block = ((nx, ny, nz), F32)
    xmsg = lambda f: ((f * 2 * ny, nz), F32)
    ymsg = lambda f: ((f * 2 * g.xp, nz), F32)
    win = pltpu.VMEM((g.win, nz), F32)
    core_scratch = [win] * 6 + [pltpu.VMEM((nx * ny, nz), F32)] * 2 + [pltpu.VMEM((8 * g.pl, nz), F32)] * 2

    tr, xa, xb = call(
        functools.partial(first_kernel, g), "first", [tr_shape, xmsg(3), xmsg(3)],
        [SMEM] + [VMEM] * 4, (flags, density, slowness, zone_map, time_obs),
    )
    trs = lax.all_to_all(tr, "gx", 0, 0)
    xa, xb = exchange("gx", xa, xb)
    rho_e, sig_e, low_e, high_e, q, table = call(
        functools.partial(spread_kernel, g, zones), "spread", [ext] * 4 + [block, ((2 * nz, 2 * nz), BF16)],
        [SMEM, SMEM] + [VMEM] * 4, (zone_low, zone_high, density, slowness, zone_map, pressure_obs),
    )
    zone_e = jnp.pad(zone_map.astype(F32), ((XO, g.xp - nx - XO), (YO, YO), (0, 0))).reshape(g.ext, nz)
    ya, yb = call(
        functools.partial(sides_kernel, g, 3), "sides", [ymsg(3)] * 2,
        [SMEM] + [VMEM] * 5, (flags, xa, xb, rho_e, sig_e, zone_e),
    )
    ya, yb = exchange("gy", ya, yb)
    outs = call(
        functools.partial(opening_step, g, zones), "opening", [ext] * 4 + [ext, ext, sums_shape, tr_shape, xmsg(2), xmsg(2)],
        [SMEM] * 3 + [VMEM] * 13,
        (flags, zone_low, zone_high, xa, xb, ya, yb, rho_e, sig_e, low_e, high_e, trs, pressure_obs, q, time_obs, table),
        core_scratch,
    )
    rho_e, sig_e, low_e, high_e, grho_e, gsig_e, sums, tr, xa, xb = outs
    history = []
    for iteration in range(1, ITERS):
        last = iteration == ITERS - 1
        sums = lax.all_to_all(sums, both, 0, 0, tiled=True)
        history.append(sums)
        tr = lax.all_to_all(tr, "gx", 0, 0)
        xa, xb = exchange("gx", xa, xb)
        ya, yb = call(
            functools.partial(sides_kernel, g, 2), "sides", [ymsg(2)] * 2,
            [SMEM] + [VMEM] * 4, (flags, xa, xb, grho_e, gsig_e),
        )
        ya, yb = exchange("gy", ya, yb)
        shapes = [ext, ext, tr_shape, ext, ext, sums_shape] + ([] if last else [tr_shape, xmsg(2), xmsg(2)])
        outs = call(
            functools.partial(later_step, g, last), "step", shapes, [SMEM] + [VMEM] * 17,
            (flags, xa, xb, ya, yb, sums, grho_e, gsig_e, tr, rho_e, sig_e, low_e, high_e, trs, pressure_obs, q, time_obs, table),
            core_scratch,
        )
        if last:
            rho_e, sig_e, trs, grho_e, gsig_e, sums = outs
        else:
            rho_e, sig_e, trs, grho_e, gsig_e, sums, tr, xa, xb = outs
    sums = lax.all_to_all(sums, both, 0, 0, tiled=True)
    history.append(sums)
    rho, sigma, obj = call(
        functools.partial(closing_kernel, g), "closing", [block, block, ((8, nz), F32)],
        [VMEM] * 9, (*history, grho_e, gsig_e, rho_e, sig_e, low_e, high_e),
    )
    return rho, sigma, obj[0, :ITERS]


def solution(mesh):
    placed = (P("gx", "gy", None),) * 5 + (P(), P())
    return jax.shard_map(
        local,
        mesh=mesh,
        in_specs=placed,
        out_specs=(P("gx", "gy", None), P("gx", "gy", None), P()),
        check_vma=False,
    )
```

```python
import functools
import math

import jax
import jax.numpy as jnp
from jax import lax
from jax.experimental import pallas as pl
from jax.experimental.pallas import tpu as pltpu
from jax.sharding import PartitionSpec as P

ITERS = 3
BETA = 1.0
ETA = 0.5
EPSILON = 1e-06

XO = 2
YO = 4
F32 = jnp.float32
BF16 = jnp.bfloat16


class Geo:
    def __init__(self, nx, ny, nz, px, py):
        self.nx, self.ny, self.nz, self.px, self.py = nx, ny, nz, px, py
        self.pl = ny + 2 * YO
        self.planes = nx + 2 * XO
        self.ext = (nx + 8) * self.pl
        self.xp = nx + 8
        self.cells = float(nx * px * ny * py * nz)
        self.zs = 1.0 / math.sqrt(nz)
        self.xs = 1.0 / math.sqrt(nx * px)
        self.win = (nx + 2) * self.pl + 8
        self.pairs = px // 2

    def own(self, x):
        return (x + XO) * self.pl + YO


def fold8(v):
    total = v[0:8]
    for i in range(8, v.shape[0], 8):
        total = total + v[i : i + 8]
    return total


def pick_sides(even, first, last, a, b):
    low = jnp.where(even, b, a)
    high = jnp.where(even, a, b)
    return jnp.where(first, 0.0, low), jnp.where(last, 0.0, high)


def put_pair(even, low, high, a_ref, b_ref, at):
    n = low.shape[0]
    a_ref[at : at + n, :] = jnp.where(even, high, low)
    b_ref[at : at + n, :] = jnp.where(even, low, high)


def flags_of(g, flags):
    ix, iy = flags[0], flags[1]
    return ((ix % 2) == 0, ix == 0, ix == g.px - 1), ((iy % 2) == 0, iy == 0, iy == g.py - 1)


def split2(v):
    high = v.astype(BF16)
    low = (v - high.astype(F32)).astype(BF16)
    return jnp.concatenate([high, low], axis=1)


def bounds_of(zones, z, zlow, zhigh):
    low = jnp.full(z.shape, zlow[0], F32)
    high = jnp.full(z.shape, zhigh[0], F32)
    for i in range(1, zones):
        hit = z == i
        low = jnp.where(hit, zlow[i], low)
        high = jnp.where(hit, zhigh[i], high)
    return low, high


def first_kernel(g, flags, rho, sigma, zone, t, own, xa, xb, rims, zrims, sig_v, t_v, sems):
    (even, _, _), _ = flags_of(g, flags)
    step = 8
    small = []
    for k, at in enumerate((0, g.nx - 2)):
        small.append(pltpu.make_async_copy(rho.at[pl.ds(at, 2)], rims.at[k, 0], sems.at[2 * k]))
        small.append(pltpu.make_async_copy(zone.at[pl.ds(at, 2)], zrims.at[k], sems.at[2 * k + 1]))
    big = []
    for c in range(g.nx // step):
        at = pl.ds(c * step, step)
        big.append((
            pltpu.make_async_copy(sigma.at[at], sig_v.at[at], sems.at[4 + 2 * c]),
            pltpu.make_async_copy(t.at[at], t_v.at[at], sems.at[5 + 2 * c]),
        ))
    for a, b in big:
        a.start()
        b.start()
    for copy in small:
        copy.start()
    zero = jnp.zeros((g.ny, g.nz), F32)
    run, total, seen = zero, zero, zero
    for c, (a, b) in enumerate(big):
        a.wait()
        b.wait()
        for k in range(step):
            run = run + sig_v[c * step + k]
            total = total + run
            seen = seen + t_v[c * step + k]
    own[0 : g.ny, :] = run
    own[g.ny : 2 * g.ny, :] = total * g.xs - seen
    for copy in small:
        copy.wait()
    at = 0
    for r in range(2):
        put_pair(even, rims[0, 0, r], rims[1, 0, r], xa, xb, at)
        at += g.ny
    for r in range(2):
        put_pair(even, sig_v[r], sig_v[g.nx - 2 + r], xa, xb, at)
        at += g.ny
    for r in range(2):
        put_pair(even, zrims[0, r].astype(F32), zrims[1, r].astype(F32), xa, xb, at)
        at += g.ny
    xa[at : at + g.ny, :] = run
    xa[at + g.ny : at + 2 * g.ny, :] = total * g.xs - seen


def spread_kernel(g, zones, zlow, zhigh, zone, p, low_o, high_o, q, table, ztable):
    nz = g.nz
    row = lax.broadcasted_iota(jnp.int32, (2 * nz, 2 * nz), 0) % nz
    col = lax.broadcasted_iota(jnp.int32, (2 * nz, 2 * nz), 1)
    first = (row <= col).astype(F32)
    second = (nz - jnp.maximum(row, col - nz)).astype(F32)
    table[...] = jnp.where(col < nz, first, second).astype(BF16)
    r2 = lax.broadcasted_iota(jnp.int32, (2 * nz, nz), 0) % nz
    c2 = lax.broadcasted_iota(jnp.int32, (2 * nz, nz), 1)
    back = (r2 >= c2).astype(F32).astype(BF16)
    ztable[...] = ((r2 == c2 + 1).astype(F32) - (r2 == c2 - 1).astype(F32)).astype(BF16)
    step = 8

    def body(c, carry):
        for k in range(step):
            x = c * step + k
            low_o[x], high_o[x] = bounds_of(zones, zone[x], zlow, zhigh)
        rows = p[pl.ds(c * step, step)].reshape(step * g.ny, nz)
        out = jnp.dot(split2(rows), back, preferred_element_type=F32) * g.zs
        q[pl.ds(c * step, step)] = out.reshape(step, g.ny, nz)
        return carry

    lax.fori_loop(0, g.nx // step, body, 0)


def sides_kernel(g, fields, flags, xa, xb, own, order, *refs):
    blocks, (ya, yb, pair) = refs[:fields], refs[fields:]
    (xeven, xfirst, xlast), (yeven, _, _) = flags_of(g, flags)
    n = g.xp
    for f in range(fields):
        for r in range(2):
            low = blocks[f][pl.ds(r, g.nx, stride=g.ny), :].astype(F32)
            high = blocks[f][pl.ds(g.ny - 2 + r, g.nx, stride=g.ny), :].astype(F32)
            put_pair(yeven, low, high, ya, yb, (f * 2 + r) * n + XO)
    for f in range(fields):
        for px in range(2):
            at = (f * 2 + px) * g.ny
            sides = pick_sides(xeven, xfirst, xlast, xa[at : at + g.ny, :], xb[at : at + g.ny, :])
            for plane, value in zip((px, XO + g.nx + px), sides):
                for r in range(2):
                    spot = (f * 2 + r) * n + plane
                    put_pair(yeven, value[r : r + 1], value[g.ny - 2 + r : g.ny - 1 + r], ya, yb, spot)
    at = fields * 2 * g.ny
    mine_t, mine_s = own[0 : g.ny, :], own[g.ny : 2 * g.ny, :]
    other_t, other_s = xa[at : at + g.ny, :], xa[at + g.ny : at + 2 * g.ny, :]
    pair[0 : g.ny, :] = mine_t + other_t
    pair[g.ny : 2 * g.ny, :] = mine_s + other_s + jnp.where(xeven, mine_t, other_t) * (g.nx * g.xs)


def halo_slots(g):
    xs = []
    for r in range(2):
        xs.append((r * g.ny, pl.ds(r * g.pl + YO, g.ny), pl.ds((XO + g.nx + r) * g.pl + YO, g.ny)))
    ys = []
    for r in range(2):
        ys.append((r * g.xp, pl.ds(YO - 2 + r, g.xp, stride=g.pl), pl.ds(YO + g.ny + r, g.xp, stride=g.pl)))
    return xs, ys


def halo_values(g, flags, field, xa, xb, ya, yb):
    (xeven, xfirst, xlast), (yeven, yfirst, ylast) = flags_of(g, flags)
    xs, ys = halo_slots(g)
    for axis, slots, n, a, b, even, first, last in (
        (0, xs, g.ny, xa, xb, xeven, xfirst, xlast),
        (1, ys, g.xp, ya, yb, yeven, yfirst, ylast),
    ):
        for at, low_rows, high_rows in slots:
            here = pl.ds(field * 2 * n + at, n)
            low, high = pick_sides(even, first, last, a[here, :], b[here, :])
            yield axis, 0, at, low_rows, low
            yield axis, 1, at, high_rows, high


def lane_value(row, lane):
    ids = lax.broadcasted_iota(jnp.int32, row.shape, 1)
    return jnp.sum(jnp.where(ids == lane, row, 0.0), axis=1, keepdims=True)


def alphas(g, sums):
    row = jnp.sum(sums[...], axis=0, keepdims=True)
    return tuple(ETA * lax.rsqrt(lane_value(row, k) / g.cells + EPSILON) for k in range(2))


def ray_offsets(g, flags, trs):
    ix = flags[0]
    q = ix // 2
    even = (ix % 2) == 0
    ny = g.ny
    mine, other = trs[0, 0:ny, :], trs[1, 0:ny, :]
    reach = float(g.nx * g.xs)
    before = jnp.where(even, 0.0, other)
    sums = jnp.zeros_like(mine)
    spread = (mine + other) * (g.pairs - 1 - q).astype(F32)
    for m in range(1, g.pairs):
        p = q ^ m
        total = trs[1 + m, 0:ny, :]
        before = before + jnp.where(p < q, total, 0.0)
        sums = sums + jnp.where(p > q, trs[1 + m, ny : 2 * ny, :], 0.0)
        spread = spread + total * (g.pairs - 1 - jnp.maximum(p, q)).astype(F32)
    near = jnp.where(even, trs[1, ny : 2 * ny, :] + (before + mine) * reach, 0.0)
    return before, near + sums + spread * (2.0 * reach)


def step_core(g, flags, update, rho_e, sig_e, trs, p, q, t, table, ztable, outs, scratch):
    grho, gsig, sums, own, xa, xb = outs
    vxr, vxs, vyr, vys, vzr, vzs, gyr, gys, rt_s, az, bz, yu, ym = scratch
    nx, ny, nz, w = g.nx, g.ny, g.nz, g.pl
    (even, _, _), _ = flags_of(g, flags)
    zero = jnp.zeros((ny, nz), F32)
    zero8 = jnp.zeros((8, nz), F32)
    before, after = ray_offsets(g, flags, trs)
    step = 8
    rows = step * w

    def zdiff(v):
        return jnp.dot(split2(v), ztable[...], preferred_element_type=F32)

    edge = [ref[pl.ds(k * w, w), :] for ref in (rho_e, sig_e) for k in (1, XO + nx)]
    out = zdiff(jnp.concatenate(edge, axis=0))
    for i, (ref, k) in enumerate(((az, 1), (az, XO + nx), (bz, 1), (bz, XO + nx))):
        ref[pl.ds(k * w, w), :] = out[i * w : (i + 1) * w]

    def fields(c, carry):
        run, acc = carry
        for k in range(step):
            x = c * step + k
            at = pl.ds(g.own(x), ny)
            rho, sig = update(x, at)
            rho_e[at, :] = rho
            sig_e[at, :] = sig
            run = run + sig
            miss = run * g.xs - t[x]
            rt_s[pl.ds(x * ny, ny), :] = miss
            acc = acc + fold8(miss * miss)
        at = pl.ds((c * step + XO) * w, rows)
        pieces = split2(rho_e[at, :])
        az[at, :] = jnp.dot(pieces, ztable[...], preferred_element_type=F32)
        y = jnp.dot(pieces, table[...], preferred_element_type=F32)
        yu[at, :] = y[:, :nz]
        ym[at, :] = y[:, nz:]
        bz[at, :] = zdiff(sig_e[at, :])
        return run, acc

    _, acc_t = lax.fori_loop(0, nx // step, fields, (before, zero8))

    rowid = lax.broadcasted_iota(jnp.int32, (w, nz), 0)
    mine = jnp.logical_and(rowid >= 1, rowid <= ny)

    def slopes(ref, z, base):
        sx = ref[pl.ds(base + w, w), :] - ref[pl.ds(base - w, w), :]
        sy = ref[pl.ds(base + 1, w), :] - ref[pl.ds(base - 1, w), :]
        return sx, sy, z[pl.ds(base, w), :]

    def cross_plane(xi, acc, inside):
        base = (xi + XO - 1) * w + YO - 1
        a0, a1, a2 = slopes(rho_e, az, base)
        b0, b1, b2 = slopes(sig_e, bz, base)
        c0 = a1 * b2 - a2 * b1
        c1 = a2 * b0 - a0 * b2
        c2 = a0 * b1 - a1 * b0
        at = pl.ds(pl.multiple_of(xi * w, 8), w)
        vxr[at, :] = b1 * c2 - b2 * c1
        vxs[at, :] = c1 * a2 - c2 * a1
        if not inside:
            return acc
        vyr[at, :] = b2 * c0 - b0 * c2
        vys[at, :] = c2 * a0 - c0 * a2
        vzr[at, :] = b0 * c1 - b1 * c0
        vzs[at, :] = c0 * a1 - c1 * a0
        return acc + fold8(jnp.where(mine, c0 * c0 + c1 * c1 + c2 * c2, 0.0))

    cross_plane(0, None, False)
    cross_plane(nx + 1, None, False)
    acc_c = lax.fori_loop(1, nx + 1, lambda xi, acc: cross_plane(xi, acc, True), zero8, unroll=2)

    def adjoints(c, carry):
        start = (1 + c * step) * w
        at = pl.ds(pl.multiple_of(start, 8), rows)
        for vy, vz, out in ((vyr, vzr, gyr), (vys, vzs, gys)):
            along_y = vy[pl.ds(start - 1, rows), :] - vy[pl.ds(start + 1, rows), :]
            out[at, :] = along_y - zdiff(vz[at, :])
        return carry

    lax.fori_loop(0, nx // step, adjoints, 0)

    def gradients(i, carry):
        back, sum_t, sum_r, nr, ns, acc = carry
        x = nx - 1 - i
        lower = pl.ds(x * w + 1, ny)
        here = pl.ds((x + 1) * w + 1, ny)
        upper = pl.ds((x + 2) * w + 1, ny)
        at = pl.ds(g.own(x), ny)
        cr = (vxr[lower, :] - vxr[upper, :] + gyr[here, :]) * (BETA / 16.0)
        cs = (vxs[lower, :] - vxs[upper, :] + gys[here, :]) * (BETA / 16.0)
        back = back + rt_s[pl.ds(x * ny, ny), :]
        miss = yu[at, :] * g.zs - p[x]
        gr = ym[at, :] * (g.zs * g.zs) - q[x] + cr
        gs = back * g.xs + cs
        out = pl.ds(pl.multiple_of(x * ny, 8), ny)
        grho[out, :] = gr
        gsig[out, :] = gs
        weight = (i + 1).astype(F32)
        return (back, sum_t + gs, sum_r + gs * weight, nr + fold8(gr * gr), ns + fold8(gs * gs),
                acc + fold8(miss * miss))

    start = (after, zero, zero, zero8, zero8, zero8)
    _, sum_t, sum_r, nr, ns, acc_p = lax.fori_loop(0, nx, gradients, start, unroll=4)

    total = lambda v: jnp.sum(jnp.sum(v, axis=0, keepdims=True), axis=1, keepdims=True)
    lane = lax.broadcasted_iota(jnp.int32, sums.shape, 1)
    obj = acc_t + acc_p + acc_c * (BETA / 16.0)
    sums[...] = jnp.where(lane == 0, total(nr), jnp.where(lane == 1, total(ns), jnp.where(lane == 2, total(obj), 0.0)))
    if own is not None:
        rest = sum_r * g.xs
        pos = 0
        for block in (grho, gsig):
            for r in range(2):
                put_pair(even, block[pl.ds(r * ny, ny), :], block[pl.ds((nx - 2 + r) * ny, ny), :], xa, xb, pos)
                pos += ny
        for ref, at in ((own, 0), (xa, pos)):
            ref[at : at + ny, :] = sum_t
            ref[at + ny : at + 2 * ny, :] = rest


def opening_step(g, zones, flags, zlow, zhigh, xa, xb, ya, yb, own, rho, sig, p, q, t, table, ztable, *refs):
    others, rest = refs[: g.pairs - 1], refs[g.pairs - 1 :]
    rho_e, sig_e, trs, xlow, xhigh, ylow, yhigh = rest[:7]
    ny = g.ny
    for f, ext in ((0, rho_e), (1, sig_e)):
        for axis, side, at, spot, value in halo_values(g, flags, f, xa, xb, ya, yb):
            ext[spot, :] = value
    for axis, side, at, spot, value in halo_values(g, flags, 2, xa, xb, ya, yb):
        low, high = bounds_of(zones, value, zlow, zhigh)
        lows, highs = ((xlow, xhigh), (ylow, yhigh))[axis]
        lows[side, pl.ds(at, value.shape[0]), :] = low
        highs[side, pl.ds(at, value.shape[0]), :] = high
    pos = 6 * ny
    trs[0] = own[...]
    trs[1] = xa[pos : pos + 2 * ny, :]
    for m, other in enumerate(others):
        trs[2 + m] = other[...]
    step_core(g, flags, lambda x, at: (rho[x], sig[x]), rho_e, sig_e, trs, p, q, t, table, ztable, rest[7:13], rest[13:])


def later_step(g, last, flags, xa, xb, ya, yb, sums_i, own_i, grho_i, gsig_i, rho_i, sig_i, low, high,
               xlow, xhigh, ylow, yhigh, trs_i, p, q, t, table, ztable, *refs):
    others, rest = refs[: g.pairs - 1], refs[g.pairs - 1 :]
    rho_e, sig_e, trs = rest[:3]
    ny = g.ny
    ar, asig = alphas(g, sums_i)
    for axis, side, at, spot, value in halo_values(g, flags, 0, xa, xb, ya, yb):
        lows, highs = ((xlow, xhigh), (ylow, yhigh))[axis]
        here = pl.ds(at, value.shape[0])
        moved = rho_i[spot, :] - ar * value
        rho_e[spot, :] = jnp.minimum(jnp.maximum(moved, lows[side, here, :]), highs[side, here, :])
    for axis, side, at, spot, value in halo_values(g, flags, 1, xa, xb, ya, yb):
        sig_e[spot, :] = sig_i[spot, :] - asig * value
    pos = 4 * ny
    trs[0] = trs_i[0] - asig * own_i[...]
    trs[1] = trs_i[1] - asig * xa[pos : pos + 2 * ny, :]
    for m, other in enumerate(others):
        trs[2 + m] = trs_i[2 + m] - asig * other[...]

    def update(x, at):
        here = pl.ds(pl.multiple_of(x * ny, 8), ny)
        moved = rho_i[at, :] - ar * grho_i[here, :]
        return jnp.minimum(jnp.maximum(moved, low[x]), high[x]), sig_i[at, :] - asig * gsig_i[here, :]

    if last:
        outs, scratch = (*rest[3:6], None, None, None), rest[6:]
    else:
        outs, scratch = rest[3:9], rest[9:]
    step_core(g, flags, update, rho_e, sig_e, trs, p, q, t, table, ztable, outs, scratch)


def closing_kernel(g, sums0, sums1, sums2, grho, gsig, rho_e, sig_e, low, high, rho_o, sig_o, obj):
    ar, asig = alphas(g, sums2)

    def body(x, carry):
        at = pl.ds(g.own(x), g.ny)
        here = pl.ds(pl.multiple_of(x * g.ny, 8), g.ny)
        rho_o[x] = jnp.minimum(jnp.maximum(rho_e[at, :] - ar * grho[here, :], low[x]), high[x])
        sig_o[x] = sig_e[at, :] - asig * gsig[here, :]
        return carry

    lax.fori_loop(0, g.nx, body, 0, unroll=4)
    lane = lax.broadcasted_iota(jnp.int32, obj.shape, 1)
    total = jnp.zeros(obj.shape, F32)
    for k, sums in enumerate((sums0, sums1, sums2)):
        row = jnp.sum(sums[...], axis=0, keepdims=True)
        total = jnp.where(lane == k, lane_value(row, 2) * (0.5 / g.cells), total)
    obj[...] = total


def pairs_of(size):
    a = [(i, i ^ 1) for i in range(size)]
    b = [(i, i if i in (0, size - 1) else ((i + 1) ^ 1) - 1) for i in range(size)]
    return a, b


def exchange(axis, a, b):
    pa, pb = pairs_of(lax.axis_size(axis))
    return lax.ppermute(a, axis, pa), lax.ppermute(b, axis, pb)


def pair_totals(pair, size):
    return [lax.ppermute(pair, "gx", [(i, i ^ (2 * m)) for i in range(size)]) for m in range(1, size // 2)]


SMEM = pl.BlockSpec(memory_space=pltpu.SMEM)
VMEM = pl.BlockSpec(memory_space=pltpu.VMEM)
HBM = pl.BlockSpec(memory_space=pltpu.HBM)


def call(body, name, shapes, specs, args, scratch=(), limit=12):
    return pl.pallas_call(
        body,
        name=name,
        out_shape=[jax.ShapeDtypeStruct(s, d) for s, d in shapes],
        in_specs=specs,
        out_specs=[VMEM] * len(shapes),
        scratch_shapes=list(scratch),
        compiler_params=pltpu.CompilerParams(vmem_limit_bytes=limit * 1024 * 1024),
    )(*args)


def local(density, slowness, pressure_obs, time_obs, zone_map, zone_low, zone_high):
    nx, ny, nz = density.shape
    px, py = lax.axis_size("gx"), lax.axis_size("gy")
    g = Geo(nx, ny, nz, px, py)
    zones = zone_low.shape[0]
    both = ("gx", "gy")
    flags = jnp.stack([lax.axis_index("gx"), lax.axis_index("gy")]).astype(jnp.int32)

    ext = ((g.ext, nz), F32)
    own_shape = ((2 * ny, nz), F32)
    trs_shape = ((g.pairs + 1, 2 * ny, nz), F32)
    sums_shape = ((px * py, nz), F32)
    block = ((nx, ny, nz), F32)
    flat = ((nx * ny, nz), F32)
    xa_shape = lambda f: (((f + 1) * 2 * ny, nz), F32)
    xb_shape = lambda f: ((f * 2 * ny, nz), F32)
    ymsg = lambda f: ((f * 2 * g.xp, nz), F32)
    xbound = ((2, 2 * ny, nz), F32)
    ybound = ((2, 2 * g.xp, nz), F32)
    win = pltpu.VMEM((g.win, nz), F32)
    ext_v = pltpu.VMEM((g.ext, nz), F32)
    core_scratch = [win] * 8 + [pltpu.VMEM((nx * ny, nz), F32)] + [ext_v] * 4

    own, xa, xb = call(
        functools.partial(first_kernel, g), "first", [own_shape, xa_shape(3), xb_shape(3)],
        [SMEM] + [HBM] * 4, (flags, density, slowness, zone_map, time_obs),
        [pltpu.VMEM((2, 1, 2, ny, nz), F32), pltpu.VMEM((2, 2, ny, nz), jnp.int32),
         pltpu.VMEM((nx, ny, nz), F32), pltpu.VMEM((nx, ny, nz), F32), pltpu.SemaphoreType.DMA((4 + nx // 4,))],
    )
    xa, xb = exchange("gx", xa, xb)
    low, high, q, table, ztable = call(
        functools.partial(spread_kernel, g, zones), "spread",
        [block] * 3 + [((2 * nz, 2 * nz), BF16), ((2 * nz, nz), BF16)],
        [SMEM, SMEM] + [VMEM] * 2, (zone_low, zone_high, zone_map, pressure_obs),
    )
    as_rows = lambda v: v.reshape(nx * ny, nz)
    ya, yb, pair = call(
        functools.partial(sides_kernel, g, 3), "sides", [ymsg(3)] * 2 + [own_shape],
        [SMEM] + [VMEM] * 7, (flags, xa, xb, own, table, as_rows(density), as_rows(slowness), as_rows(zone_map)),
    )
    ya, yb = exchange("gy", ya, yb)
    others = pair_totals(pair, px)
    ends = [flat, flat, sums_shape, own_shape, xa_shape(2), xb_shape(2)]
    outs = call(
        functools.partial(opening_step, g, zones), "opening",
        [ext, ext, trs_shape, xbound, xbound, ybound, ybound] + ends,
        [SMEM] * 3 + [VMEM] * (12 + len(others)),
        (flags, zone_low, zone_high, xa, xb, ya, yb, own, density, slowness, pressure_obs, q, time_obs, table, ztable, *others),
        core_scratch, 24,
    )
    rho_e, sig_e, trs, xlow, xhigh, ylow, yhigh, grho, gsig, sums, own, xa, xb = outs
    history = []
    for iteration in range(1, ITERS):
        last = iteration == ITERS - 1
        xa, xb = exchange("gx", xa, xb)
        sums = lax.all_to_all(sums, both, 0, 0, tiled=True)
        history.append(sums)
        ya, yb, pair = call(
            functools.partial(sides_kernel, g, 2), "sides", [ymsg(2)] * 2 + [own_shape],
            [SMEM] + [VMEM] * 6, (flags, xa, xb, own, sums, grho, gsig),
        )
        ya, yb = exchange("gy", ya, yb)
        others = pair_totals(pair, px)
        outs = call(
            functools.partial(later_step, g, last), "step", [ext, ext, trs_shape] + (ends[:3] if last else ends),
            [SMEM] + [VMEM] * (22 + len(others)),
            (flags, xa, xb, ya, yb, sums, own, grho, gsig, rho_e, sig_e, low, high, xlow, xhigh, ylow, yhigh, trs,
             pressure_obs, q, time_obs, table, ztable, *others),
            core_scratch, 24,
        )
        rho_e, sig_e, trs, grho, gsig, sums = outs[:6]
        if not last:
            own, xa, xb = outs[6:]
    sums = lax.all_to_all(sums, both, 0, 0, tiled=True)
    history.append(sums)
    rho, sigma, obj = call(
        functools.partial(closing_kernel, g), "closing", [block, block, ((8, nz), F32)],
        [VMEM] * 9, (*history, grho, gsig, rho_e, sig_e, low, high),
    )
    return rho, sigma, obj[0, :ITERS]


def solution(mesh):
    placed = (P("gx", "gy", None),) * 5 + (P(), P())
    return jax.shard_map(
        local,
        mesh=mesh,
        in_specs=placed,
        out_specs=(P("gx", "gy", None), P("gx", "gy", None), P()),
        check_vma=False,
    )
```

```python
import functools
import math

import jax
import jax.numpy as jnp
from jax import lax
from jax.experimental import pallas as pl
from jax.experimental.pallas import tpu as pltpu
from jax.sharding import PartitionSpec as P

ITERS = 3
BETA = 1.0
ETA = 0.5
EPSILON = 1e-06

XO = 2
YO = 4
F32 = jnp.float32
BF16 = jnp.bfloat16


class Geo:
    def __init__(self, nx, ny, nz, px, py):
        self.nx, self.ny, self.nz, self.px, self.py = nx, ny, nz, px, py
        self.pl = ny + 2 * YO
        self.planes = nx + 2 * XO
        self.ext = (nx + 8) * self.pl
        self.xp = nx + 8
        self.cells = float(nx * px * ny * py * nz)
        self.zs = 1.0 / math.sqrt(nz)
        self.xs = 1.0 / math.sqrt(nx * px)
        self.win = (nx + 2) * self.pl + 8
        self.pairs = px // 2

    def own(self, x):
        return (x + XO) * self.pl + YO


def fold8(v):
    total = v[0:8]
    for i in range(8, v.shape[0], 8):
        total = total + v[i : i + 8]
    return total


def pick_sides(even, first, last, a, b):
    low = jnp.where(even, b, a)
    high = jnp.where(even, a, b)
    return jnp.where(first, 0.0, low), jnp.where(last, 0.0, high)


def put_pair(even, low, high, a_ref, b_ref, at):
    n = low.shape[0]
    a_ref[at : at + n, :] = jnp.where(even, high, low)
    b_ref[at : at + n, :] = jnp.where(even, low, high)


def flags_of(g, flags):
    ix, iy = flags[0], flags[1]
    return ((ix % 2) == 0, ix == 0, ix == g.px - 1), ((iy % 2) == 0, iy == 0, iy == g.py - 1)


def split2(v):
    high = v.astype(BF16)
    low = (v - high.astype(F32)).astype(BF16)
    return jnp.concatenate([high, low], axis=1)


def bounds_of(zones, z, zlow, zhigh):
    low = jnp.full(z.shape, zlow[0], F32)
    high = jnp.full(z.shape, zhigh[0], F32)
    for i in range(1, zones):
        hit = z == i
        low = jnp.where(hit, zlow[i], low)
        high = jnp.where(hit, zhigh[i], high)
    return low, high


def first_kernel(g, flags, rho, sigma, zone, t, own, xa, xb, rims, zrims, sig_v, t_v, sems):
    (even, _, _), _ = flags_of(g, flags)
    step = 8
    small = []
    for k, at in enumerate((0, g.nx - 2)):
        small.append(pltpu.make_async_copy(rho.at[pl.ds(at, 2)], rims.at[k, 0], sems.at[2 * k]))
        small.append(pltpu.make_async_copy(zone.at[pl.ds(at, 2)], zrims.at[k], sems.at[2 * k + 1]))
    big = []
    for c in range(g.nx // step):
        at = pl.ds(c * step, step)
        big.append((
            pltpu.make_async_copy(sigma.at[at], sig_v.at[at], sems.at[4 + 2 * c]),
            pltpu.make_async_copy(t.at[at], t_v.at[at], sems.at[5 + 2 * c]),
        ))
    for a, b in big:
        a.start()
        b.start()
    for copy in small:
        copy.start()
    zero = jnp.zeros((g.ny, g.nz), F32)
    run, total, seen = zero, zero, zero
    for c, (a, b) in enumerate(big):
        a.wait()
        b.wait()
        for k in range(step):
            run = run + sig_v[c * step + k]
            total = total + run
            seen = seen + t_v[c * step + k]
    own[0 : g.ny, :] = run
    own[g.ny : 2 * g.ny, :] = total * g.xs - seen
    for copy in small:
        copy.wait()
    at = 0
    for r in range(2):
        put_pair(even, rims[0, 0, r], rims[1, 0, r], xa, xb, at)
        at += g.ny
    for r in range(2):
        put_pair(even, sig_v[r], sig_v[g.nx - 2 + r], xa, xb, at)
        at += g.ny
    for r in range(2):
        put_pair(even, zrims[0, r].astype(F32), zrims[1, r].astype(F32), xa, xb, at)
        at += g.ny
    xa[at : at + g.ny, :] = run
    xa[at + g.ny : at + 2 * g.ny, :] = total * g.xs - seen


def spread_kernel(g, zones, zlow, zhigh, zone, p, low_o, high_o, q, table, ztable):
    nz = g.nz
    row = lax.broadcasted_iota(jnp.int32, (2 * nz, 2 * nz), 0) % nz
    col = lax.broadcasted_iota(jnp.int32, (2 * nz, 2 * nz), 1)
    first = (row <= col).astype(F32)
    second = (nz - jnp.maximum(row, col - nz)).astype(F32)
    table[...] = jnp.where(col < nz, first, second).astype(BF16)
    r2 = lax.broadcasted_iota(jnp.int32, (2 * nz, nz), 0) % nz
    c2 = lax.broadcasted_iota(jnp.int32, (2 * nz, nz), 1)
    back = (r2 >= c2).astype(F32).astype(BF16)
    ztable[...] = ((r2 == c2 + 1).astype(F32) - (r2 == c2 - 1).astype(F32)).astype(BF16)
    step = 8

    def body(c, carry):
        for k in range(step):
            x = c * step + k
            low_o[x], high_o[x] = bounds_of(zones, zone[x], zlow, zhigh)
        rows = p[pl.ds(c * step, step)].reshape(step * g.ny, nz)
        out = jnp.dot(split2(rows), back, preferred_element_type=F32) * g.zs
        q[pl.ds(c * step, step)] = out.reshape(step, g.ny, nz)
        return carry

    lax.fori_loop(0, g.nx // step, body, 0)


def sides_kernel(g, fields, flags, xa, xb, own, order, *refs):
    blocks, (ya, yb, pair) = refs[:fields], refs[fields:]
    (xeven, xfirst, xlast), (yeven, _, _) = flags_of(g, flags)
    n = g.xp
    for f in range(fields):
        for r in range(2):
            low = blocks[f][pl.ds(r, g.nx, stride=g.ny), :].astype(F32)
            high = blocks[f][pl.ds(g.ny - 2 + r, g.nx, stride=g.ny), :].astype(F32)
            put_pair(yeven, low, high, ya, yb, (f * 2 + r) * n + XO)
    for f in range(fields):
        for px in range(2):
            at = (f * 2 + px) * g.ny
            sides = pick_sides(xeven, xfirst, xlast, xa[at : at + g.ny, :], xb[at : at + g.ny, :])
            for plane, value in zip((px, XO + g.nx + px), sides):
                for r in range(2):
                    spot = (f * 2 + r) * n + plane
                    put_pair(yeven, value[r : r + 1], value[g.ny - 2 + r : g.ny - 1 + r], ya, yb, spot)
    at = fields * 2 * g.ny
    mine_t, mine_s = own[0 : g.ny, :], own[g.ny : 2 * g.ny, :]
    other_t, other_s = xa[at : at + g.ny, :], xa[at + g.ny : at + 2 * g.ny, :]
    pair[0 : g.ny, :] = mine_t + other_t
    pair[g.ny : 2 * g.ny, :] = mine_s + other_s + jnp.where(xeven, mine_t, other_t) * (g.nx * g.xs)


def halo_slots(g):
    xs = []
    for r in range(2):
        xs.append((r * g.ny, pl.ds(r * g.pl + YO, g.ny), pl.ds((XO + g.nx + r) * g.pl + YO, g.ny)))
    ys = []
    for r in range(2):
        ys.append((r * g.xp, pl.ds(YO - 2 + r, g.xp, stride=g.pl), pl.ds(YO + g.ny + r, g.xp, stride=g.pl)))
    return xs, ys


def halo_values(g, flags, field, xa, xb, ya, yb):
    (xeven, xfirst, xlast), (yeven, yfirst, ylast) = flags_of(g, flags)
    xs, ys = halo_slots(g)
    for axis, slots, n, a, b, even, first, last in (
        (0, xs, g.ny, xa, xb, xeven, xfirst, xlast),
        (1, ys, g.xp, ya, yb, yeven, yfirst, ylast),
    ):
        for at, low_rows, high_rows in slots:
            here = pl.ds(field * 2 * n + at, n)
            low, high = pick_sides(even, first, last, a[here, :], b[here, :])
            yield axis, 0, at, low_rows, low
            yield axis, 1, at, high_rows, high


def lane_value(row, lane):
    ids = lax.broadcasted_iota(jnp.int32, row.shape, 1)
    return jnp.sum(jnp.where(ids == lane, row, 0.0), axis=1, keepdims=True)


def alphas(g, sums):
    row = jnp.sum(sums[...], axis=0, keepdims=True)
    return tuple(ETA * lax.rsqrt(lane_value(row, k) / g.cells + EPSILON) for k in range(2))


def ray_offsets(g, flags, trs):
    ix = flags[0]
    q = ix // 2
    even = (ix % 2) == 0
    ny = g.ny
    mine, other = trs[0, 0:ny, :], trs[1, 0:ny, :]
    reach = float(g.nx * g.xs)
    before = jnp.where(even, 0.0, other)
    sums = jnp.zeros_like(mine)
    spread = (mine + other) * (g.pairs - 1 - q).astype(F32)
    for m in range(1, g.pairs):
        p = q ^ m
        total = trs[1 + m, 0:ny, :]
        before = before + jnp.where(p < q, total, 0.0)
        sums = sums + jnp.where(p > q, trs[1 + m, ny : 2 * ny, :], 0.0)
        spread = spread + total * (g.pairs - 1 - jnp.maximum(p, q)).astype(F32)
    near = jnp.where(even, trs[1, ny : 2 * ny, :] + (before + mine) * reach, 0.0)
    return before, near + sums + spread * (2.0 * reach)


def step_core(g, flags, update, rho_e, sig_e, trs, p, q, t, table, ztable, outs, scratch):
    grho, gsig, sums, own, xa, xb = outs
    vxr, vxs, vyr, vys, vzr, vzs, gyr, gys, rt_s, az, bz, yu, ym = scratch
    nx, ny, nz, w = g.nx, g.ny, g.nz, g.pl
    (even, _, _), _ = flags_of(g, flags)
    zero = jnp.zeros((ny, nz), F32)
    zero8 = jnp.zeros((8, nz), F32)
    before, after = ray_offsets(g, flags, trs)
    step = 8
    rows = step * w

    def zdiff(v):
        return jnp.dot(split2(v), ztable[...], preferred_element_type=F32)

    edge = [ref[pl.ds(k * w, w), :] for ref in (rho_e, sig_e) for k in (1, XO + nx)]
    out = zdiff(jnp.concatenate(edge, axis=0))
    for i, (ref, k) in enumerate(((az, 1), (az, XO + nx), (bz, 1), (bz, XO + nx))):
        ref[pl.ds(k * w, w), :] = out[i * w : (i + 1) * w]

    def fields(c, carry):
        run, acc = carry
        for k in range(step):
            x = c * step + k
            at = pl.ds(g.own(x), ny)
            rho, sig = update(x, at)
            rho_e[at, :] = rho
            sig_e[at, :] = sig
            run = run + sig
            miss = run * g.xs - t[x]
            rt_s[pl.ds(x * ny, ny), :] = miss
            acc = acc + fold8(miss * miss)
        at = pl.ds((c * step + XO) * w, rows)
        pieces = split2(rho_e[at, :])
        az[at, :] = jnp.dot(pieces, ztable[...], preferred_element_type=F32)
        y = jnp.dot(pieces, table[...], preferred_element_type=F32)
        yu[at, :] = y[:, :nz]
        ym[at, :] = y[:, nz:]
        bz[at, :] = zdiff(sig_e[at, :])
        return run, acc

    _, acc_t = lax.fori_loop(0, nx // step, fields, (before, zero8), unroll=True)

    rowid = lax.broadcasted_iota(jnp.int32, (w, nz), 0)
    mine = jnp.logical_and(rowid >= 1, rowid <= ny)

    def slopes(ref, z, base):
        sx = ref[pl.ds(base + w, w), :] - ref[pl.ds(base - w, w), :]
        sy = ref[pl.ds(base + 1, w), :] - ref[pl.ds(base - 1, w), :]
        return sx, sy, z[pl.ds(base, w), :]

    def cross_plane(xi, acc, inside):
        base = (xi + XO - 1) * w + YO - 1
        a0, a1, a2 = slopes(rho_e, az, base)
        b0, b1, b2 = slopes(sig_e, bz, base)
        c0 = a1 * b2 - a2 * b1
        c1 = a2 * b0 - a0 * b2
        c2 = a0 * b1 - a1 * b0
        at = pl.ds(pl.multiple_of(xi * w, 8), w)
        vxr[at, :] = b1 * c2 - b2 * c1
        vxs[at, :] = c1 * a2 - c2 * a1
        if not inside:
            return acc
        vyr[at, :] = b2 * c0 - b0 * c2
        vys[at, :] = c2 * a0 - c0 * a2
        vzr[at, :] = b0 * c1 - b1 * c0
        vzs[at, :] = c0 * a1 - c1 * a0
        return acc + fold8(jnp.where(mine, c0 * c0 + c1 * c1 + c2 * c2, 0.0))

    cross_plane(0, None, False)
    cross_plane(nx + 1, None, False)
    acc_c = lax.fori_loop(1, nx + 1, lambda xi, acc: cross_plane(xi, acc, True), zero8, unroll=4)

    def adjoints(c, carry):
        start = (1 + c * step) * w
        at = pl.ds(pl.multiple_of(start, 8), rows)
        for vy, vz, out in ((vyr, vzr, gyr), (vys, vzs, gys)):
            along_y = vy[pl.ds(start - 1, rows), :] - vy[pl.ds(start + 1, rows), :]
            out[at, :] = along_y - zdiff(vz[at, :])
        return carry

    lax.fori_loop(0, nx // step, adjoints, 0, unroll=True)

    def gradients(i, carry):
        back, sum_t, sum_r, nr, ns, acc = carry
        x = nx - 1 - i
        lower = pl.ds(x * w + 1, ny)
        here = pl.ds((x + 1) * w + 1, ny)
        upper = pl.ds((x + 2) * w + 1, ny)
        at = pl.ds(g.own(x), ny)
        cr = (vxr[lower, :] - vxr[upper, :] + gyr[here, :]) * (BETA / 16.0)
        cs = (vxs[lower, :] - vxs[upper, :] + gys[here, :]) * (BETA / 16.0)
        back = back + rt_s[pl.ds(x * ny, ny), :]
        miss = yu[at, :] * g.zs - p[x]
        gr = ym[at, :] * (g.zs * g.zs) - q[x] + cr
        gs = back * g.xs + cs
        out = pl.ds(pl.multiple_of(x * ny, 8), ny)
        grho[out, :] = gr
        gsig[out, :] = gs
        weight = (i + 1).astype(F32)
        return (back, sum_t + gs, sum_r + gs * weight, nr + fold8(gr * gr), ns + fold8(gs * gs),
                acc + fold8(miss * miss))

    start = (after, zero, zero, zero8, zero8, zero8)
    _, sum_t, sum_r, nr, ns, acc_p = lax.fori_loop(0, nx, gradients, start, unroll=8)

    total = lambda v: jnp.sum(jnp.sum(v, axis=0, keepdims=True), axis=1, keepdims=True)
    lane = lax.broadcasted_iota(jnp.int32, sums.shape, 1)
    obj = acc_t + acc_p + acc_c * (BETA / 16.0)
    sums[...] = jnp.where(lane == 0, total(nr), jnp.where(lane == 1, total(ns), jnp.where(lane == 2, total(obj), 0.0)))
    if own is not None:
        rest = sum_r * g.xs
        pos = 0
        for block in (grho, gsig):
            for r in range(2):
                put_pair(even, block[pl.ds(r * ny, ny), :], block[pl.ds((nx - 2 + r) * ny, ny), :], xa, xb, pos)
                pos += ny
        for ref, at in ((own, 0), (xa, pos)):
            ref[at : at + ny, :] = sum_t
            ref[at + ny : at + 2 * ny, :] = rest


def opening_step(g, zones, flags, zlow, zhigh, xa, xb, ya, yb, own, rho, sig, p, q, t, table, ztable, *refs):
    others, rest = refs[: g.pairs - 1], refs[g.pairs - 1 :]
    rho_e, sig_e, trs, xlow, xhigh, ylow, yhigh = rest[:7]
    ny = g.ny
    for f, ext in ((0, rho_e), (1, sig_e)):
        for axis, side, at, spot, value in halo_values(g, flags, f, xa, xb, ya, yb):
            ext[spot, :] = value
    for axis, side, at, spot, value in halo_values(g, flags, 2, xa, xb, ya, yb):
        low, high = bounds_of(zones, value, zlow, zhigh)
        lows, highs = ((xlow, xhigh), (ylow, yhigh))[axis]
        lows[side, pl.ds(at, value.shape[0]), :] = low
        highs[side, pl.ds(at, value.shape[0]), :] = high
    pos = 6 * ny
    trs[0] = own[...]
    trs[1] = xa[pos : pos + 2 * ny, :]
    for m, other in enumerate(others):
        trs[2 + m] = other[...]
    step_core(g, flags, lambda x, at: (rho[x], sig[x]), rho_e, sig_e, trs, p, q, t, table, ztable, rest[7:13], rest[13:])


def later_step(g, last, flags, xa, xb, ya, yb, sums_i, own_i, grho_i, gsig_i, rho_i, sig_i, low, high,
               xlow, xhigh, ylow, yhigh, trs_i, p, q, t, table, ztable, *refs):
    others, rest = refs[: g.pairs - 1], refs[g.pairs - 1 :]
    rho_e, sig_e, trs = rest[:3]
    ny = g.ny
    ar, asig = alphas(g, sums_i)
    for axis, side, at, spot, value in halo_values(g, flags, 0, xa, xb, ya, yb):
        lows, highs = ((xlow, xhigh), (ylow, yhigh))[axis]
        here = pl.ds(at, value.shape[0])
        moved = rho_i[spot, :] - ar * value
        rho_e[spot, :] = jnp.minimum(jnp.maximum(moved, lows[side, here, :]), highs[side, here, :])
    for axis, side, at, spot, value in halo_values(g, flags, 1, xa, xb, ya, yb):
        sig_e[spot, :] = sig_i[spot, :] - asig * value
    pos = 4 * ny
    trs[0] = trs_i[0] - asig * own_i[...]
    trs[1] = trs_i[1] - asig * xa[pos : pos + 2 * ny, :]
    for m, other in enumerate(others):
        trs[2 + m] = trs_i[2 + m] - asig * other[...]

    def update(x, at):
        here = pl.ds(pl.multiple_of(x * ny, 8), ny)
        moved = rho_i[at, :] - ar * grho_i[here, :]
        return jnp.minimum(jnp.maximum(moved, low[x]), high[x]), sig_i[at, :] - asig * gsig_i[here, :]

    if last:
        outs, scratch = (*rest[3:6], None, None, None), rest[6:]
    else:
        outs, scratch = rest[3:9], rest[9:]
    step_core(g, flags, update, rho_e, sig_e, trs, p, q, t, table, ztable, outs, scratch)


def closing_kernel(g, sums0, sums1, sums2, grho, gsig, rho_e, sig_e, low, high, rho_o, sig_o, obj):
    ar, asig = alphas(g, sums2)

    def body(x, carry):
        at = pl.ds(g.own(x), g.ny)
        here = pl.ds(pl.multiple_of(x * g.ny, 8), g.ny)
        rho_o[x] = jnp.minimum(jnp.maximum(rho_e[at, :] - ar * grho[here, :], low[x]), high[x])
        sig_o[x] = sig_e[at, :] - asig * gsig[here, :]
        return carry

    lax.fori_loop(0, g.nx, body, 0, unroll=4)
    for k, sums in enumerate((sums0, sums1, sums2)):
        row = jnp.sum(sums[...], axis=0, keepdims=True)
        lane = lax.broadcasted_iota(jnp.int32, row.shape, 1)
        obj[k] = jnp.sum(jnp.where(lane == 2, row, 0.0)) * (0.5 / g.cells)


def pairs_of(size):
    a = [(i, i ^ 1) for i in range(size)]
    b = [(i, i if i in (0, size - 1) else ((i + 1) ^ 1) - 1) for i in range(size)]
    return a, b


def exchange(axis, a, b):
    pa, pb = pairs_of(lax.axis_size(axis))
    return lax.ppermute(a, axis, pa), lax.ppermute(b, axis, pb)


def pair_totals(pair, size):
    return [lax.ppermute(pair, "gx", [(i, i ^ (2 * m)) for i in range(size)]) for m in range(1, size // 2)]


SMEM = pl.BlockSpec(memory_space=pltpu.SMEM)
VMEM = pl.BlockSpec(memory_space=pltpu.VMEM)
HBM = pl.BlockSpec(memory_space=pltpu.HBM)


def call(body, name, shapes, specs, args, scratch=(), limit=12, outs=None):
    return pl.pallas_call(
        body,
        name=name,
        out_shape=[jax.ShapeDtypeStruct(s, d) for s, d in shapes],
        in_specs=specs,
        out_specs=outs or [VMEM] * len(shapes),
        scratch_shapes=list(scratch),
        compiler_params=pltpu.CompilerParams(vmem_limit_bytes=limit * 1024 * 1024),
    )(*args)


def local(density, slowness, pressure_obs, time_obs, zone_map, zone_low, zone_high):
    nx, ny, nz = density.shape
    px, py = lax.axis_size("gx"), lax.axis_size("gy")
    g = Geo(nx, ny, nz, px, py)
    zones = zone_low.shape[0]
    both = ("gx", "gy")
    flags = jnp.stack([lax.axis_index("gx"), lax.axis_index("gy")]).astype(jnp.int32)

    ext = ((g.ext, nz), F32)
    own_shape = ((2 * ny, nz), F32)
    trs_shape = ((g.pairs + 1, 2 * ny, nz), F32)
    sums_shape = ((px * py, nz), F32)
    block = ((nx, ny, nz), F32)
    flat = ((nx * ny, nz), F32)
    xa_shape = lambda f: (((f + 1) * 2 * ny, nz), F32)
    xb_shape = lambda f: ((f * 2 * ny, nz), F32)
    ymsg = lambda f: ((f * 2 * g.xp, nz), F32)
    xbound = ((2, 2 * ny, nz), F32)
    ybound = ((2, 2 * g.xp, nz), F32)
    win = pltpu.VMEM((g.win, nz), F32)
    ext_v = pltpu.VMEM((g.ext, nz), F32)
    core_scratch = [win] * 8 + [pltpu.VMEM((nx * ny, nz), F32)] + [ext_v] * 4

    own, xa, xb = call(
        functools.partial(first_kernel, g), "first", [own_shape, xa_shape(3), xb_shape(3)],
        [SMEM] + [HBM] * 4, (flags, *(pltpu.with_memory_space_constraint(v, pltpu.HBM) for v in (density, slowness, zone_map, time_obs))),
        [pltpu.VMEM((2, 1, 2, ny, nz), F32), pltpu.VMEM((2, 2, ny, nz), jnp.int32),
         pltpu.VMEM((nx, ny, nz), F32), pltpu.VMEM((nx, ny, nz), F32), pltpu.SemaphoreType.DMA((4 + nx // 4,))],
    )
    xa, xb = exchange("gx", xa, xb)
    low, high, q, table, ztable = call(
        functools.partial(spread_kernel, g, zones), "spread",
        [block] * 3 + [((2 * nz, 2 * nz), BF16), ((2 * nz, nz), BF16)],
        [SMEM, SMEM] + [VMEM] * 2, (zone_low, zone_high, zone_map, pressure_obs),
    )
    as_rows = lambda v: v.reshape(nx * ny, nz)
    ya, yb, pair = call(
        functools.partial(sides_kernel, g, 3), "sides", [ymsg(3)] * 2 + [own_shape],
        [SMEM] + [VMEM] * 7, (flags, xa, xb, own, table, as_rows(density), as_rows(slowness), as_rows(zone_map)),
    )
    ya, yb = exchange("gy", ya, yb)
    others = pair_totals(pair, px)
    ends = [flat, flat, sums_shape, own_shape, xa_shape(2), xb_shape(2)]
    outs = call(
        functools.partial(opening_step, g, zones), "opening",
        [ext, ext, trs_shape, xbound, xbound, ybound, ybound] + ends,
        [SMEM] * 3 + [VMEM] * (12 + len(others)),
        (flags, zone_low, zone_high, xa, xb, ya, yb, own, density, slowness, pressure_obs, q, time_obs, table, ztable, *others),
        core_scratch, 24,
    )
    rho_e, sig_e, trs, xlow, xhigh, ylow, yhigh, grho, gsig, sums, own, xa, xb = outs
    history = []
    for iteration in range(1, ITERS):
        last = iteration == ITERS - 1
        xa, xb = exchange("gx", xa, xb)
        sums = lax.all_to_all(sums, both, 0, 0, tiled=True)
        history.append(sums)
        ya, yb, pair = call(
            functools.partial(sides_kernel, g, 2), "sides", [ymsg(2)] * 2 + [own_shape],
            [SMEM] + [VMEM] * 6, (flags, xa, xb, own, sums, grho, gsig),
        )
        ya, yb = exchange("gy", ya, yb)
        others = pair_totals(pair, px)
        outs = call(
            functools.partial(later_step, g, last), "step", [ext, ext, trs_shape] + (ends[:3] if last else ends),
            [SMEM] + [VMEM] * (22 + len(others)),
            (flags, xa, xb, ya, yb, sums, own, grho, gsig, rho_e, sig_e, low, high, xlow, xhigh, ylow, yhigh, trs,
             pressure_obs, q, time_obs, table, ztable, *others),
            core_scratch, 24,
        )
        rho_e, sig_e, trs, grho, gsig, sums = outs[:6]
        if not last:
            own, xa, xb = outs[6:]
    sums = lax.all_to_all(sums, both, 0, 0, tiled=True)
    history.append(sums)
    rho, sigma, obj = call(
        functools.partial(closing_kernel, g), "closing", [block, block, ((ITERS,), F32)],
        [VMEM] * 9, (*history, grho, gsig, rho_e, sig_e, low, high), outs=[VMEM, VMEM, SMEM],
    )
    return rho, sigma, obj


def solution(mesh):
    placed = (P("gx", "gy", None),) * 5 + (P(), P())
    return jax.shard_map(
        local,
        mesh=mesh,
        in_specs=placed,
        out_specs=(P("gx", "gy", None), P("gx", "gy", None), P()),
        check_vma=False,
    )
```

```python
import functools
import math

import jax
import jax.numpy as jnp
from jax import lax
from jax.experimental import pallas as pl
from jax.experimental.pallas import tpu as pltpu
from jax.sharding import PartitionSpec as P


ITERS = 3
BETA = 1.0
ETA = 0.5
EPSILON = 1e-06

XO = 2
YO = 4
CHUNK = 4
DIAGONALS = ((-1, -1), (-1, 1), (1, -1), (1, 1))
F32 = jnp.float32
BF16 = jnp.bfloat16


class Geo:
    def __init__(self, nx, ny, nz, px, py):
        self.nx, self.ny, self.nz, self.px, self.py = nx, ny, nz, px, py
        self.pl = ny + 2 * YO
        self.ext = (nx + 8) * self.pl
        self.xp = nx + 8
        self.cells = float(nx * px * ny * py * nz)
        self.zs = 1.0 / math.sqrt(nz)
        self.xs = 1.0 / math.sqrt(nx * px)
        self.win = (nx + 2) * self.pl + 8
        self.pairs = px // 2

    def own(self, x):
        return (x + XO) * self.pl + YO


def fold8(v):
    total = v[0:8]
    for i in range(8, v.shape[0], 8):
        total = total + v[i : i + 8]
    return total


def pick_sides(even, first, last, a, b):
    low = jnp.where(even, b, a)
    high = jnp.where(even, a, b)
    return jnp.where(first, 0.0, low), jnp.where(last, 0.0, high)


def put_pair(even, low, high, a_ref, b_ref, at):
    n = low.shape[0]
    a_ref[at : at + n, :] = jnp.where(even, high, low)
    b_ref[at : at + n, :] = jnp.where(even, low, high)


def flags_of(g, flags):
    ix, iy = flags[0], flags[1]
    return ((ix % 2) == 0, ix == 0, ix == g.px - 1), ((iy % 2) == 0, iy == 0, iy == g.py - 1)


def split2(v):
    high = v.astype(BF16)
    low = (v - high.astype(F32)).astype(BF16)
    return jnp.concatenate([high, low], axis=1)


def bounds_of(zones, z, zlow, zhigh):
    low = jnp.full(z.shape, zlow[0], F32)
    high = jnp.full(z.shape, zhigh[0], F32)
    for i in range(1, zones):
        hit = z == i
        low = jnp.where(hit, zlow[i], low)
        high = jnp.where(hit, zhigh[i], high)
    return low, high


def first_kernel(g, flags, rho, sigma, zone, t, own, xa, xb, rims, zrims, sig_v, t_v, sems):
    (even, _, _), _ = flags_of(g, flags)
    step = 8
    small = []
    for k, at in enumerate((0, g.nx - 2)):
        small.append(pltpu.make_async_copy(rho.at[pl.ds(at, 2)], rims.at[k, 0], sems.at[2 * k]))
        small.append(pltpu.make_async_copy(zone.at[pl.ds(at, 2)], zrims.at[k], sems.at[2 * k + 1]))
    big = []
    for c in range(g.nx // step):
        at = pl.ds(c * step, step)
        big.append((
            pltpu.make_async_copy(sigma.at[at], sig_v.at[at], sems.at[4 + 2 * c]),
            pltpu.make_async_copy(t.at[at], t_v.at[at], sems.at[5 + 2 * c]),
        ))
    for a, b in big:
        a.start()
        b.start()
    for copy in small:
        copy.start()
    zero = jnp.zeros((g.ny, g.nz), F32)
    run, total, seen = zero, zero, zero
    for c, (a, b) in enumerate(big):
        a.wait()
        b.wait()
        for k in range(step):
            run = run + sig_v[c * step + k]
            total = total + run
            seen = seen + t_v[c * step + k]
    own[0 : g.ny, :] = run
    own[g.ny : 2 * g.ny, :] = total * g.xs - seen
    for copy in small:
        copy.wait()
    at = 0
    for r in range(2):
        put_pair(even, rims[0, 0, r], rims[1, 0, r], xa, xb, at)
        at += g.ny
    for r in range(2):
        put_pair(even, sig_v[r], sig_v[g.nx - 2 + r], xa, xb, at)
        at += g.ny
    for r in range(2):
        put_pair(even, zrims[0, r].astype(F32), zrims[1, r].astype(F32), xa, xb, at)
        at += g.ny
    xa[at : at + g.ny, :] = run
    xa[at + g.ny : at + 2 * g.ny, :] = total * g.xs - seen


def spread_kernel(g, zones, zlow, zhigh, zone, p, low_o, high_o, q, table, ztable):
    nz = g.nz
    row = lax.broadcasted_iota(jnp.int32, (2 * nz, 2 * nz), 0) % nz
    col = lax.broadcasted_iota(jnp.int32, (2 * nz, 2 * nz), 1)
    first = (row <= col).astype(F32)
    second = (nz - jnp.maximum(row, col - nz)).astype(F32)
    table[...] = jnp.where(col < nz, first, second).astype(BF16)
    r2 = lax.broadcasted_iota(jnp.int32, (2 * nz, nz), 0) % nz
    c2 = lax.broadcasted_iota(jnp.int32, (2 * nz, nz), 1)
    back = (r2 >= c2).astype(F32).astype(BF16)
    ztable[...] = ((r2 == c2 + 1).astype(F32) - (r2 == c2 - 1).astype(F32)).astype(BF16)
    step = 8

    def body(c, carry):
        for k in range(step):
            x = c * step + k
            low_o[x], high_o[x] = bounds_of(zones, zone[x], zlow, zhigh)
        rows = p[pl.ds(c * step, step)].reshape(step * g.ny, nz)
        out = jnp.dot(split2(rows), back, preferred_element_type=F32) * g.zs
        q[pl.ds(c * step, step)] = out.reshape(step, g.ny, nz)
        return carry

    lax.fori_loop(0, g.nx // step, body, 0)


def join_kernel(g, flags, xa, own, head, pair, sums):
    (even, _, _), _ = flags_of(g, flags)
    ny = g.ny
    at = 4 * ny
    join_pair(g, even, own, xa, at, pair)
    n = sums.shape[0] // CHUNK
    sums[...] = jnp.zeros(sums.shape, F32)
    sums[pl.ds(0, n, stride=CHUNK), :] = jnp.broadcast_to(head[0:1, :], (n, g.nz))
    for k, (dx, dy) in enumerate(DIAGONALS):
        ok, there = diagonal(g, flags, dx, dy)

        @pl.when(ok)
        def _():
            for f in range(2):
                sums[pl.ds(there * CHUNK + 1 + f, 1), :] = head[8 + 2 * k + f : 9 + 2 * k + f, :]


def diagonal(g, flags, dx, dy):
    ix, iy = flags[0] + dx, flags[1] + dy
    ok = jnp.logical_and(jnp.logical_and(ix >= 0, ix < g.px), jnp.logical_and(iy >= 0, iy < g.py))
    return ok, jnp.where(ok, ix * g.py + iy, 0)


def join_pair(g, even, own, xa, at, pair):
    ny = g.ny
    mine_t, mine_s = own[0:ny, :], own[ny : 2 * ny, :]
    other_t, other_s = xa[at : at + ny, :], xa[at + ny : at + 2 * ny, :]
    pair[0:ny, :] = mine_t + other_t
    pair[ny : 2 * ny, :] = mine_s + other_s + jnp.where(even, mine_t, other_t) * (g.nx * g.xs)


def sides_kernel(g, fields, flags, xa, xb, own, *refs):
    blocks, (ya, yb, pair) = refs[:fields], refs[fields:]
    (xeven, xfirst, xlast), (yeven, _, _) = flags_of(g, flags)
    n = g.xp
    for f in range(fields):
        for r in range(2):
            low = blocks[f][pl.ds(r, g.nx, stride=g.ny), :].astype(F32)
            high = blocks[f][pl.ds(g.ny - 2 + r, g.nx, stride=g.ny), :].astype(F32)
            put_pair(yeven, low, high, ya, yb, (f * 2 + r) * n + XO)
    for f in range(fields):
        for px in range(2):
            at = (f * 2 + px) * g.ny
            sides = pick_sides(xeven, xfirst, xlast, xa[at : at + g.ny, :], xb[at : at + g.ny, :])
            for plane, value in zip((px, XO + g.nx + px), sides):
                for r in range(2):
                    spot = (f * 2 + r) * n + plane
                    put_pair(yeven, value[r : r + 1], value[g.ny - 2 + r : g.ny - 1 + r], ya, yb, spot)
    join_pair(g, xeven, own, xa, fields * 2 * g.ny, pair)


def halo_slots(g, n, off):
    xs = []
    for r in range(2):
        xs.append((r * g.ny, pl.ds(r * g.pl + YO, g.ny), pl.ds((XO + g.nx + r) * g.pl + YO, g.ny)))
    ys = []
    for r in range(2):
        first = off * g.pl + r
        ys.append((r * n, pl.ds(first + YO - 2, n, stride=g.pl), pl.ds(first + YO + g.ny, n, stride=g.pl)))
    return xs, ys


def halo_values(g, flags, field, xa, xb, ya, yb, yn, off):
    (xeven, xfirst, xlast), (yeven, yfirst, ylast) = flags_of(g, flags)
    xs, ys = halo_slots(g, yn, off)
    for axis, slots, n, a, b, even, first, last in (
        (0, xs, g.ny, xa, xb, xeven, xfirst, xlast),
        (1, ys, yn, ya, yb, yeven, yfirst, ylast),
    ):
        for at, low_rows, high_rows in slots:
            here = pl.ds(field * 2 * n + at, n)
            low, high = pick_sides(even, first, last, a[here, :], b[here, :])
            yield axis, 0, at, low_rows, low
            yield axis, 1, at, high_rows, high


def lane_value(row, lane):
    ids = lax.broadcasted_iota(jnp.int32, row.shape, 1)
    return jnp.sum(jnp.where(ids == lane, row, 0.0), axis=1, keepdims=True)


def sum_row(g, sums):
    n = g.px * g.py
    return jnp.sum(sums[pl.ds(0, n, stride=sums.shape[0] // n), :], axis=0, keepdims=True)


def alphas(g, sums):
    row = sum_row(g, sums)
    return tuple(ETA * lax.rsqrt(lane_value(row, k) / g.cells + EPSILON) for k in range(2))


def ray_offsets(g, flags, trs):
    ix = flags[0]
    q = ix // 2
    even = (ix % 2) == 0
    ny = g.ny
    mine, other = trs[0, 0:ny, :], trs[1, 0:ny, :]
    reach = float(g.nx * g.xs)
    before = jnp.where(even, 0.0, other)
    sums = jnp.zeros_like(mine)
    spread = (mine + other) * (g.pairs - 1 - q).astype(F32)
    for m in range(1, g.pairs):
        p = q ^ m
        total = trs[1 + m, 0:ny, :]
        before = before + jnp.where(p < q, total, 0.0)
        sums = sums + jnp.where(p > q, trs[1 + m, ny : 2 * ny, :], 0.0)
        spread = spread + total * (g.pairs - 1 - jnp.maximum(p, q)).astype(F32)
    near = jnp.where(even, trs[1, ny : 2 * ny, :] + (before + mine) * reach, 0.0)
    return before, near + sums + spread * (2.0 * reach)


def step_core(g, flags, update, rho_e, sig_e, trs, p, q, t, table, ztable, outs, scratch):
    grho, gsig, sums, own, xa, xb, ya, yb = outs
    vxr, vxs, vyr, vys, vzr, vzs, gyr, gys, rt_s, az, bz, yu, ym = scratch
    nx, ny, nz, w = g.nx, g.ny, g.nz, g.pl
    (even, _, _), (yeven, _, _) = flags_of(g, flags)
    zero = jnp.zeros((ny, nz), F32)
    zero8 = jnp.zeros((8, nz), F32)
    before, after = ray_offsets(g, flags, trs)
    step = 8
    rows = step * w

    def zdiff(v):
        return jnp.dot(split2(v), ztable[...], preferred_element_type=F32)

    edge = [ref[pl.ds(k * w, w), :] for ref in (rho_e, sig_e) for k in (1, XO + nx)]
    out = zdiff(jnp.concatenate(edge, axis=0))
    for i, (ref, k) in enumerate(((az, 1), (az, XO + nx), (bz, 1), (bz, XO + nx))):
        ref[pl.ds(k * w, w), :] = out[i * w : (i + 1) * w]

    def fields(c, carry):
        run, acc = carry
        for k in range(step):
            x = c * step + k
            at = pl.ds(g.own(x), ny)
            rho, sig = update(x, at)
            rho_e[at, :] = rho
            sig_e[at, :] = sig
            run = run + sig
            miss = run * g.xs - t[x]
            rt_s[pl.ds(x * ny, ny), :] = miss
            acc = acc + fold8(miss * miss)
        at = pl.ds((c * step + XO) * w, rows)
        pieces = split2(rho_e[at, :])
        az[at, :] = jnp.dot(pieces, ztable[...], preferred_element_type=F32)
        y = jnp.dot(pieces, table[...], preferred_element_type=F32)
        yu[at, :] = y[:, :nz]
        ym[at, :] = y[:, nz:]
        bz[at, :] = zdiff(sig_e[at, :])
        return run, acc

    _, acc_t = lax.fori_loop(0, nx // step, fields, (before, zero8), unroll=True)

    rowid = lax.broadcasted_iota(jnp.int32, (w, nz), 0)
    mine = jnp.logical_and(rowid >= 1, rowid <= ny)

    def slopes(ref, z, base):
        sx = ref[pl.ds(base + w, w), :] - ref[pl.ds(base - w, w), :]
        sy = ref[pl.ds(base + 1, w), :] - ref[pl.ds(base - 1, w), :]
        return sx, sy, z[pl.ds(base, w), :]

    def cross_plane(xi, acc, inside):
        base = (xi + XO - 1) * w + YO - 1
        a0, a1, a2 = slopes(rho_e, az, base)
        b0, b1, b2 = slopes(sig_e, bz, base)
        c0 = a1 * b2 - a2 * b1
        c1 = a2 * b0 - a0 * b2
        c2 = a0 * b1 - a1 * b0
        at = pl.ds(pl.multiple_of(xi * w, 8), w)
        vxr[at, :] = b1 * c2 - b2 * c1
        vxs[at, :] = c1 * a2 - c2 * a1
        if not inside:
            return acc
        vyr[at, :] = b2 * c0 - b0 * c2
        vys[at, :] = c2 * a0 - c0 * a2
        vzr[at, :] = b0 * c1 - b1 * c0
        vzs[at, :] = c0 * a1 - c1 * a0
        return acc + fold8(jnp.where(mine, c0 * c0 + c1 * c1 + c2 * c2, 0.0))

    cross_plane(0, None, False)
    cross_plane(nx + 1, None, False)
    acc_c = lax.fori_loop(1, nx + 1, lambda xi, acc: cross_plane(xi, acc, True), zero8, unroll=4)

    def adjoints(c, carry):
        start = (1 + c * step) * w
        at = pl.ds(pl.multiple_of(start, 8), rows)
        for vy, vz, out in ((vyr, vzr, gyr), (vys, vzs, gys)):
            along_y = vy[pl.ds(start - 1, rows), :] - vy[pl.ds(start + 1, rows), :]
            out[at, :] = along_y - zdiff(vz[at, :])
        return carry

    lax.fori_loop(0, nx // step, adjoints, 0, unroll=True)

    def gradients(i, carry):
        back, sum_t, sum_r, nr, ns, acc = carry
        x = nx - 1 - i
        lower = pl.ds(x * w + 1, ny)
        here = pl.ds((x + 1) * w + 1, ny)
        upper = pl.ds((x + 2) * w + 1, ny)
        at = pl.ds(g.own(x), ny)
        cr = (vxr[lower, :] - vxr[upper, :] + gyr[here, :]) * (BETA / 16.0)
        cs = (vxs[lower, :] - vxs[upper, :] + gys[here, :]) * (BETA / 16.0)
        back = back + rt_s[pl.ds(x * ny, ny), :]
        miss = yu[at, :] * g.zs - p[x]
        gr = ym[at, :] * (g.zs * g.zs) - q[x] + cr
        gs = back * g.xs + cs
        out = pl.ds(pl.multiple_of(x * ny, 8), ny)
        grho[out, :] = gr
        gsig[out, :] = gs
        weight = (i + 1).astype(F32)
        return (back, sum_t + gs, sum_r + gs * weight, nr + fold8(gr * gr), ns + fold8(gs * gs),
                acc + fold8(miss * miss))

    start = (after, zero, zero, zero8, zero8, zero8)
    _, sum_t, sum_r, nr, ns, acc_p = lax.fori_loop(0, nx, gradients, start, unroll=8)

    total = lambda v: jnp.sum(jnp.sum(v, axis=0, keepdims=True), axis=1, keepdims=True)
    spread = sums.shape[0] if own is None else 8
    lane = lax.broadcasted_iota(jnp.int32, (spread, nz), 1)
    obj = acc_t + acc_p + acc_c * (BETA / 16.0)
    sums[0:spread, :] = jnp.where(lane == 0, total(nr), jnp.where(lane == 1, total(ns), jnp.where(lane == 2, total(obj), 0.0)))
    if own is not None:
        rest = sum_r * g.xs
        pos = 0
        for block in (grho, gsig):
            for r in range(2):
                put_pair(even, block[pl.ds(r * ny, ny), :], block[pl.ds((nx - 2 + r) * ny, ny), :], xa, xb, pos)
                pos += ny
        for ref, at in ((own, 0), (xa, pos)):
            ref[at : at + ny, :] = sum_t
            ref[at + ny : at + 2 * ny, :] = rest
        for f, block in enumerate((grho, gsig)):
            for r in range(2):
                rows_low = block[pl.ds(r, nx, stride=ny), :]
                rows_high = block[pl.ds(ny - 2 + r, nx, stride=ny), :]
                put_pair(yeven, rows_low, rows_high, ya, yb, (f * 2 + r) * nx)
            for k, (dx, dy) in enumerate(DIAGONALS):
                cell = (0 if dx < 0 else nx - 1) * ny + (0 if dy < 0 else ny - 1)
                sums[8 + 2 * k + f : 9 + 2 * k + f, :] = block[cell : cell + 1, :]


def opening_step(g, zones, flags, zlow, zhigh, xa, xb, ya, yb, own, rho, sig, p, q, t, table, ztable, *refs):
    others, rest = refs[: g.pairs - 1], refs[g.pairs - 1 :]
    rho_e, sig_e, trs, xlow, xhigh, ylow, yhigh = rest[:7]
    ny = g.ny
    for f, ext in ((0, rho_e), (1, sig_e)):
        for axis, side, at, spot, value in halo_values(g, flags, f, xa, xb, ya, yb, g.xp, 0):
            ext[spot, :] = value
    for axis, side, at, spot, value in halo_values(g, flags, 2, xa, xb, ya, yb, g.xp, 0):
        low, high = bounds_of(zones, value, zlow, zhigh)
        lows, highs = ((xlow, xhigh), (ylow, yhigh))[axis]
        lows[side, pl.ds(at, value.shape[0]), :] = low
        highs[side, pl.ds(at, value.shape[0]), :] = high
    pos = 6 * ny
    trs[0] = own[...]
    trs[1] = xa[pos : pos + 2 * ny, :]
    for m, other in enumerate(others):
        trs[2 + m] = other[...]
    step_core(g, flags, lambda x, at: (rho[x], sig[x]), rho_e, sig_e, trs, p, q, t, table, ztable, rest[7:15], rest[15:])


def later_step(g, last, flags, xa, xb, ya, yb, sums_i, own_i, grho_i, gsig_i, rho_i, sig_i, low, high,
               xlow, xhigh, ylow, yhigh, trs_i, p, q, t, table, ztable, *refs):
    others, rest = refs[: g.pairs - 1], refs[g.pairs - 1 :]
    rho_e, sig_e, trs = rest[:3]
    ny = g.ny
    ar, asig = alphas(g, sums_i)
    clip = lambda v, lows, highs: jnp.minimum(jnp.maximum(v, lows), highs)
    for axis, side, at, spot, value in halo_values(g, flags, 0, xa, xb, ya, yb, g.nx, XO):
        lows, highs = ((xlow, xhigh), (ylow, yhigh))[axis]
        if axis == 1:
            at = at // g.nx * g.xp + XO
        here = pl.ds(at, value.shape[0])
        rho_e[spot, :] = clip(rho_i[spot, :] - ar * value, lows[side, here, :], highs[side, here, :])
    for axis, side, at, spot, value in halo_values(g, flags, 1, xa, xb, ya, yb, g.nx, XO):
        sig_e[spot, :] = sig_i[spot, :] - asig * value
    for dx, dy in DIAGONALS:
        ok, there = diagonal(g, flags, dx, dy)
        plane = XO - 1 if dx < 0 else XO + g.nx
        side = 0 if dy < 0 else 1
        here = pl.ds((1 - side) * g.xp + plane, 1)
        spot = pl.ds(plane * g.pl + (YO - 1 if dy < 0 else YO + ny), 1)
        value = jnp.where(ok, sums_i[pl.ds(there * CHUNK + 1, 1), :], 0.0)
        rho_e[spot, :] = clip(rho_i[spot, :] - ar * value, ylow[side, here, :], yhigh[side, here, :])
        value = jnp.where(ok, sums_i[pl.ds(there * CHUNK + 2, 1), :], 0.0)
        sig_e[spot, :] = sig_i[spot, :] - asig * value
    pos = 4 * ny
    trs[0] = trs_i[0] - asig * own_i[...]
    trs[1] = trs_i[1] - asig * xa[pos : pos + 2 * ny, :]
    for m, other in enumerate(others):
        trs[2 + m] = trs_i[2 + m] - asig * other[...]

    def update(x, at):
        here = pl.ds(pl.multiple_of(x * ny, 8), ny)
        moved = rho_i[at, :] - ar * grho_i[here, :]
        return clip(moved, low[x], high[x]), sig_i[at, :] - asig * gsig_i[here, :]

    if last:
        outs, scratch = (*rest[3:6], None, None, None, None, None), rest[6:]
    else:
        outs, scratch = rest[3:11], rest[11:]
    step_core(g, flags, update, rho_e, sig_e, trs, p, q, t, table, ztable, outs, scratch)


def closing_kernel(g, sums0, sums1, sums2, grho, gsig, rho_e, sig_e, low, high, rho_o, sig_o, obj):
    ar, asig = alphas(g, sums2)

    def body(x, carry):
        at = pl.ds(g.own(x), g.ny)
        here = pl.ds(pl.multiple_of(x * g.ny, 8), g.ny)
        rho_o[x] = jnp.minimum(jnp.maximum(rho_e[at, :] - ar * grho[here, :], low[x]), high[x])
        sig_o[x] = sig_e[at, :] - asig * gsig[here, :]
        return carry

    lax.fori_loop(0, g.nx, body, 0, unroll=4)
    for k, sums in enumerate((sums0, sums1, sums2)):
        row = sum_row(g, sums)
        lane = lax.broadcasted_iota(jnp.int32, row.shape, 1)
        obj[k] = jnp.sum(jnp.where(lane == 2, row, 0.0)) * (0.5 / g.cells)


def pairs_of(size):
    a = [(i, i ^ 1) for i in range(size)]
    b = [(i, i if i in (0, size - 1) else ((i + 1) ^ 1) - 1) for i in range(size)]
    return a, b


def exchange(axis, a, b):
    pa, pb = pairs_of(lax.axis_size(axis))
    a = lax.ppermute(a, axis, pa)
    b = lax.ppermute(b, axis, pb)
    return a, b


def pair_totals(pair, size):
    out = []
    for m in range(1, size // 2):
        out.append(lax.ppermute(pair, "gx", [(i, i ^ (2 * m)) for i in range(size)]))
    return out


SMEM = pl.BlockSpec(memory_space=pltpu.SMEM)
VMEM = pl.BlockSpec(memory_space=pltpu.VMEM)
HBM = pl.BlockSpec(memory_space=pltpu.HBM)


def call(body, shapes, specs, args, scratch=(), limit=12, outs=None):
    return pl.pallas_call(
        body,
        out_shape=[jax.ShapeDtypeStruct(s, d) for s, d in shapes],
        in_specs=specs,
        out_specs=outs or [VMEM] * len(shapes),
        scratch_shapes=list(scratch),
        compiler_params=pltpu.CompilerParams(vmem_limit_bytes=limit * 1024 * 1024),
    )(*args)


def local(density, slowness, pressure_obs, time_obs, zone_map, zone_low, zone_high):
    nx, ny, nz = density.shape
    px, py = lax.axis_size("gx"), lax.axis_size("gy")
    g = Geo(nx, ny, nz, px, py)
    zones = zone_low.shape[0]
    both = ("gx", "gy")
    flags = jnp.stack([lax.axis_index("gx"), lax.axis_index("gy")]).astype(jnp.int32)

    ext = ((g.ext, nz), F32)
    own_shape = ((2 * ny, nz), F32)
    trs_shape = ((g.pairs + 1, 2 * ny, nz), F32)
    sums_shape = ((px * py, nz), F32)
    block = ((nx, ny, nz), F32)
    flat = ((nx * ny, nz), F32)
    xa_shape = lambda f: (((f + 1) * 2 * ny, nz), F32)
    xb_shape = lambda f: ((f * 2 * ny, nz), F32)
    ymsg = lambda f: ((f * 2 * g.xp, nz), F32)
    xbound = ((2, 2 * ny, nz), F32)
    ybound = ((2, 2 * g.xp, nz), F32)
    win = pltpu.VMEM((g.win, nz), F32)
    ext_v = pltpu.VMEM((g.ext, nz), F32)
    core_scratch = [win] * 8 + [pltpu.VMEM((nx * ny, nz), F32)] + [ext_v] * 4

    own, xa, xb = call(
        functools.partial(first_kernel, g), [own_shape, xa_shape(3), xb_shape(3)],
        [SMEM] + [HBM] * 4, (flags, *(pltpu.with_memory_space_constraint(v, pltpu.HBM) for v in (density, slowness, zone_map, time_obs))),
        [pltpu.VMEM((2, 1, 2, ny, nz), F32), pltpu.VMEM((2, 2, ny, nz), jnp.int32),
         pltpu.VMEM((nx, ny, nz), F32), pltpu.VMEM((nx, ny, nz), F32), pltpu.SemaphoreType.DMA((4 + nx // 4,))],
    )
    xa, xb = exchange("gx", xa, xb)
    low, high, q, table, ztable = call(
        functools.partial(spread_kernel, g, zones),
        [block] * 3 + [((2 * nz, 2 * nz), BF16), ((2 * nz, nz), BF16)],
        [SMEM, SMEM] + [VMEM] * 2, (zone_low, zone_high, zone_map, pressure_obs),
    )
    as_rows = lambda v: v.reshape(nx * ny, nz)
    ya, yb, pair = call(
        functools.partial(sides_kernel, g, 3), [ymsg(3)] * 2 + [own_shape],
        [SMEM] + [VMEM] * 6, (flags, xa, xb, own, as_rows(density), as_rows(slowness), as_rows(zone_map)),
    )
    ya, yb = exchange("gy", ya, yb)
    others = pair_totals(pair, px)
    yown = ((4 * nx, nz), F32)
    ends = [flat, flat, ((16, nz), F32), own_shape, xa_shape(2), xb_shape(2), yown, yown]
    chunks = ((px * py * CHUNK, nz), F32)
    outs = call(
        functools.partial(opening_step, g, zones),
        [ext, ext, trs_shape, xbound, xbound, ybound, ybound] + ends,
        [SMEM] * 3 + [VMEM] * (12 + len(others)),
        (flags, zone_low, zone_high, xa, xb, ya, yb, own, density, slowness, pressure_obs, q, time_obs, table, ztable, *others),
        core_scratch, 24,
    )
    rho_e, sig_e, trs, xlow, xhigh, ylow, yhigh, grho, gsig, head, own, xa, xb, ya, yb = outs
    history = []
    for iteration in range(1, ITERS):
        last = iteration == ITERS - 1
        xa, xb = exchange("gx", xa, xb)
        ya, yb = exchange("gy", ya, yb)
        pair, sums = call(
            functools.partial(join_kernel, g), [own_shape, chunks], [SMEM] + [VMEM] * 3,
            (flags, xa, own, head),
        )
        others = pair_totals(pair, px)
        sums = lax.all_to_all(sums, both, 0, 0, tiled=True)
        history.append(sums)
        outs = call(
            functools.partial(later_step, g, last), [ext, ext, trs_shape] + ([flat, flat, sums_shape] if last else ends),
            [SMEM] + [VMEM] * (22 + len(others)),
            (flags, xa, xb, ya, yb, sums, own, grho, gsig, rho_e, sig_e, low, high, xlow, xhigh, ylow, yhigh, trs,
             pressure_obs, q, time_obs, table, ztable, *others),
            core_scratch, 24,
        )
        rho_e, sig_e, trs, grho, gsig, head = outs[:6]
        if not last:
            own, xa, xb, ya, yb = outs[6:]
    history.append(lax.all_to_all(head, both, 0, 0, tiled=True))
    rho, sigma, obj = call(
        functools.partial(closing_kernel, g), [block, block, ((ITERS,), F32)],
        [VMEM] * 9, (*history, grho, gsig, rho_e, sig_e, low, high), outs=[VMEM, VMEM, SMEM],
    )
    return rho, sigma, obj


def solution(mesh):
    placed = (P("gx", "gy", None),) * 5 + (P(), P())
    return jax.shard_map(
        local,
        mesh=mesh,
        in_specs=placed,
        out_specs=(P("gx", "gy", None), P("gx", "gy", None), P()),
        check_vma=False,
    )
```

```python
import functools
import math

import jax
import jax.numpy as jnp
from jax import lax
from jax.experimental import pallas as pl
from jax.experimental.pallas import tpu as pltpu
from jax.sharding import PartitionSpec as P


ITERS = 3
BETA = 1.0
ETA = 0.5
EPSILON = 1e-06

XO = 2
YO = 8
CHUNK = 4
STEP = 16
UNROLL_FIELDS = 4
UNROLL_MAIN = 2
SCALE = 16.0 / BETA
DIAGONALS = ((-1, -1), (-1, 1), (1, -1), (1, 1))
F32 = jnp.float32
BF16 = jnp.bfloat16


class Geo:
    def __init__(self, nx, ny, nz, px, py):
        self.nx, self.ny, self.nz, self.px, self.py = nx, ny, nz, px, py
        self.pl = ny + YO
        self.ext = (nx + 9) * self.pl
        self.xp = nx + 8
        self.cells = float(nx * px * ny * py * nz)
        self.zs = 1.0 / math.sqrt(nz)
        self.xs = 1.0 / math.sqrt(nx * px)
        self.win = (nx + 2) * ny
        self.pairs = px // 2

    def own(self, x):
        return (x + XO) * self.pl + YO


def fold8(v):
    total = v[0:8]
    for i in range(8, v.shape[0], 8):
        total = total + v[i : i + 8]
    return total


def pick_sides(even, first, last, a, b):
    low = jnp.where(even, b, a)
    high = jnp.where(even, a, b)
    return jnp.where(first, 0.0, low), jnp.where(last, 0.0, high)


def put_pair(even, low, high, a_ref, b_ref, at):
    n = low.shape[0]
    a_ref[at : at + n, :] = jnp.where(even, high, low)
    b_ref[at : at + n, :] = jnp.where(even, low, high)


def flags_of(g, flags):
    ix, iy = flags[0], flags[1]
    return ((ix % 2) == 0, ix == 0, ix == g.px - 1), ((iy % 2) == 0, iy == 0, iy == g.py - 1)


def split2(v):
    high = v.astype(BF16)
    low = (v - high.astype(F32)).astype(BF16)
    return jnp.concatenate([high, low], axis=1)


def bounds_of(zones, z, zlow, zhigh):
    low = jnp.full(z.shape, zlow[0], F32)
    high = jnp.full(z.shape, zhigh[0], F32)
    for i in range(1, zones):
        hit = z == i
        low = jnp.where(hit, zlow[i], low)
        high = jnp.where(hit, zhigh[i], high)
    return low, high


def first_kernel(g, flags, rho, sigma, zone, t, own, xa, xb, rims, zrims, sig_v, t_v, sems):
    (even, _, _), _ = flags_of(g, flags)
    step = 8
    small = []
    for k, at in enumerate((0, g.nx - 2)):
        small.append(pltpu.make_async_copy(rho.at[pl.ds(at, 2)], rims.at[k, 0], sems.at[2 * k]))
        small.append(pltpu.make_async_copy(zone.at[pl.ds(at, 2)], zrims.at[k], sems.at[2 * k + 1]))
    big = []
    for c in range(g.nx // step):
        at = pl.ds(c * step, step)
        big.append((
            pltpu.make_async_copy(sigma.at[at], sig_v.at[at], sems.at[4 + 2 * c]),
            pltpu.make_async_copy(t.at[at], t_v.at[at], sems.at[5 + 2 * c]),
        ))
    for a, b in big:
        a.start()
        b.start()
    for copy in small:
        copy.start()
    zero = jnp.zeros((g.ny, g.nz), F32)
    run, total, seen = zero, zero, zero
    for c, (a, b) in enumerate(big):
        a.wait()
        b.wait()
        for k in range(step):
            run = run + sig_v[c * step + k]
            total = total + run
            seen = seen + t_v[c * step + k]
    own[0 : g.ny, :] = run
    own[g.ny : 2 * g.ny, :] = total - seen * (1.0 / g.xs)
    for copy in small:
        copy.wait()
    at = 0
    for r in range(2):
        put_pair(even, rims[0, 0, r], rims[1, 0, r], xa, xb, at)
        at += g.ny
    for r in range(2):
        put_pair(even, sig_v[r], sig_v[g.nx - 2 + r], xa, xb, at)
        at += g.ny
    for r in range(2):
        put_pair(even, zrims[0, r].astype(F32), zrims[1, r].astype(F32), xa, xb, at)
        at += g.ny
    xa[at : at + g.ny, :] = run
    xa[at + g.ny : at + 2 * g.ny, :] = total - seen * (1.0 / g.xs)


def bounds_kernel(g, zones, zlow, zhigh, zone, t, low_o, high_o, t_o):
    def body(x, carry):
        low_o[x], high_o[x] = bounds_of(zones, zone[x], zlow, zhigh)
        t_o[x] = t[x] * (1.0 / g.xs)
        return carry

    lax.fori_loop(0, g.nx, body, 0, unroll=8)


def spread_kernel(g, p, q, p_o, table, ztable):
    nz = g.nz
    row = lax.broadcasted_iota(jnp.int32, (2 * nz, 2 * nz), 0) % nz
    col = lax.broadcasted_iota(jnp.int32, (2 * nz, 2 * nz), 1)
    first = (row <= col).astype(F32)
    second = (nz - jnp.maximum(row, col - nz)).astype(F32) * (SCALE / nz)
    table[...] = jnp.where(col < nz, first, second).astype(BF16)
    r2 = lax.broadcasted_iota(jnp.int32, (2 * nz, nz), 0) % nz
    c2 = lax.broadcasted_iota(jnp.int32, (2 * nz, nz), 1)
    back = (r2 >= c2).astype(F32).astype(BF16)
    ztable[...] = ((r2 == c2 + 1).astype(F32) - (r2 == c2 - 1).astype(F32)).astype(BF16)
    step = 16

    def body(c, carry):
        here = pl.ds(c * step, step)
        values = p[here]
        p_o[here] = values * (1.0 / g.zs)
        out = jnp.dot(split2(values.reshape(step * g.ny, nz)), back, preferred_element_type=F32) * (g.zs * SCALE)
        q[here] = out.reshape(step, g.ny, nz)
        return carry

    lax.fori_loop(0, g.nx // step, body, 0, unroll=True)


def join_kernel(g, flags, xa, own, head, pair, sums):
    (even, _, _), _ = flags_of(g, flags)
    ny = g.ny
    at = 4 * ny
    join_pair(g, even, own, xa, at, pair)
    n = sums.shape[0] // CHUNK
    sums[...] = jnp.zeros(sums.shape, F32)
    sums[pl.ds(0, n, stride=CHUNK), :] = jnp.broadcast_to(head[0:1, :], (n, g.nz))
    for k, (dx, dy) in enumerate(DIAGONALS):
        ok, there = diagonal(g, flags, dx, dy)

        @pl.when(ok)
        def _():
            for f in range(2):
                sums[pl.ds(there * CHUNK + 1 + f, 1), :] = head[8 + 2 * k + f : 9 + 2 * k + f, :]


def diagonal(g, flags, dx, dy):
    ix, iy = flags[0] + dx, flags[1] + dy
    ok = jnp.logical_and(jnp.logical_and(ix >= 0, ix < g.px), jnp.logical_and(iy >= 0, iy < g.py))
    return ok, jnp.where(ok, ix * g.py + iy, 0)


def join_pair(g, even, own, xa, at, pair):
    ny = g.ny
    mine_t, mine_s = own[0:ny, :], own[ny : 2 * ny, :]
    other_t, other_s = xa[at : at + ny, :], xa[at + ny : at + 2 * ny, :]
    pair[0:ny, :] = mine_t + other_t
    pair[ny : 2 * ny, :] = mine_s + other_s + jnp.where(even, mine_t, other_t) * float(g.nx)


def sides_kernel(g, fields, flags, xa, xb, own, order, *refs):
    blocks, (ya, yb, pair) = refs[:fields], refs[fields:]
    (xeven, xfirst, xlast), (yeven, _, _) = flags_of(g, flags)
    n = g.xp
    for f in range(fields):
        for r in range(2):
            low = blocks[f][pl.ds(r, g.nx, stride=g.ny), :].astype(F32)
            high = blocks[f][pl.ds(g.ny - 2 + r, g.nx, stride=g.ny), :].astype(F32)
            put_pair(yeven, low, high, ya, yb, (f * 2 + r) * n + XO)
    for f in range(fields):
        for px in range(2):
            at = (f * 2 + px) * g.ny
            sides = pick_sides(xeven, xfirst, xlast, xa[at : at + g.ny, :], xb[at : at + g.ny, :])
            for plane, value in zip((px, XO + g.nx + px), sides):
                for r in range(2):
                    spot = (f * 2 + r) * n + plane
                    put_pair(yeven, value[r : r + 1], value[g.ny - 2 + r : g.ny - 1 + r], ya, yb, spot)
    join_pair(g, xeven, own, xa, fields * 2 * g.ny, pair)


def halo_slots(g, n, off):
    xs = []
    for r in range(2):
        xs.append((r * g.ny, pl.ds(r * g.pl + YO, g.ny), pl.ds((XO + g.nx + r) * g.pl + YO, g.ny)))
    ys = []
    for r in range(2):
        first = off * g.pl + r
        ys.append((r * n, pl.ds(first + YO - 2, n, stride=g.pl), pl.ds(first + YO + g.ny, n, stride=g.pl)))
    return xs, ys


def halo_values(g, flags, field, xa, xb, ya, yb, yn, off):
    (xeven, xfirst, xlast), (yeven, yfirst, ylast) = flags_of(g, flags)
    xs, ys = halo_slots(g, yn, off)
    for axis, slots, n, a, b, even, first, last in (
        (0, xs, g.ny, xa, xb, xeven, xfirst, xlast),
        (1, ys, yn, ya, yb, yeven, yfirst, ylast),
    ):
        for at, low_rows, high_rows in slots:
            here = pl.ds(field * 2 * n + at, n)
            low, high = pick_sides(even, first, last, a[here, :], b[here, :])
            yield axis, 0, at, low_rows, low
            yield axis, 1, at, high_rows, high


def lane_value(row, lane):
    ids = lax.broadcasted_iota(jnp.int32, row.shape, 1)
    return jnp.sum(jnp.where(ids == lane, row, 0.0), axis=1, keepdims=True)


def sum_row(g, sums):
    n = g.px * g.py
    return jnp.sum(sums[pl.ds(0, n, stride=sums.shape[0] // n), :], axis=0, keepdims=True)


def alphas(g, sums):
    row = sum_row(g, sums)
    return tuple(
        ETA / SCALE * lax.rsqrt(lane_value(row, k) * (1.0 / (g.cells * SCALE * SCALE)) + EPSILON) for k in range(2)
    )


def ray_offsets(g, flags, trs):
    ix = flags[0]
    q = ix // 2
    even = (ix % 2) == 0
    ny = g.ny
    mine, other = trs[0, 0:ny, :], trs[1, 0:ny, :]
    reach = float(g.nx)
    before = jnp.where(even, 0.0, other)
    sums = jnp.zeros_like(mine)
    spread = (mine + other) * (g.pairs - 1 - q).astype(F32)
    for m in range(1, g.pairs):
        p = q ^ m
        total = trs[1 + m, 0:ny, :]
        before = before + jnp.where(p < q, total, 0.0)
        sums = sums + jnp.where(p > q, trs[1 + m, ny : 2 * ny, :], 0.0)
        spread = spread + total * (g.pairs - 1 - jnp.maximum(p, q)).astype(F32)
    near = jnp.where(even, trs[1, ny : 2 * ny, :] + (before + mine) * reach, 0.0)
    return before, near + sums + spread * (2.0 * reach)


def cross(a, b):
    return a[1] * b[2] - a[2] * b[1], a[2] * b[0] - a[0] * b[2], a[0] * b[1] - a[1] * b[0]


def step_core(g, flags, update, rho_e, sig_e, trs, p, q, t, table, ztable, outs, scratch):
    grho, gsig, sums, own, xa, xb, ya, yb = outs
    vxr, vxs, vyr, vys, vzr, vzs, rt_s, az, bz, yu, ym = scratch
    nx, ny, nz, w = g.nx, g.ny, g.nz, g.pl
    (even, _, _), (yeven, _, _) = flags_of(g, flags)
    zero = jnp.zeros((ny, nz), F32)
    zero8 = jnp.zeros((8, nz), F32)
    before, after = ray_offsets(g, flags, trs)
    step = STEP
    rows = step * ny
    ext = ((rho_e, az), (sig_e, bz))

    def span(start, size, tile=8):
        return pl.ds(start if isinstance(start, int) or tile == 1 else pl.multiple_of(start, tile), size)

    def plane(x):
        return span((x + 1) * ny, ny)

    def zdiff(v):
        return jnp.dot(split2(v), ztable[...], preferred_element_type=F32)

    def slopes(ref, z, x):
        at = g.own(x)
        sx = ref[pl.ds(at + w, ny), :] - ref[pl.ds(at - w, ny), :]
        sy = ref[pl.ds(at + 1, ny), :] - ref[pl.ds(at - 1, ny), :]
        return sx, sy, z[plane(x), :]

    def cross_plane(x, acc, inside):
        a = slopes(*ext[0], x)
        b = slopes(*ext[1], x)
        c = cross(a, b)
        vxr[plane(x), :] = b[1] * c[2] - b[2] * c[1]
        vxs[plane(x), :] = c[1] * a[2] - c[2] * a[1]
        if not inside:
            return acc
        at = pl.ds(g.own(x), ny)
        vyr[at, :] = b[2] * c[0] - b[0] * c[2]
        vys[at, :] = c[2] * a[0] - c[0] * a[2]
        vzr[plane(x), :] = b[0] * c[1] - b[1] * c[0]
        vzs[plane(x), :] = c[0] * a[1] - c[1] * a[0]
        return acc + fold8(c[0] * c[0] + c[1] * c[1] + c[2] * c[2])

    def fields_chunk(c, carry):
        run, acc = carry
        values = ([], [])
        for k in range(step):
            x = c * step + k
            at = pl.ds(g.own(x), ny)
            rho, sig = update(x, at)
            rho_e[at, :] = rho
            sig_e[at, :] = sig
            values[0].append(rho)
            values[1].append(sig)
            run = run + sig
            miss = run - t[x]
            rt_s[span(x * ny, ny), :] = miss
            acc = acc + fold8(miss * miss)
        at = span(c * rows + ny, rows)
        pieces = split2(jnp.concatenate(values[0] + values[1], axis=0))
        y = jnp.dot(pieces[:rows], table[...], preferred_element_type=F32)
        yu[at, :] = y[:, :nz]
        ym[at, :] = y[:, nz:]
        z = jnp.dot(pieces, ztable[...], preferred_element_type=F32)
        az[at, :] = z[:rows]
        bz[at, :] = z[rows:]
        return run, acc

    chunks = nx // step
    _, acc_t = lax.fori_loop(0, chunks, fields_chunk, (before, zero8), unroll=UNROLL_FIELDS)

    lines = (-1, ny)
    line = lambda ref, x, y: ref[pl.ds((XO + x) * w + YO + y, nx, stride=w), :]
    flat = lambda ref, x: ref[g.own(x) : g.own(x) + ny, :]
    pieces = [line(ref, 0, y) for ref, _ in ext for y in lines] + [flat(ref, x) for ref, _ in ext for x in (-1, nx)]
    deep = zdiff(jnp.concatenate(pieces, axis=0))
    for k, y in enumerate(lines):
        fields = []
        for f, (ref, _) in enumerate(ext):
            at = (2 * f + k) * nx
            fields.append((line(ref, 1, y) - line(ref, -1, y), line(ref, 0, y + 1) - line(ref, 0, y - 1), deep[at : at + nx]))
        a, b = fields
        c = cross(a, b)
        spot = pl.ds(XO * w + YO + y, nx, stride=w)
        vyr[spot, :] = b[2] * c[0] - b[0] * c[2]
        vys[spot, :] = c[2] * a[0] - c[0] * a[2]
    base = 4 * nx
    for k, x in enumerate((-1, nx)):
        for f, (_, z) in enumerate(ext):
            at = base + (2 * f + k) * ny
            z[plane(x), :] = deep[at : at + ny]

    def gradient_plane(x, carry):
        back, sum_t, sum_r, nr, ns, acc = carry
        at = g.own(x)
        here = plane(x)
        flat_at = span(x * ny, ny)

        def term(vx, vy, vz):
            along_x = vx[plane(x - 1), :] - vx[plane(x + 1), :]
            along_y = vy[pl.ds(at - 1, ny), :] - vy[pl.ds(at + 1, ny), :]
            return along_x + along_y - vz[here, :]

        back = back + rt_s[flat_at, :]
        miss = yu[here, :] - p[x]
        gr = ym[here, :] - q[x] + term(vxr, vyr, vzr)
        gs = back * (SCALE * g.xs * g.xs) + term(vxs, vys, vzs)
        grho[flat_at, :] = gr
        gsig[flat_at, :] = gs
        sum_t = sum_t + gs
        return back, sum_t, sum_r + sum_t, nr + fold8(gr * gr), ns + fold8(gs * gs), acc + fold8(miss * miss)

    def crosses(c, acc):
        for k in range(step):
            acc = cross_plane(c * step + step - 1 - k, acc, True)
        return acc

    def adjoint(c):
        at = span(c * rows + ny, rows)
        z = zdiff(jnp.concatenate([vzr[at, :], vzs[at, :]], axis=0))
        vzr[at, :] = z[:rows]
        vzs[at, :] = z[rows:]

    def gradients(c, carry):
        for k in range(step):
            carry = gradient_plane(c * step + step - 1 - k, carry)
        return carry

    carry = (after, zero, zero, zero8, zero8, zero8)
    cross_plane(-1, None, False)
    cross_plane(nx, None, False)
    acc_c = crosses(chunks - 1, zero8)
    acc_c = crosses(chunks - 2, acc_c)
    adjoint(chunks - 1)

    def main(i, carry):
        c = chunks - 3 - i
        acc = crosses(c, carry[0])
        adjoint(c + 1)
        return acc, gradients(c + 2, carry[1])

    acc_c, carry = lax.fori_loop(0, chunks - 2, main, (acc_c, carry), unroll=UNROLL_MAIN)
    adjoint(0)
    carry = gradients(1, carry)
    _, sum_t, sum_r, nr, ns, acc_p = gradients(0, carry)

    total = lambda v: jnp.sum(jnp.sum(v, axis=0, keepdims=True), axis=1, keepdims=True)
    spread = sums.shape[0] if own is None else 8
    lane = lax.broadcasted_iota(jnp.int32, (spread, nz), 1)
    obj = acc_t * (g.xs * g.xs) + acc_p * (g.zs * g.zs) + acc_c * (BETA / 16.0)
    sums[0:spread, :] = jnp.where(lane == 0, total(nr), jnp.where(lane == 1, total(ns), jnp.where(lane == 2, total(obj), 0.0)))
    if own is not None:
        rest = sum_t * (nx + 1.0) - sum_r
        pos = 0
        for block in (grho, gsig):
            for r in range(2):
                put_pair(even, block[pl.ds(r * ny, ny), :], block[pl.ds((nx - 2 + r) * ny, ny), :], xa, xb, pos)
                pos += ny
        for ref, at in ((own, 0), (xa, pos)):
            ref[at : at + ny, :] = sum_t
            ref[at + ny : at + 2 * ny, :] = rest
        for f, block in enumerate((grho, gsig)):
            for r in range(2):
                rows_low = block[pl.ds(r, nx, stride=ny), :]
                rows_high = block[pl.ds(ny - 2 + r, nx, stride=ny), :]
                put_pair(yeven, rows_low, rows_high, ya, yb, (f * 2 + r) * nx)
            for k, (dx, dy) in enumerate(DIAGONALS):
                cell = (0 if dx < 0 else nx - 1) * ny + (0 if dy < 0 else ny - 1)
                sums[8 + 2 * k + f : 9 + 2 * k + f, :] = block[cell : cell + 1, :]


def opening_step(g, zones, flags, zlow, zhigh, xa, xb, ya, yb, own, rho, sig, p, q, t, table, ztable, *refs):
    others, rest = refs[: g.pairs - 1], refs[g.pairs - 1 :]
    rho_e, sig_e, trs, xlow, xhigh, ylow, yhigh = rest[:7]
    ny = g.ny
    for f, ext in ((0, rho_e), (1, sig_e)):
        for axis, side, at, spot, value in halo_values(g, flags, f, xa, xb, ya, yb, g.xp, 0):
            ext[spot, :] = value
    for axis, side, at, spot, value in halo_values(g, flags, 2, xa, xb, ya, yb, g.xp, 0):
        low, high = bounds_of(zones, value, zlow, zhigh)
        lows, highs = ((xlow, xhigh), (ylow, yhigh))[axis]
        lows[side, pl.ds(at, value.shape[0]), :] = low
        highs[side, pl.ds(at, value.shape[0]), :] = high
    pos = 6 * ny
    trs[0] = own[...]
    trs[1] = xa[pos : pos + 2 * ny, :]
    for m, other in enumerate(others):
        trs[2 + m] = other[...]
    step_core(g, flags, lambda x, at: (rho[x], sig[x]), rho_e, sig_e, trs, p, q, t, table, ztable, rest[7:15], rest[15:])


def later_step(g, last, flags, xa, xb, ya, yb, sums_i, own_i, grho_i, gsig_i, rho_i, sig_i, low, high,
               xlow, xhigh, ylow, yhigh, trs_i, p, q, t, table, ztable, *refs):
    others, rest = refs[: g.pairs - 1], refs[g.pairs - 1 :]
    rho_e, sig_e, trs = rest[:3]
    ny = g.ny
    ar, asig = alphas(g, sums_i)
    clip = lambda v, lows, highs: jnp.minimum(jnp.maximum(v, lows), highs)
    for axis, side, at, spot, value in halo_values(g, flags, 0, xa, xb, ya, yb, g.nx, XO):
        lows, highs = ((xlow, xhigh), (ylow, yhigh))[axis]
        if axis == 1:
            at = at // g.nx * g.xp + XO
        here = pl.ds(at, value.shape[0])
        rho_e[spot, :] = clip(rho_i[spot, :] - ar * value, lows[side, here, :], highs[side, here, :])
    for axis, side, at, spot, value in halo_values(g, flags, 1, xa, xb, ya, yb, g.nx, XO):
        sig_e[spot, :] = sig_i[spot, :] - asig * value
    for dx, dy in DIAGONALS:
        ok, there = diagonal(g, flags, dx, dy)
        plane = XO - 1 if dx < 0 else XO + g.nx
        side = 0 if dy < 0 else 1
        here = pl.ds((1 - side) * g.xp + plane, 1)
        spot = pl.ds(plane * g.pl + (YO - 1 if dy < 0 else YO + ny), 1)
        value = jnp.where(ok, sums_i[pl.ds(there * CHUNK + 1, 1), :], 0.0)
        rho_e[spot, :] = clip(rho_i[spot, :] - ar * value, ylow[side, here, :], yhigh[side, here, :])
        value = jnp.where(ok, sums_i[pl.ds(there * CHUNK + 2, 1), :], 0.0)
        sig_e[spot, :] = sig_i[spot, :] - asig * value
    pos = 4 * ny
    trs[0] = trs_i[0] - asig * own_i[...]
    trs[1] = trs_i[1] - asig * xa[pos : pos + 2 * ny, :]
    for m, other in enumerate(others):
        trs[2 + m] = trs_i[2 + m] - asig * other[...]

    def update(x, at):
        here = pl.ds(pl.multiple_of(x * ny, 8), ny)
        moved = rho_i[at, :] - ar * grho_i[here, :]
        return clip(moved, low[x], high[x]), sig_i[at, :] - asig * gsig_i[here, :]

    if last:
        outs, scratch = (*rest[3:6], None, None, None, None, None), rest[6:]
    else:
        outs, scratch = rest[3:11], rest[11:]
    step_core(g, flags, update, rho_e, sig_e, trs, p, q, t, table, ztable, outs, scratch)


def closing_kernel(g, sums0, sums1, sums2, grho, gsig, rho_e, sig_e, low, high, rho_o, sig_o, obj, rho_v, sig_v, sems):
    ar, asig = alphas(g, sums2)
    step = 8
    copies = []
    for c in range(g.nx // step):

        def body(k, carry):
            x = c * step + k
            at = pl.ds(g.own(x), g.ny)
            here = pl.ds(pl.multiple_of(x * g.ny, 8), g.ny)
            rho_v[x] = jnp.minimum(jnp.maximum(rho_e[at, :] - ar * grho[here, :], low[x]), high[x])
            sig_v[x] = sig_e[at, :] - asig * gsig[here, :]
            return carry

        lax.fori_loop(0, step, body, 0, unroll=True)
        here = pl.ds(c * step, step)
        for k, (v, o) in enumerate(((rho_v, rho_o), (sig_v, sig_o))):
            copies.append(pltpu.make_async_copy(v.at[here], o.at[here], sems.at[2 * c + k]))
            copies[-1].start()
    for k, sums in enumerate((sums0, sums1, sums2)):
        row = sum_row(g, sums)
        lane = lax.broadcasted_iota(jnp.int32, row.shape, 1)
        obj[k] = jnp.sum(jnp.where(lane == 2, row, 0.0)) * (0.5 / g.cells)
    for copy in copies:
        copy.wait()


def pairs_of(size):
    a = [(i, i ^ 1) for i in range(size)]
    b = [(i, i if i in (0, size - 1) else ((i + 1) ^ 1) - 1) for i in range(size)]
    return a, b


def exchange(axis, a, b):
    pa, pb = pairs_of(lax.axis_size(axis))
    a = lax.ppermute(a, axis, pa)
    b = lax.ppermute(b, axis, pb)
    return a, b


def pair_totals(pair, size):
    out = []
    for m in range(1, size // 2):
        out.append(lax.ppermute(pair, "gx", [(i, i ^ (2 * m)) for i in range(size)]))
    return out


SMEM = pl.BlockSpec(memory_space=pltpu.SMEM)
VMEM = pl.BlockSpec(memory_space=pltpu.VMEM)
HBM = pl.BlockSpec(memory_space=pltpu.HBM)


def call(body, shapes, specs, args, scratch=(), limit=12, outs=None):
    return pl.pallas_call(
        body,
        out_shape=[jax.ShapeDtypeStruct(s, d) for s, d in shapes],
        in_specs=specs,
        out_specs=outs or [VMEM] * len(shapes),
        scratch_shapes=list(scratch),
        compiler_params=pltpu.CompilerParams(vmem_limit_bytes=limit * 1024 * 1024),
    )(*args)


def local(density, slowness, pressure_obs, time_obs, zone_map, zone_low, zone_high):
    nx, ny, nz = density.shape
    px, py = lax.axis_size("gx"), lax.axis_size("gy")
    g = Geo(nx, ny, nz, px, py)
    zones = zone_low.shape[0]
    both = ("gx", "gy")
    flags = jnp.stack([lax.axis_index("gx"), lax.axis_index("gy")]).astype(jnp.int32)

    ext = ((g.ext, nz), F32)
    own_shape = ((2 * ny, nz), F32)
    trs_shape = ((g.pairs + 1, 2 * ny, nz), F32)
    sums_shape = ((px * py, nz), F32)
    block = ((nx, ny, nz), F32)
    flat = ((nx * ny, nz), F32)
    xa_shape = lambda f: (((f + 1) * 2 * ny, nz), F32)
    xb_shape = lambda f: ((f * 2 * ny, nz), F32)
    ymsg = lambda f: ((f * 2 * g.xp, nz), F32)
    xbound = ((2, 2 * ny, nz), F32)
    ybound = ((2, 2 * g.xp, nz), F32)
    win = pltpu.VMEM((g.win, nz), F32)
    ext_v = pltpu.VMEM((g.ext, nz), F32)
    core_scratch = [win] * 2 + [ext_v] * 2 + [win] * 2 + [pltpu.VMEM((nx * ny, nz), F32)] + [win] * 4

    own, xa, xb = call(
        functools.partial(first_kernel, g), [own_shape, xa_shape(3), xb_shape(3)],
        [SMEM] + [HBM] * 4, (flags, *(pltpu.with_memory_space_constraint(v, pltpu.HBM) for v in (density, slowness, zone_map, time_obs))),
        [pltpu.VMEM((2, 1, 2, ny, nz), F32), pltpu.VMEM((2, 2, ny, nz), jnp.int32),
         pltpu.VMEM((nx, ny, nz), F32), pltpu.VMEM((nx, ny, nz), F32), pltpu.SemaphoreType.DMA((4 + nx // 4,))],
    )
    xa, xb = exchange("gx", xa, xb)
    low, high, t = call(
        functools.partial(bounds_kernel, g, zones), [block] * 3,
        [SMEM, SMEM] + [VMEM] * 2, (zone_low, zone_high, zone_map, time_obs),
    )
    q, p, table, ztable = call(
        functools.partial(spread_kernel, g),
        [block] * 2 + [((2 * nz, 2 * nz), BF16), ((2 * nz, nz), BF16)], [VMEM], (pressure_obs,),
    )
    as_rows = lambda v: v.reshape(nx * ny, nz)
    ya, yb, pair = call(
        functools.partial(sides_kernel, g, 3), [ymsg(3)] * 2 + [own_shape],
        [SMEM] + [VMEM] * 7, (flags, xa, xb, own, low, as_rows(density), as_rows(slowness), as_rows(zone_map)),
    )
    ya, yb = exchange("gy", ya, yb)
    others = pair_totals(pair, px)
    yown = ((4 * nx, nz), F32)
    ends = [flat, flat, ((16, nz), F32), own_shape, xa_shape(2), xb_shape(2), yown, yown]
    chunks = ((px * py * CHUNK, nz), F32)
    outs = call(
        functools.partial(opening_step, g, zones),
        [ext, ext, trs_shape, xbound, xbound, ybound, ybound] + ends,
        [SMEM] * 3 + [VMEM] * (12 + len(others)),
        (flags, zone_low, zone_high, xa, xb, ya, yb, own, density, slowness, p, q, t, table, ztable, *others),
        core_scratch, 24,
    )
    rho_e, sig_e, trs, xlow, xhigh, ylow, yhigh, grho, gsig, head, own, xa, xb, ya, yb = outs
    history = []
    for iteration in range(1, ITERS):
        last = iteration == ITERS - 1
        xa, xb = exchange("gx", xa, xb)
        ya, yb = exchange("gy", ya, yb)
        pair, sums = call(
            functools.partial(join_kernel, g), [own_shape, chunks], [SMEM] + [VMEM] * 3,
            (flags, xa, own, head),
        )
        others = pair_totals(pair, px)
        sums = lax.all_to_all(sums, both, 0, 0, tiled=True)
        history.append(sums)
        outs = call(
            functools.partial(later_step, g, last), [ext, ext, trs_shape] + ([flat, flat, sums_shape] if last else ends),
            [SMEM] + [VMEM] * (22 + len(others)),
            (flags, xa, xb, ya, yb, sums, own, grho, gsig, rho_e, sig_e, low, high, xlow, xhigh, ylow, yhigh, trs,
             p, q, t, table, ztable, *others),
            core_scratch, 24,
        )
        rho_e, sig_e, trs, grho, gsig, head = outs[:6]
        if not last:
            own, xa, xb, ya, yb = outs[6:]
    history.append(lax.all_to_all(head, both, 0, 0, tiled=True))
    rho, sigma, obj = call(
        functools.partial(closing_kernel, g), [block, block, ((ITERS,), F32)],
        [VMEM] * 9, (*history, grho, gsig, rho_e, sig_e, low, high),
        [pltpu.VMEM((nx, ny, nz), F32)] * 2 + [pltpu.SemaphoreType.DMA((nx // 4,))], outs=[HBM, HBM, SMEM],
    )
    return rho, sigma, obj


def solution(mesh):
    placed = (P("gx", "gy", None),) * 5 + (P(), P())
    return jax.shard_map(
        local,
        mesh=mesh,
        in_specs=placed,
        out_specs=(P("gx", "gy", None), P("gx", "gy", None), P()),
        check_vma=False,
    )
```

```python
import functools
import math

import jax
import jax.numpy as jnp
from jax import lax
from jax.experimental import pallas as pl
from jax.experimental.pallas import tpu as pltpu
from jax.sharding import PartitionSpec as P


ITERS = 3
BETA = 1.0
ETA = 0.5
EPSILON = 1e-06

XO = 2
YO = 8
CHUNK = 4
STEP = 16
UNROLL_FIELDS = 4
UNROLL_MAIN = 2
SCALE = 16.0 / BETA
DIAGONALS = ((-1, -1), (-1, 1), (1, -1), (1, 1))
F32 = jnp.float32
BF16 = jnp.bfloat16


class Geo:
    def __init__(self, nx, ny, nz, px, py):
        self.nx, self.ny, self.nz, self.px, self.py = nx, ny, nz, px, py
        self.pl = ny + YO
        self.ext = (nx + 9) * self.pl
        self.xp = nx + 8
        self.cells = float(nx * px * ny * py * nz)
        self.zs = 1.0 / math.sqrt(nz)
        self.xs = 1.0 / math.sqrt(nx * px)
        self.win = (nx + 2) * ny
        self.pairs = px // 2

    def own(self, x):
        return (x + XO) * self.pl + YO


def fold8(v):
    total = v[0:8]
    for i in range(8, v.shape[0], 8):
        total = total + v[i : i + 8]
    return total


def pick_sides(even, first, last, a, b):
    low = jnp.where(even, b, a)
    high = jnp.where(even, a, b)
    return jnp.where(first, 0.0, low), jnp.where(last, 0.0, high)


def put_pair(even, low, high, a_ref, b_ref, at):
    n = low.shape[0]
    a_ref[at : at + n, :] = jnp.where(even, high, low)
    b_ref[at : at + n, :] = jnp.where(even, low, high)


def flags_of(g, flags):
    ix, iy = flags[0], flags[1]
    return ((ix % 2) == 0, ix == 0, ix == g.px - 1), ((iy % 2) == 0, iy == 0, iy == g.py - 1)


def split2(v):
    high = v.astype(BF16)
    low = (v - high.astype(F32)).astype(BF16)
    return jnp.concatenate([high, low], axis=1)


def bounds_of(zones, z, zlow, zhigh):
    low = jnp.full(z.shape, zlow[0], F32)
    high = jnp.full(z.shape, zhigh[0], F32)
    for i in range(1, zones):
        hit = z == i
        low = jnp.where(hit, zlow[i], low)
        high = jnp.where(hit, zhigh[i], high)
    return low, high


def first_kernel(g, flags, rho, sigma, zone, t, own, xa, xb, rims, zrims, sig_v, t_v, sems):
    (even, _, _), _ = flags_of(g, flags)
    step = 8
    small = []
    for k, at in enumerate((0, g.nx - 2)):
        small.append(pltpu.make_async_copy(rho.at[pl.ds(at, 2)], rims.at[k, 0], sems.at[2 * k]))
        small.append(pltpu.make_async_copy(zone.at[pl.ds(at, 2)], zrims.at[k], sems.at[2 * k + 1]))
    big = []
    for c in range(g.nx // step):
        at = pl.ds(c * step, step)
        big.append((
            pltpu.make_async_copy(sigma.at[at], sig_v.at[at], sems.at[4 + 2 * c]),
            pltpu.make_async_copy(t.at[at], t_v.at[at], sems.at[5 + 2 * c]),
        ))
    for a, b in big:
        a.start()
        b.start()
    for copy in small:
        copy.start()
    zero = jnp.zeros((g.ny, g.nz), F32)
    run, total, seen = zero, zero, zero
    for c, (a, b) in enumerate(big):
        a.wait()
        b.wait()
        for k in range(step):
            run = run + sig_v[c * step + k]
            total = total + run
            seen = seen + t_v[c * step + k]
    own[0 : g.ny, :] = run
    own[g.ny : 2 * g.ny, :] = total - seen * (1.0 / g.xs)
    for copy in small:
        copy.wait()
    at = 0
    for r in range(2):
        put_pair(even, rims[0, 0, r], rims[1, 0, r], xa, xb, at)
        at += g.ny
    for r in range(2):
        put_pair(even, sig_v[r], sig_v[g.nx - 2 + r], xa, xb, at)
        at += g.ny
    for r in range(2):
        put_pair(even, zrims[0, r].astype(F32), zrims[1, r].astype(F32), xa, xb, at)
        at += g.ny
    xa[at : at + g.ny, :] = run
    xa[at + g.ny : at + 2 * g.ny, :] = total - seen * (1.0 / g.xs)


def bounds_kernel(g, zones, zlow, zhigh, zone, t, low_o, high_o, t_o):
    def body(x, carry):
        low_o[x], high_o[x] = bounds_of(zones, zone[x], zlow, zhigh)
        t_o[x] = t[x] * (1.0 / g.xs)
        return carry

    lax.fori_loop(0, g.nx, body, 0, unroll=8)


def spread_kernel(g, p, q, p_o, table, ztable):
    nz = g.nz
    row = lax.broadcasted_iota(jnp.int32, (2 * nz, 2 * nz), 0) % nz
    col = lax.broadcasted_iota(jnp.int32, (2 * nz, 2 * nz), 1)
    first = (row <= col).astype(F32)
    second = (nz - jnp.maximum(row, col - nz)).astype(F32) * (SCALE / nz)
    table[...] = jnp.where(col < nz, first, second).astype(BF16)
    r2 = lax.broadcasted_iota(jnp.int32, (2 * nz, nz), 0) % nz
    c2 = lax.broadcasted_iota(jnp.int32, (2 * nz, nz), 1)
    back = (r2 >= c2).astype(F32).astype(BF16)
    ztable[...] = ((r2 == c2 + 1).astype(F32) - (r2 == c2 - 1).astype(F32)).astype(BF16)
    step = 16

    def body(c, carry):
        here = pl.ds(c * step, step)
        values = p[here]
        p_o[here] = values * (1.0 / g.zs)
        out = jnp.dot(split2(values.reshape(step * g.ny, nz)), back, preferred_element_type=F32) * (g.zs * SCALE)
        q[here] = out.reshape(step, g.ny, nz)
        return carry

    lax.fori_loop(0, g.nx // step, body, 0, unroll=True)


def join_kernel(g, flags, xa, own, head, pair, sums):
    (even, _, _), _ = flags_of(g, flags)
    ny = g.ny
    at = 4 * ny
    join_pair(g, even, own, xa, at, pair)
    n = sums.shape[0] // CHUNK
    sums[...] = jnp.zeros(sums.shape, F32)
    sums[pl.ds(0, n, stride=CHUNK), :] = jnp.broadcast_to(head[0:1, :], (n, g.nz))
    for k, (dx, dy) in enumerate(DIAGONALS):
        ok, there = diagonal(g, flags, dx, dy)

        @pl.when(ok)
        def _():
            for f in range(2):
                sums[pl.ds(there * CHUNK + 1 + f, 1), :] = head[8 + 2 * k + f : 9 + 2 * k + f, :]


def diagonal(g, flags, dx, dy):
    ix, iy = flags[0] + dx, flags[1] + dy
    ok = jnp.logical_and(jnp.logical_and(ix >= 0, ix < g.px), jnp.logical_and(iy >= 0, iy < g.py))
    return ok, jnp.where(ok, ix * g.py + iy, 0)


def join_pair(g, even, own, xa, at, pair):
    ny = g.ny
    mine_t, mine_s = own[0:ny, :], own[ny : 2 * ny, :]
    other_t, other_s = xa[at : at + ny, :], xa[at + ny : at + 2 * ny, :]
    pair[0:ny, :] = mine_t + other_t
    pair[ny : 2 * ny, :] = mine_s + other_s + jnp.where(even, mine_t, other_t) * float(g.nx)


def sides_kernel(g, fields, flags, order, *refs):
    blocks, (ya, yb) = refs[:fields], refs[fields:]
    _, (even, _, _) = flags_of(g, flags)
    for f in range(fields):
        for r in range(2):
            low = blocks[f][pl.ds(r, g.nx, stride=g.ny), :].astype(F32)
            high = blocks[f][pl.ds(g.ny - 2 + r, g.nx, stride=g.ny), :].astype(F32)
            put_pair(even, low, high, ya, yb, (f * 2 + r) * g.nx)


def corners_kernel(g, fields, flags, xa, xb, own, order, ca, cb, pair):
    (even, first, last), (yeven, _, _) = flags_of(g, flags)
    ca[...] = jnp.zeros(ca.shape, F32)
    cb[...] = jnp.zeros(cb.shape, F32)
    for f in range(fields):
        for side, px in ((0, 1), (1, 0)):
            at = (f * 2 + px) * g.ny
            value = pick_sides(even, first, last, xa[at : at + g.ny, :], xb[at : at + g.ny, :])[side]
            put_pair(yeven, value[0:1], value[g.ny - 1 : g.ny], ca, cb, 2 * f + side)
    join_pair(g, even, own, xa, fields * 2 * g.ny, pair)


def halo_slots(g, n, off):
    xs = []
    for r in range(2):
        xs.append((r * g.ny, pl.ds(r * g.pl + YO, g.ny), pl.ds((XO + g.nx + r) * g.pl + YO, g.ny)))
    ys = []
    for r in range(2):
        first = off * g.pl + r
        ys.append((r * n, pl.ds(first + YO - 2, n, stride=g.pl), pl.ds(first + YO + g.ny, n, stride=g.pl)))
    return xs, ys


def halo_values(g, flags, field, xa, xb, ya, yb, yn, off):
    (xeven, xfirst, xlast), (yeven, yfirst, ylast) = flags_of(g, flags)
    xs, ys = halo_slots(g, yn, off)
    for axis, slots, n, a, b, even, first, last in (
        (0, xs, g.ny, xa, xb, xeven, xfirst, xlast),
        (1, ys, yn, ya, yb, yeven, yfirst, ylast),
    ):
        for at, low_rows, high_rows in slots:
            here = pl.ds(field * 2 * n + at, n)
            low, high = pick_sides(even, first, last, a[here, :], b[here, :])
            yield axis, 0, at, low_rows, low
            yield axis, 1, at, high_rows, high


def lane_value(row, lane):
    ids = lax.broadcasted_iota(jnp.int32, row.shape, 1)
    return jnp.sum(jnp.where(ids == lane, row, 0.0), axis=1, keepdims=True)


def sum_row(g, sums):
    n = g.px * g.py
    return jnp.sum(sums[pl.ds(0, n, stride=sums.shape[0] // n), :], axis=0, keepdims=True)


def alphas(g, sums):
    row = sum_row(g, sums)
    return tuple(
        ETA / SCALE * lax.rsqrt(lane_value(row, k) * (1.0 / (g.cells * SCALE * SCALE)) + EPSILON) for k in range(2)
    )


def ray_offsets(g, flags, trs):
    ix = flags[0]
    q = ix // 2
    even = (ix % 2) == 0
    ny = g.ny
    mine, other = trs[0, 0:ny, :], trs[1, 0:ny, :]
    reach = float(g.nx)
    before = jnp.where(even, 0.0, other)
    sums = jnp.zeros_like(mine)
    spread = (mine + other) * (g.pairs - 1 - q).astype(F32)
    for m in range(1, g.pairs):
        p = q ^ m
        total = trs[1 + m, 0:ny, :]
        before = before + jnp.where(p < q, total, 0.0)
        sums = sums + jnp.where(p > q, trs[1 + m, ny : 2 * ny, :], 0.0)
        spread = spread + total * (g.pairs - 1 - jnp.maximum(p, q)).astype(F32)
    near = jnp.where(even, trs[1, ny : 2 * ny, :] + (before + mine) * reach, 0.0)
    return before, near + sums + spread * (2.0 * reach)


def cross(a, b):
    return a[1] * b[2] - a[2] * b[1], a[2] * b[0] - a[0] * b[2], a[0] * b[1] - a[1] * b[0]


def step_core(g, flags, update, rho_e, sig_e, trs, p, q, t, table, ztable, outs, scratch):
    grho, gsig, sums, own, xa, xb, ya, yb = outs
    vxr, vxs, vyr, vys, vzr, vzs, rt_s, az, bz, yu, ym = scratch
    nx, ny, nz, w = g.nx, g.ny, g.nz, g.pl
    (even, _, _), (yeven, _, _) = flags_of(g, flags)
    zero = jnp.zeros((ny, nz), F32)
    zero8 = jnp.zeros((8, nz), F32)
    before, after = ray_offsets(g, flags, trs)
    step = STEP
    rows = step * ny
    ext = ((rho_e, az), (sig_e, bz))

    def span(start, size, tile=8):
        return pl.ds(start if isinstance(start, int) or tile == 1 else pl.multiple_of(start, tile), size)

    def plane(x):
        return span((x + 1) * ny, ny)

    def zdiff(v):
        return jnp.dot(split2(v), ztable[...], preferred_element_type=F32)

    def slopes(ref, z, x):
        at = g.own(x)
        sx = ref[pl.ds(at + w, ny), :] - ref[pl.ds(at - w, ny), :]
        sy = ref[pl.ds(at + 1, ny), :] - ref[pl.ds(at - 1, ny), :]
        return sx, sy, z[plane(x), :]

    def cross_plane(x, acc, inside):
        a = slopes(*ext[0], x)
        b = slopes(*ext[1], x)
        c = cross(a, b)
        vxr[plane(x), :] = b[1] * c[2] - b[2] * c[1]
        vxs[plane(x), :] = c[1] * a[2] - c[2] * a[1]
        if not inside:
            return acc
        at = pl.ds(g.own(x), ny)
        vyr[at, :] = b[2] * c[0] - b[0] * c[2]
        vys[at, :] = c[2] * a[0] - c[0] * a[2]
        vzr[plane(x), :] = b[0] * c[1] - b[1] * c[0]
        vzs[plane(x), :] = c[0] * a[1] - c[1] * a[0]
        return acc + fold8(c[0] * c[0] + c[1] * c[1] + c[2] * c[2])

    def fields_chunk(c, carry):
        run, acc = carry
        values = ([], [])
        for k in range(step):
            x = c * step + k
            at = pl.ds(g.own(x), ny)
            rho, sig = update(x, at)
            rho_e[at, :] = rho
            sig_e[at, :] = sig
            values[0].append(rho)
            values[1].append(sig)
            run = run + sig
            miss = run - t[x]
            rt_s[span(x * ny, ny), :] = miss
            acc = acc + fold8(miss * miss)
        at = span(c * rows + ny, rows)
        pieces = split2(jnp.concatenate(values[0] + values[1], axis=0))
        y = jnp.dot(pieces[:rows], table[...], preferred_element_type=F32)
        yu[at, :] = y[:, :nz]
        ym[at, :] = y[:, nz:]
        z = jnp.dot(pieces, ztable[...], preferred_element_type=F32)
        az[at, :] = z[:rows]
        bz[at, :] = z[rows:]
        return run, acc

    chunks = nx // step
    _, acc_t = lax.fori_loop(0, chunks, fields_chunk, (before, zero8), unroll=UNROLL_FIELDS)

    lines = (-1, ny)
    line = lambda ref, x, y: ref[pl.ds((XO + x) * w + YO + y, nx, stride=w), :]
    flat = lambda ref, x: ref[g.own(x) : g.own(x) + ny, :]
    pieces = [line(ref, 0, y) for ref, _ in ext for y in lines] + [flat(ref, x) for ref, _ in ext for x in (-1, nx)]
    deep = zdiff(jnp.concatenate(pieces, axis=0))
    for k, y in enumerate(lines):
        fields = []
        for f, (ref, _) in enumerate(ext):
            at = (2 * f + k) * nx
            fields.append((line(ref, 1, y) - line(ref, -1, y), line(ref, 0, y + 1) - line(ref, 0, y - 1), deep[at : at + nx]))
        a, b = fields
        c = cross(a, b)
        spot = pl.ds(XO * w + YO + y, nx, stride=w)
        vyr[spot, :] = b[2] * c[0] - b[0] * c[2]
        vys[spot, :] = c[2] * a[0] - c[0] * a[2]
    base = 4 * nx
    for k, x in enumerate((-1, nx)):
        for f, (_, z) in enumerate(ext):
            at = base + (2 * f + k) * ny
            z[plane(x), :] = deep[at : at + ny]

    def gradient_plane(x, carry):
        back, sum_t, sum_r, nr, ns, acc = carry
        at = g.own(x)
        here = plane(x)
        flat_at = span(x * ny, ny)

        def term(vx, vy, vz):
            along_x = vx[plane(x - 1), :] - vx[plane(x + 1), :]
            along_y = vy[pl.ds(at - 1, ny), :] - vy[pl.ds(at + 1, ny), :]
            return along_x + along_y - vz[here, :]

        back = back + rt_s[flat_at, :]
        miss = yu[here, :] - p[x]
        gr = ym[here, :] - q[x] + term(vxr, vyr, vzr)
        gs = back * (SCALE * g.xs * g.xs) + term(vxs, vys, vzs)
        grho[flat_at, :] = gr
        gsig[flat_at, :] = gs
        sum_t = sum_t + gs
        return back, sum_t, sum_r + sum_t, nr + fold8(gr * gr), ns + fold8(gs * gs), acc + fold8(miss * miss)

    def crosses(c, acc):
        for k in range(step):
            acc = cross_plane(c * step + step - 1 - k, acc, True)
        return acc

    def adjoint(c):
        at = span(c * rows + ny, rows)
        z = zdiff(jnp.concatenate([vzr[at, :], vzs[at, :]], axis=0))
        vzr[at, :] = z[:rows]
        vzs[at, :] = z[rows:]

    def gradients(c, carry):
        for k in range(step):
            carry = gradient_plane(c * step + step - 1 - k, carry)
        return carry

    carry = (after, zero, zero, zero8, zero8, zero8)
    cross_plane(-1, None, False)
    cross_plane(nx, None, False)
    acc_c = crosses(chunks - 1, zero8)
    acc_c = crosses(chunks - 2, acc_c)
    adjoint(chunks - 1)

    def main(i, carry):
        c = chunks - 3 - i
        acc = crosses(c, carry[0])
        adjoint(c + 1)
        return acc, gradients(c + 2, carry[1])

    acc_c, carry = lax.fori_loop(0, chunks - 2, main, (acc_c, carry), unroll=UNROLL_MAIN)
    adjoint(0)
    carry = gradients(1, carry)
    _, sum_t, sum_r, nr, ns, acc_p = gradients(0, carry)

    total = lambda v: jnp.sum(jnp.sum(v, axis=0, keepdims=True), axis=1, keepdims=True)
    spread = sums.shape[0] if own is None else 8
    lane = lax.broadcasted_iota(jnp.int32, (spread, nz), 1)
    obj = acc_t * (g.xs * g.xs) + acc_p * (g.zs * g.zs) + acc_c * (BETA / 16.0)
    sums[0:spread, :] = jnp.where(lane == 0, total(nr), jnp.where(lane == 1, total(ns), jnp.where(lane == 2, total(obj), 0.0)))
    if own is not None:
        rest = sum_t * (nx + 1.0) - sum_r
        pos = 0
        for block in (grho, gsig):
            for r in range(2):
                put_pair(even, block[pl.ds(r * ny, ny), :], block[pl.ds((nx - 2 + r) * ny, ny), :], xa, xb, pos)
                pos += ny
        for ref, at in ((own, 0), (xa, pos)):
            ref[at : at + ny, :] = sum_t
            ref[at + ny : at + 2 * ny, :] = rest
        for f, block in enumerate((grho, gsig)):
            for r in range(2):
                rows_low = block[pl.ds(r, nx, stride=ny), :]
                rows_high = block[pl.ds(ny - 2 + r, nx, stride=ny), :]
                put_pair(yeven, rows_low, rows_high, ya, yb, (f * 2 + r) * nx)
            for k, (dx, dy) in enumerate(DIAGONALS):
                cell = (0 if dx < 0 else nx - 1) * ny + (0 if dy < 0 else ny - 1)
                sums[8 + 2 * k + f : 9 + 2 * k + f, :] = block[cell : cell + 1, :]


def opening_step(g, zones, flags, zlow, zhigh, xa, xb, ya, yb, ca, cb, own, rho, sig, p, q, t, table, ztable, *refs):
    others, rest = refs[: g.pairs - 1], refs[g.pairs - 1 :]
    rho_e, sig_e, trs, xlow, xhigh, ylow, yhigh = rest[:7]
    ny = g.ny
    _, (yeven, yfirst, ylast) = flags_of(g, flags)
    for f, ext in ((0, rho_e), (1, sig_e)):
        for axis, side, at, spot, value in halo_values(g, flags, f, xa, xb, ya, yb, g.nx, XO):
            ext[spot, :] = value
    for axis, side, at, spot, value in halo_values(g, flags, 2, xa, xb, ya, yb, g.nx, XO):
        low, high = bounds_of(zones, value, zlow, zhigh)
        lows, highs = ((xlow, xhigh), (ylow, yhigh))[axis]
        if axis == 1:
            at = at // g.nx * g.xp + XO
        lows[side, pl.ds(at, value.shape[0]), :] = low
        highs[side, pl.ds(at, value.shape[0]), :] = high
    cells = pick_sides(yeven, yfirst, ylast, ca[...], cb[...])
    limits = [bounds_of(zones, values, zlow, zhigh) for values in cells]
    for side, row in ((0, YO - 1), (1, YO + ny)):
        for k, plane in enumerate((XO - 1, XO + g.nx)):
            at = plane * g.pl + row
            rho_e[at : at + 1, :] = cells[side][k : k + 1]
            sig_e[at : at + 1, :] = cells[side][2 + k : 3 + k]
            at = (1 - side) * g.xp + plane
            ylow[side, at : at + 1, :] = limits[side][0][4 + k : 5 + k]
            yhigh[side, at : at + 1, :] = limits[side][1][4 + k : 5 + k]
    pos = 6 * ny
    trs[0] = own[...]
    trs[1] = xa[pos : pos + 2 * ny, :]
    for m, other in enumerate(others):
        trs[2 + m] = other[...]
    step_core(g, flags, lambda x, at: (rho[x], sig[x]), rho_e, sig_e, trs, p, q, t, table, ztable, rest[7:15], rest[15:])


def later_step(g, last, flags, xa, xb, ya, yb, sums_i, own_i, grho_i, gsig_i, rho_i, sig_i, low, high,
               xlow, xhigh, ylow, yhigh, trs_i, p, q, t, table, ztable, *refs):
    others, rest = refs[: g.pairs - 1], refs[g.pairs - 1 :]
    rho_e, sig_e, trs = rest[:3]
    ny = g.ny
    ar, asig = alphas(g, sums_i)
    clip = lambda v, lows, highs: jnp.minimum(jnp.maximum(v, lows), highs)
    for axis, side, at, spot, value in halo_values(g, flags, 0, xa, xb, ya, yb, g.nx, XO):
        lows, highs = ((xlow, xhigh), (ylow, yhigh))[axis]
        if axis == 1:
            at = at // g.nx * g.xp + XO
        here = pl.ds(at, value.shape[0])
        rho_e[spot, :] = clip(rho_i[spot, :] - ar * value, lows[side, here, :], highs[side, here, :])
    for axis, side, at, spot, value in halo_values(g, flags, 1, xa, xb, ya, yb, g.nx, XO):
        sig_e[spot, :] = sig_i[spot, :] - asig * value
    for dx, dy in DIAGONALS:
        ok, there = diagonal(g, flags, dx, dy)
        plane = XO - 1 if dx < 0 else XO + g.nx
        side = 0 if dy < 0 else 1
        here = pl.ds((1 - side) * g.xp + plane, 1)
        spot = pl.ds(plane * g.pl + (YO - 1 if dy < 0 else YO + ny), 1)
        value = jnp.where(ok, sums_i[pl.ds(there * CHUNK + 1, 1), :], 0.0)
        rho_e[spot, :] = clip(rho_i[spot, :] - ar * value, ylow[side, here, :], yhigh[side, here, :])
        value = jnp.where(ok, sums_i[pl.ds(there * CHUNK + 2, 1), :], 0.0)
        sig_e[spot, :] = sig_i[spot, :] - asig * value
    pos = 4 * ny
    trs[0] = trs_i[0] - asig * own_i[...]
    trs[1] = trs_i[1] - asig * xa[pos : pos + 2 * ny, :]
    for m, other in enumerate(others):
        trs[2 + m] = trs_i[2 + m] - asig * other[...]

    def update(x, at):
        here = pl.ds(pl.multiple_of(x * ny, 8), ny)
        moved = rho_i[at, :] - ar * grho_i[here, :]
        return clip(moved, low[x], high[x]), sig_i[at, :] - asig * gsig_i[here, :]

    if last:
        outs, scratch = (*rest[3:6], None, None, None, None, None), rest[6:]
    else:
        outs, scratch = rest[3:11], rest[11:]
    step_core(g, flags, update, rho_e, sig_e, trs, p, q, t, table, ztable, outs, scratch)


def closing_kernel(g, sums0, sums1, sums2, grho, gsig, rho_e, sig_e, low, high, rho_o, sig_o, obj):
    ar, asig = alphas(g, sums2)

    def body(x, carry):
        at = pl.ds(g.own(x), g.ny)
        here = pl.ds(pl.multiple_of(x * g.ny, 8), g.ny)
        rho_o[x] = jnp.minimum(jnp.maximum(rho_e[at, :] - ar * grho[here, :], low[x]), high[x])
        sig_o[x] = sig_e[at, :] - asig * gsig[here, :]
        return carry

    lax.fori_loop(0, g.nx, body, 0, unroll=8)
    for k, sums in enumerate((sums0, sums1, sums2)):
        row = sum_row(g, sums)
        lane = lax.broadcasted_iota(jnp.int32, row.shape, 1)
        obj[k] = jnp.sum(jnp.where(lane == 2, row, 0.0)) * (0.5 / g.cells)


def pairs_of(size):
    a = [(i, i ^ 1) for i in range(size)]
    b = [(i, i if i in (0, size - 1) else ((i + 1) ^ 1) - 1) for i in range(size)]
    return a, b


def exchange(axis, a, b):
    pa, pb = pairs_of(lax.axis_size(axis))
    a = lax.ppermute(a, axis, pa)
    b = lax.ppermute(b, axis, pb)
    return a, b


def pair_totals(pair, size):
    out = []
    for m in range(1, size // 2):
        out.append(lax.ppermute(pair, "gx", [(i, i ^ (2 * m)) for i in range(size)]))
    return out


SMEM = pl.BlockSpec(memory_space=pltpu.SMEM)
VMEM = pl.BlockSpec(memory_space=pltpu.VMEM)
HBM = pl.BlockSpec(memory_space=pltpu.HBM)


def call(body, shapes, specs, args, scratch=(), limit=12, outs=None):
    return pl.pallas_call(
        body,
        out_shape=[jax.ShapeDtypeStruct(s, d) for s, d in shapes],
        in_specs=specs,
        out_specs=outs or [VMEM] * len(shapes),
        scratch_shapes=list(scratch),
        compiler_params=pltpu.CompilerParams(vmem_limit_bytes=limit * 1024 * 1024),
    )(*args)


def local(density, slowness, pressure_obs, time_obs, zone_map, zone_low, zone_high):
    nx, ny, nz = density.shape
    px, py = lax.axis_size("gx"), lax.axis_size("gy")
    g = Geo(nx, ny, nz, px, py)
    zones = zone_low.shape[0]
    both = ("gx", "gy")
    flags = jnp.stack([lax.axis_index("gx"), lax.axis_index("gy")]).astype(jnp.int32)

    ext = ((g.ext, nz), F32)
    own_shape = ((2 * ny, nz), F32)
    trs_shape = ((g.pairs + 1, 2 * ny, nz), F32)
    sums_shape = ((px * py, nz), F32)
    block = ((nx, ny, nz), F32)
    flat = ((nx * ny, nz), F32)
    xa_shape = lambda f: (((f + 1) * 2 * ny, nz), F32)
    xb_shape = lambda f: ((f * 2 * ny, nz), F32)
    ymsg = lambda f: ((f * 2 * nx, nz), F32)
    xbound = ((2, 2 * ny, nz), F32)
    ybound = ((2, 2 * g.xp, nz), F32)
    win = pltpu.VMEM((g.win, nz), F32)
    ext_v = pltpu.VMEM((g.ext, nz), F32)
    core_scratch = [win] * 2 + [ext_v] * 2 + [win] * 2 + [pltpu.VMEM((nx * ny, nz), F32)] + [win] * 4

    own, xa, xb = call(
        functools.partial(first_kernel, g), [own_shape, xa_shape(3), xb_shape(3)],
        [SMEM] + [HBM] * 4, (flags, *(pltpu.with_memory_space_constraint(v, pltpu.HBM) for v in (density, slowness, zone_map, time_obs))),
        [pltpu.VMEM((2, 1, 2, ny, nz), F32), pltpu.VMEM((2, 2, ny, nz), jnp.int32),
         pltpu.VMEM((nx, ny, nz), F32), pltpu.VMEM((nx, ny, nz), F32), pltpu.SemaphoreType.DMA((4 + nx // 4,))],
    )
    xa, xb = exchange("gx", xa, xb)
    low, high, t = call(
        functools.partial(bounds_kernel, g, zones), [block] * 3,
        [SMEM, SMEM] + [VMEM] * 2, (zone_low, zone_high, zone_map, time_obs),
    )
    q, p, table, ztable = call(
        functools.partial(spread_kernel, g),
        [block] * 2 + [((2 * nz, 2 * nz), BF16), ((2 * nz, nz), BF16)], [VMEM], (pressure_obs,),
    )
    as_rows = lambda v: v.reshape(nx * ny, nz)
    ya, yb = call(
        functools.partial(sides_kernel, g, 3), [ymsg(3)] * 2,
        [SMEM] + [VMEM] * 4, (flags, own, as_rows(density), as_rows(slowness), as_rows(zone_map)),
    )
    ya, yb = exchange("gy", ya, yb)
    ca, cb, pair = call(
        functools.partial(corners_kernel, g, 3), [((8, nz), F32)] * 2 + [own_shape],
        [SMEM] + [VMEM] * 4, (flags, xa, xb, own, low),
    )
    ca, cb = exchange("gy", ca, cb)
    others = pair_totals(pair, px)
    ends = [flat, flat, ((16, nz), F32), own_shape, xa_shape(2), xb_shape(2), ymsg(2), ymsg(2)]
    chunks = ((px * py * CHUNK, nz), F32)
    outs = call(
        functools.partial(opening_step, g, zones),
        [ext, ext, trs_shape, xbound, xbound, ybound, ybound] + ends,
        [SMEM] * 3 + [VMEM] * (14 + len(others)),
        (flags, zone_low, zone_high, xa, xb, ya, yb, ca, cb, own, density, slowness, p, q, t, table, ztable, *others),
        core_scratch, 24,
    )
    rho_e, sig_e, trs, xlow, xhigh, ylow, yhigh, grho, gsig, head, own, xa, xb, ya, yb = outs
    history = []
    for iteration in range(1, ITERS):
        last = iteration == ITERS - 1
        xa, xb = exchange("gx", xa, xb)
        ya, yb = exchange("gy", ya, yb)
        pair, sums = call(
            functools.partial(join_kernel, g), [own_shape, chunks], [SMEM] + [VMEM] * 3,
            (flags, xa, own, head),
        )
        others = pair_totals(pair, px)
        sums = lax.all_to_all(sums, both, 0, 0, tiled=True)
        history.append(sums)
        outs = call(
            functools.partial(later_step, g, last), [ext, ext, trs_shape] + ([flat, flat, sums_shape] if last else ends),
            [SMEM] + [VMEM] * (22 + len(others)),
            (flags, xa, xb, ya, yb, sums, own, grho, gsig, rho_e, sig_e, low, high, xlow, xhigh, ylow, yhigh, trs,
             p, q, t, table, ztable, *others),
            core_scratch, 24,
        )
        rho_e, sig_e, trs, grho, gsig, head = outs[:6]
        if not last:
            own, xa, xb, ya, yb = outs[6:]
    history.append(lax.all_to_all(head, both, 0, 0, tiled=True))
    rho, sigma, obj = call(
        functools.partial(closing_kernel, g), [block, block, ((ITERS,), F32)],
        [VMEM] * 9, (*history, grho, gsig, rho_e, sig_e, low, high), outs=[VMEM, VMEM, SMEM],
    )
    return rho, sigma, obj


def solution(mesh):
    placed = (P("gx", "gy", None),) * 5 + (P(), P())
    return jax.shard_map(
        local,
        mesh=mesh,
        in_specs=placed,
        out_specs=(P("gx", "gy", None), P("gx", "gy", None), P()),
        check_vma=False,
    )
```

```python
import functools
import math

import jax
import jax.numpy as jnp
from jax import lax
from jax.experimental import pallas as pl
from jax.experimental.pallas import tpu as pltpu
from jax.sharding import PartitionSpec as P


ITERS = 3
BETA = 1.0
ETA = 0.5
EPSILON = 1e-06

XO = 2
YO = 8
CHUNK = 4
STEP = 16
UNROLL_FIELDS = 4
UNROLL_MAIN = 2
SCALE = 16.0 / BETA
DIAGONALS = ((-1, -1), (-1, 1), (1, -1), (1, 1))
F32 = jnp.float32
BF16 = jnp.bfloat16


class Geo:
    def __init__(self, nx, ny, nz, px, py):
        self.nx, self.ny, self.nz, self.px, self.py = nx, ny, nz, px, py
        self.pl = ny + YO + 1
        self.gp = ny + 1
        self.ext = (nx + 9) * self.pl
        self.xp = nx + 8
        self.cells = float(nx * px * ny * py * nz)
        self.zs = 1.0 / math.sqrt(nz)
        self.xs = 1.0 / math.sqrt(nx * px)
        self.win = (nx + 2) * ny
        self.pairs = px // 2

    def own(self, x):
        return (x + XO) * self.pl + YO


def fold8(v):
    total = v[0:8]
    for i in range(8, v.shape[0], 8):
        total = total + v[i : i + 8]
    return total


def pick_sides(even, first, last, a, b):
    low = jnp.where(even, b, a)
    high = jnp.where(even, a, b)
    return jnp.where(first, 0.0, low), jnp.where(last, 0.0, high)


def put_pair(even, low, high, a_ref, b_ref, at):
    n = low.shape[0]
    a_ref[at : at + n, :] = jnp.where(even, high, low)
    b_ref[at : at + n, :] = jnp.where(even, low, high)


def flags_of(g, flags):
    ix, iy = flags[0], flags[1]
    return ((ix % 2) == 0, ix == 0, ix == g.px - 1), ((iy % 2) == 0, iy == 0, iy == g.py - 1)


def split2(v):
    high = v.astype(BF16)
    low = (v - high.astype(F32)).astype(BF16)
    return jnp.concatenate([high, low], axis=1)


def bounds_of(zones, z, zlow, zhigh):
    low = jnp.full(z.shape, zlow[0], F32)
    high = jnp.full(z.shape, zhigh[0], F32)
    for i in range(1, zones):
        hit = z == i
        low = jnp.where(hit, zlow[i], low)
        high = jnp.where(hit, zhigh[i], high)
    return low, high


def first_kernel(g, flags, rho, sigma, zone, t, own, xa, xb, rims, zrims, sig_v, t_v, sems):
    (even, _, _), _ = flags_of(g, flags)
    step = 8
    small = []
    for k, at in enumerate((0, g.nx - 2)):
        small.append(pltpu.make_async_copy(rho.at[pl.ds(at, 2)], rims.at[k, 0], sems.at[2 * k]))
        small.append(pltpu.make_async_copy(zone.at[pl.ds(at, 2)], zrims.at[k], sems.at[2 * k + 1]))
    big = []
    for c in range(g.nx // step):
        at = pl.ds(c * step, step)
        big.append((
            pltpu.make_async_copy(sigma.at[at], sig_v.at[at], sems.at[4 + 2 * c]),
            pltpu.make_async_copy(t.at[at], t_v.at[at], sems.at[5 + 2 * c]),
        ))
    for a, b in big:
        a.start()
        b.start()
    for copy in small:
        copy.start()
    zero = jnp.zeros((g.ny, g.nz), F32)
    run, total, seen = zero, zero, zero
    for c, (a, b) in enumerate(big):
        a.wait()
        b.wait()
        for k in range(step):
            run = run + sig_v[c * step + k]
            total = total + run
            seen = seen + t_v[c * step + k]
    own[0 : g.ny, :] = run
    own[g.ny : 2 * g.ny, :] = total - seen * (1.0 / g.xs)
    for copy in small:
        copy.wait()
    at = 0
    for r in range(2):
        put_pair(even, rims[0, 0, r], rims[1, 0, r], xa, xb, at)
        at += g.ny
    for r in range(2):
        put_pair(even, sig_v[r], sig_v[g.nx - 2 + r], xa, xb, at)
        at += g.ny
    for r in range(2):
        put_pair(even, zrims[0, r].astype(F32), zrims[1, r].astype(F32), xa, xb, at)
        at += g.ny
    xa[at : at + g.ny, :] = run
    xa[at + g.ny : at + 2 * g.ny, :] = total - seen * (1.0 / g.xs)


def bounds_kernel(g, zones, zlow, zhigh, zone, t, low_o, high_o, t_o):
    def body(x, carry):
        low_o[x], high_o[x] = bounds_of(zones, zone[x], zlow, zhigh)
        t_o[x] = t[x] * (1.0 / g.xs)
        return carry

    lax.fori_loop(0, g.nx, body, 0, unroll=8)


def spread_kernel(g, p, q, p_o, table, ztable):
    nz = g.nz
    row = lax.broadcasted_iota(jnp.int32, (2 * nz, 2 * nz), 0) % nz
    col = lax.broadcasted_iota(jnp.int32, (2 * nz, 2 * nz), 1)
    first = (row <= col).astype(F32)
    second = (nz - jnp.maximum(row, col - nz)).astype(F32) * (SCALE / nz)
    table[...] = jnp.where(col < nz, first, second).astype(BF16)
    r2 = lax.broadcasted_iota(jnp.int32, (2 * nz, nz), 0) % nz
    c2 = lax.broadcasted_iota(jnp.int32, (2 * nz, nz), 1)
    back = (r2 >= c2).astype(F32).astype(BF16)
    ztable[...] = ((r2 == c2 + 1).astype(F32) - (r2 == c2 - 1).astype(F32)).astype(BF16)
    step = 16

    def body(c, carry):
        here = pl.ds(c * step, step)
        values = p[here]
        p_o[here] = values * (1.0 / g.zs)
        out = jnp.dot(split2(values.reshape(step * g.ny, nz)), back, preferred_element_type=F32) * (g.zs * SCALE)
        q[here] = out.reshape(step, g.ny, nz)
        return carry

    lax.fori_loop(0, g.nx // step, body, 0, unroll=True)


def join_kernel(g, flags, xa, own, head, pair, sums):
    (even, _, _), _ = flags_of(g, flags)
    ny = g.ny
    at = 4 * ny
    join_pair(g, even, own, xa, at, pair)
    n = sums.shape[0] // CHUNK
    sums[...] = jnp.zeros(sums.shape, F32)
    sums[pl.ds(0, n, stride=CHUNK), :] = jnp.broadcast_to(head[0:1, :], (n, g.nz))
    for k, (dx, dy) in enumerate(DIAGONALS):
        ok, there = diagonal(g, flags, dx, dy)

        @pl.when(ok)
        def _():
            for f in range(2):
                sums[pl.ds(there * CHUNK + 1 + f, 1), :] = head[8 + 2 * k + f : 9 + 2 * k + f, :]


def diagonal(g, flags, dx, dy):
    ix, iy = flags[0] + dx, flags[1] + dy
    ok = jnp.logical_and(jnp.logical_and(ix >= 0, ix < g.px), jnp.logical_and(iy >= 0, iy < g.py))
    return ok, jnp.where(ok, ix * g.py + iy, 0)


def join_pair(g, even, own, xa, at, pair):
    ny = g.ny
    mine_t, mine_s = own[0:ny, :], own[ny : 2 * ny, :]
    other_t, other_s = xa[at : at + ny, :], xa[at + ny : at + 2 * ny, :]
    pair[0:ny, :] = mine_t + other_t
    pair[ny : 2 * ny, :] = mine_s + other_s + jnp.where(even, mine_t, other_t) * float(g.nx)


def sides_kernel(g, fields, flags, order, *refs):
    blocks, (ya, yb) = refs[:fields], refs[fields:]
    _, (even, _, _) = flags_of(g, flags)
    for f in range(fields):
        for r in range(2):
            low = blocks[f][pl.ds(r, g.nx, stride=g.ny), :].astype(F32)
            high = blocks[f][pl.ds(g.ny - 2 + r, g.nx, stride=g.ny), :].astype(F32)
            put_pair(even, low, high, ya, yb, (f * 2 + r) * g.nx)


def corners_kernel(g, fields, flags, xa, xb, own, ca, cb, pair):
    (even, first, last), (yeven, _, _) = flags_of(g, flags)
    ca[...] = jnp.zeros(ca.shape, F32)
    cb[...] = jnp.zeros(cb.shape, F32)
    for f in range(fields):
        for side, px in ((0, 1), (1, 0)):
            at = (f * 2 + px) * g.ny
            value = pick_sides(even, first, last, xa[at : at + g.ny, :], xb[at : at + g.ny, :])[side]
            put_pair(yeven, value[0:1], value[g.ny - 1 : g.ny], ca, cb, 2 * f + side)
    join_pair(g, even, own, xa, fields * 2 * g.ny, pair)


def halo_slots(g, n, off):
    xs = []
    for r in range(2):
        xs.append((r * g.ny, pl.ds(r * g.pl + YO, g.ny), pl.ds((XO + g.nx + r) * g.pl + YO, g.ny)))
    ys = []
    for r in range(2):
        first = off * g.pl + r
        ys.append((r * n, pl.ds(first + YO - 2, n, stride=g.pl), pl.ds(first + YO + g.ny, n, stride=g.pl)))
    return xs, ys


def halo_values(g, flags, field, xa, xb, ya, yb, yn, off):
    (xeven, xfirst, xlast), (yeven, yfirst, ylast) = flags_of(g, flags)
    xs, ys = halo_slots(g, yn, off)
    for axis, slots, n, a, b, even, first, last in (
        (0, xs, g.ny, xa, xb, xeven, xfirst, xlast),
        (1, ys, yn, ya, yb, yeven, yfirst, ylast),
    ):
        for at, low_rows, high_rows in slots:
            here = pl.ds(field * 2 * n + at, n)
            low, high = pick_sides(even, first, last, a[here, :], b[here, :])
            yield axis, 0, at, low_rows, low
            yield axis, 1, at, high_rows, high


def lane_value(row, lane):
    ids = lax.broadcasted_iota(jnp.int32, row.shape, 1)
    return jnp.sum(jnp.where(ids == lane, row, 0.0), axis=1, keepdims=True)


def sum_row(g, sums):
    n = g.px * g.py
    return jnp.sum(sums[pl.ds(0, n, stride=sums.shape[0] // n), :], axis=0, keepdims=True)


def alphas(g, sums):
    row = sum_row(g, sums)
    return tuple(
        ETA / SCALE * lax.rsqrt(lane_value(row, k) * (1.0 / (g.cells * SCALE * SCALE)) + EPSILON) for k in range(2)
    )


def ray_offsets(g, flags, trs):
    ix = flags[0]
    q = ix // 2
    even = (ix % 2) == 0
    ny = g.ny
    mine, other = trs[0, 0:ny, :], trs[1, 0:ny, :]
    reach = float(g.nx)
    before = jnp.where(even, 0.0, other)
    sums = jnp.zeros_like(mine)
    spread = (mine + other) * (g.pairs - 1 - q).astype(F32)
    for m in range(1, g.pairs):
        p = q ^ m
        total = trs[1 + m, 0:ny, :]
        before = before + jnp.where(p < q, total, 0.0)
        sums = sums + jnp.where(p > q, trs[1 + m, ny : 2 * ny, :], 0.0)
        spread = spread + total * (g.pairs - 1 - jnp.maximum(p, q)).astype(F32)
    near = jnp.where(even, trs[1, ny : 2 * ny, :] + (before + mine) * reach, 0.0)
    return before, near + sums + spread * (2.0 * reach)


def cross(a, b):
    return a[1] * b[2] - a[2] * b[1], a[2] * b[0] - a[0] * b[2], a[0] * b[1] - a[1] * b[0]


def step_core(g, flags, update, rho_e, sig_e, trs, p, q, t, table, ztable, outs, scratch):
    grho, gsig, sums, own, xa, xb, ya, yb = outs
    vxr, vxs, vyr, vys, vzr, vzs, rt_s, az, bz, yu, ym = scratch
    nx, ny, nz, w = g.nx, g.ny, g.nz, g.pl
    (even, _, _), (yeven, _, _) = flags_of(g, flags)
    zero = jnp.zeros((ny, nz), F32)
    zero8 = jnp.zeros((8, nz), F32)
    before, after = ray_offsets(g, flags, trs)
    step = STEP
    rows = step * ny
    ext = ((rho_e, az), (sig_e, bz))

    def span(start, size, tile=8):
        return pl.ds(start if isinstance(start, int) or tile == 1 else pl.multiple_of(start, tile), size)

    def plane(x):
        return span((x + 1) * ny, ny)

    def zdiff(v):
        return jnp.dot(split2(v), ztable[...], preferred_element_type=F32)

    def slopes(ref, z, x):
        at = g.own(x)
        sx = ref[pl.ds(at + w, ny), :] - ref[pl.ds(at - w, ny), :]
        sy = ref[pl.ds(at + 1, ny), :] - ref[pl.ds(at - 1, ny), :]
        return sx, sy, z[plane(x), :]

    def cross_plane(x, acc, inside):
        a = slopes(*ext[0], x)
        b = slopes(*ext[1], x)
        c = cross(a, b)
        vxr[plane(x), :] = b[1] * c[2] - b[2] * c[1]
        vxs[plane(x), :] = c[1] * a[2] - c[2] * a[1]
        if not inside:
            return acc
        at = pl.ds(g.own(x), ny)
        vyr[at, :] = b[2] * c[0] - b[0] * c[2]
        vys[at, :] = c[2] * a[0] - c[0] * a[2]
        vzr[plane(x), :] = b[0] * c[1] - b[1] * c[0]
        vzs[plane(x), :] = c[0] * a[1] - c[1] * a[0]
        return acc + fold8(c[0] * c[0] + c[1] * c[1] + c[2] * c[2])

    def fields_chunk(c, carry):
        run, acc = carry
        values = ([], [])
        for k in range(step):
            x = c * step + k
            at = pl.ds(g.own(x), ny)
            rho, sig = update(x, at)
            rho_e[at, :] = rho
            sig_e[at, :] = sig
            values[0].append(rho)
            values[1].append(sig)
            run = run + sig
            miss = run - t[x]
            rt_s[span(x * ny, ny), :] = miss
            acc = acc + fold8(miss * miss)
        at = span(c * rows + ny, rows)
        pieces = split2(jnp.concatenate(values[0] + values[1], axis=0))
        y = jnp.dot(pieces[:rows], table[...], preferred_element_type=F32)
        yu[at, :] = y[:, :nz]
        ym[at, :] = y[:, nz:]
        z = jnp.dot(pieces, ztable[...], preferred_element_type=F32)
        az[at, :] = z[:rows]
        bz[at, :] = z[rows:]
        return run, acc

    chunks = nx // step
    _, acc_t = lax.fori_loop(0, chunks, fields_chunk, (before, zero8), unroll=UNROLL_FIELDS)

    lines = (-1, ny)
    line = lambda ref, x, y: ref[pl.ds((XO + x) * w + YO + y, nx, stride=w), :]
    flat = lambda ref, x: ref[g.own(x) : g.own(x) + ny, :]
    pieces = [line(ref, 0, y) for ref, _ in ext for y in lines] + [flat(ref, x) for ref, _ in ext for x in (-1, nx)]
    deep = zdiff(jnp.concatenate(pieces, axis=0))
    for k, y in enumerate(lines):
        fields = []
        for f, (ref, _) in enumerate(ext):
            at = (2 * f + k) * nx
            fields.append((line(ref, 1, y) - line(ref, -1, y), line(ref, 0, y + 1) - line(ref, 0, y - 1), deep[at : at + nx]))
        a, b = fields
        c = cross(a, b)
        spot = pl.ds(XO * w + YO + y, nx, stride=w)
        vyr[spot, :] = b[2] * c[0] - b[0] * c[2]
        vys[spot, :] = c[2] * a[0] - c[0] * a[2]
    base = 4 * nx
    for k, x in enumerate((-1, nx)):
        for f, (_, z) in enumerate(ext):
            at = base + (2 * f + k) * ny
            z[plane(x), :] = deep[at : at + ny]

    def gradient_plane(x, carry):
        back, sum_t, sum_r, nr, ns, acc = carry
        at = g.own(x)
        here = plane(x)
        flat_at = span(x * ny, ny)

        def term(vx, vy, vz):
            along_x = vx[plane(x - 1), :] - vx[plane(x + 1), :]
            along_y = vy[pl.ds(at - 1, ny), :] - vy[pl.ds(at + 1, ny), :]
            return along_x + along_y - vz[here, :]

        back = back + rt_s[flat_at, :]
        miss = yu[here, :] - p[x]
        gr = ym[here, :] - q[x] + term(vxr, vyr, vzr)
        gs = back * (SCALE * g.xs * g.xs) + term(vxs, vys, vzs)
        out = pl.ds(x * g.gp, ny)
        grho[out, :] = gr
        gsig[out, :] = gs
        sum_t = sum_t + gs
        return back, sum_t, sum_r + sum_t, nr + fold8(gr * gr), ns + fold8(gs * gs), acc + fold8(miss * miss)

    def crosses(c, acc):
        for k in range(step):
            acc = cross_plane(c * step + step - 1 - k, acc, True)
        return acc

    def adjoint(c):
        at = span(c * rows + ny, rows)
        z = zdiff(jnp.concatenate([vzr[at, :], vzs[at, :]], axis=0))
        vzr[at, :] = z[:rows]
        vzs[at, :] = z[rows:]

    def gradients(c, carry):
        for k in range(step):
            carry = gradient_plane(c * step + step - 1 - k, carry)
        return carry

    carry = (after, zero, zero, zero8, zero8, zero8)
    cross_plane(-1, None, False)
    cross_plane(nx, None, False)
    acc_c = crosses(chunks - 1, zero8)
    acc_c = crosses(chunks - 2, acc_c)
    adjoint(chunks - 1)

    def main(i, carry):
        c = chunks - 3 - i
        acc = crosses(c, carry[0])
        adjoint(c + 1)
        return acc, gradients(c + 2, carry[1])

    acc_c, carry = lax.fori_loop(0, chunks - 2, main, (acc_c, carry), unroll=UNROLL_MAIN)
    adjoint(0)
    carry = gradients(1, carry)
    _, sum_t, sum_r, nr, ns, acc_p = gradients(0, carry)

    total = lambda v: jnp.sum(jnp.sum(v, axis=0, keepdims=True), axis=1, keepdims=True)
    spread = sums.shape[0] if own is None else 8
    lane = lax.broadcasted_iota(jnp.int32, (spread, nz), 1)
    obj = acc_t * (g.xs * g.xs) + acc_p * (g.zs * g.zs) + acc_c * (BETA / 16.0)
    sums[0:spread, :] = jnp.where(lane == 0, total(nr), jnp.where(lane == 1, total(ns), jnp.where(lane == 2, total(obj), 0.0)))
    if own is not None:
        rest = sum_t * (nx + 1.0) - sum_r
        pos = 0
        for block in (grho, gsig):
            for r in range(2):
                put_pair(even, block[pl.ds(r * g.gp, ny), :], block[pl.ds((nx - 2 + r) * g.gp, ny), :], xa, xb, pos)
                pos += ny
        for ref, at in ((own, 0), (xa, pos)):
            ref[at : at + ny, :] = sum_t
            ref[at + ny : at + 2 * ny, :] = rest
        for f, block in enumerate((grho, gsig)):
            for r in range(2):
                rows_low = block[pl.ds(r, nx, stride=g.gp), :]
                rows_high = block[pl.ds(ny - 2 + r, nx, stride=g.gp), :]
                put_pair(yeven, rows_low, rows_high, ya, yb, (f * 2 + r) * nx)
            for k, (dx, dy) in enumerate(DIAGONALS):
                cell = (0 if dx < 0 else nx - 1) * g.gp + (0 if dy < 0 else ny - 1)
                sums[8 + 2 * k + f : 9 + 2 * k + f, :] = block[cell : cell + 1, :]


def opening_step(g, zones, flags, zlow, zhigh, xa, xb, ya, yb, ca, cb, own, rho, sig, p, q, t, table, ztable, *refs):
    others, rest = refs[: g.pairs - 1], refs[g.pairs - 1 :]
    rho_e, sig_e, trs, xlow, xhigh, ylow, yhigh = rest[:7]
    ny = g.ny
    _, (yeven, yfirst, ylast) = flags_of(g, flags)
    for f, ext in ((0, rho_e), (1, sig_e)):
        for axis, side, at, spot, value in halo_values(g, flags, f, xa, xb, ya, yb, g.nx, XO):
            ext[spot, :] = value
    for axis, side, at, spot, value in halo_values(g, flags, 2, xa, xb, ya, yb, g.nx, XO):
        low, high = bounds_of(zones, value, zlow, zhigh)
        lows, highs = ((xlow, xhigh), (ylow, yhigh))[axis]
        if axis == 1:
            at = at // g.nx * g.xp + XO
        lows[side, pl.ds(at, value.shape[0]), :] = low
        highs[side, pl.ds(at, value.shape[0]), :] = high
    cells = pick_sides(yeven, yfirst, ylast, ca[...], cb[...])
    limits = [bounds_of(zones, values, zlow, zhigh) for values in cells]
    for side, row in ((0, YO - 1), (1, YO + ny)):
        for k, plane in enumerate((XO - 1, XO + g.nx)):
            at = plane * g.pl + row
            rho_e[at : at + 1, :] = cells[side][k : k + 1]
            sig_e[at : at + 1, :] = cells[side][2 + k : 3 + k]
            at = (1 - side) * g.xp + plane
            ylow[side, at : at + 1, :] = limits[side][0][4 + k : 5 + k]
            yhigh[side, at : at + 1, :] = limits[side][1][4 + k : 5 + k]
    pos = 6 * ny
    trs[0] = own[...]
    trs[1] = xa[pos : pos + 2 * ny, :]
    for m, other in enumerate(others):
        trs[2 + m] = other[...]
    step_core(g, flags, lambda x, at: (rho[x], sig[x]), rho_e, sig_e, trs, p, q, t, table, ztable, rest[7:15], rest[15:])


def later_step(g, last, flags, xa, xb, ya, yb, sums_i, own_i, grho_i, gsig_i, rho_i, sig_i, low, high,
               xlow, xhigh, ylow, yhigh, trs_i, p, q, t, table, ztable, *refs):
    others, rest = refs[: g.pairs - 1], refs[g.pairs - 1 :]
    rho_e, sig_e, trs = rest[:3]
    ny = g.ny
    ar, asig = alphas(g, sums_i)
    clip = lambda v, lows, highs: jnp.minimum(jnp.maximum(v, lows), highs)
    for axis, side, at, spot, value in halo_values(g, flags, 0, xa, xb, ya, yb, g.nx, XO):
        lows, highs = ((xlow, xhigh), (ylow, yhigh))[axis]
        if axis == 1:
            at = at // g.nx * g.xp + XO
        here = pl.ds(at, value.shape[0])
        rho_e[spot, :] = clip(rho_i[spot, :] - ar * value, lows[side, here, :], highs[side, here, :])
    for axis, side, at, spot, value in halo_values(g, flags, 1, xa, xb, ya, yb, g.nx, XO):
        sig_e[spot, :] = sig_i[spot, :] - asig * value
    for dx, dy in DIAGONALS:
        ok, there = diagonal(g, flags, dx, dy)
        plane = XO - 1 if dx < 0 else XO + g.nx
        side = 0 if dy < 0 else 1
        here = pl.ds((1 - side) * g.xp + plane, 1)
        spot = pl.ds(plane * g.pl + (YO - 1 if dy < 0 else YO + ny), 1)
        value = jnp.where(ok, sums_i[pl.ds(there * CHUNK + 1, 1), :], 0.0)
        rho_e[spot, :] = clip(rho_i[spot, :] - ar * value, ylow[side, here, :], yhigh[side, here, :])
        value = jnp.where(ok, sums_i[pl.ds(there * CHUNK + 2, 1), :], 0.0)
        sig_e[spot, :] = sig_i[spot, :] - asig * value
    pos = 4 * ny
    trs[0] = trs_i[0] - asig * own_i[...]
    trs[1] = trs_i[1] - asig * xa[pos : pos + 2 * ny, :]
    for m, other in enumerate(others):
        trs[2 + m] = trs_i[2 + m] - asig * other[...]

    def update(x, at):
        here = pl.ds(x * g.gp, ny)
        moved = rho_i[at, :] - ar * grho_i[here, :]
        return clip(moved, low[x], high[x]), sig_i[at, :] - asig * gsig_i[here, :]

    if last:
        outs, scratch = (*rest[3:6], None, None, None, None, None), rest[6:]
    else:
        outs, scratch = rest[3:11], rest[11:]
    step_core(g, flags, update, rho_e, sig_e, trs, p, q, t, table, ztable, outs, scratch)


def closing_kernel(g, sums0, sums1, sums2, grho, gsig, rho_e, sig_e, low, high, rho_o, sig_o, obj):
    ar, asig = alphas(g, sums2)

    def body(x, carry):
        at = pl.ds(g.own(x), g.ny)
        here = pl.ds(x * g.gp, g.ny)
        rho_o[x] = jnp.minimum(jnp.maximum(rho_e[at, :] - ar * grho[here, :], low[x]), high[x])
        sig_o[x] = sig_e[at, :] - asig * gsig[here, :]
        return carry

    lax.fori_loop(0, g.nx, body, 0, unroll=8)
    for k, sums in enumerate((sums0, sums1, sums2)):
        row = sum_row(g, sums)
        lane = lax.broadcasted_iota(jnp.int32, row.shape, 1)
        obj[k] = jnp.sum(jnp.where(lane == 2, row, 0.0)) * (0.5 / g.cells)


def pairs_of(size):
    a = [(i, i ^ 1) for i in range(size)]
    b = [(i, i if i in (0, size - 1) else ((i + 1) ^ 1) - 1) for i in range(size)]
    return a, b


def exchange(axis, a, b):
    pa, pb = pairs_of(lax.axis_size(axis))
    a = lax.ppermute(a, axis, pa)
    b = lax.ppermute(b, axis, pb)
    return a, b


def pair_totals(pair, size):
    out = []
    for m in range(1, size // 2):
        out.append(lax.ppermute(pair, "gx", [(i, i ^ (2 * m)) for i in range(size)]))
    return out


SMEM = pl.BlockSpec(memory_space=pltpu.SMEM)
VMEM = pl.BlockSpec(memory_space=pltpu.VMEM)
HBM = pl.BlockSpec(memory_space=pltpu.HBM)


def call(body, shapes, specs, args, scratch=(), limit=12, outs=None):
    return pl.pallas_call(
        body,
        out_shape=[jax.ShapeDtypeStruct(s, d) for s, d in shapes],
        in_specs=specs,
        out_specs=outs or [VMEM] * len(shapes),
        scratch_shapes=list(scratch),
        compiler_params=pltpu.CompilerParams(vmem_limit_bytes=limit * 1024 * 1024),
    )(*args)


def local(density, slowness, pressure_obs, time_obs, zone_map, zone_low, zone_high):
    nx, ny, nz = density.shape
    px, py = lax.axis_size("gx"), lax.axis_size("gy")
    g = Geo(nx, ny, nz, px, py)
    zones = zone_low.shape[0]
    both = ("gx", "gy")
    flags = jnp.stack([lax.axis_index("gx"), lax.axis_index("gy")]).astype(jnp.int32)

    ext = ((g.ext, nz), F32)
    own_shape = ((2 * ny, nz), F32)
    trs_shape = ((g.pairs + 1, 2 * ny, nz), F32)
    sums_shape = ((px * py, nz), F32)
    block = ((nx, ny, nz), F32)
    flat = ((nx * g.gp, nz), F32)
    xa_shape = lambda f: (((f + 1) * 2 * ny, nz), F32)
    xb_shape = lambda f: ((f * 2 * ny, nz), F32)
    ymsg = lambda f: ((f * 2 * nx, nz), F32)
    xbound = ((2, 2 * ny, nz), F32)
    ybound = ((2, 2 * g.xp, nz), F32)
    win = pltpu.VMEM((g.win, nz), F32)
    ext_v = pltpu.VMEM((g.ext, nz), F32)
    core_scratch = [win] * 2 + [ext_v] * 2 + [win] * 2 + [pltpu.VMEM((nx * ny, nz), F32)] + [win] * 4

    own, xa, xb = call(
        functools.partial(first_kernel, g), [own_shape, xa_shape(3), xb_shape(3)],
        [SMEM] + [HBM] * 4, (flags, *(pltpu.with_memory_space_constraint(v, pltpu.HBM) for v in (density, slowness, zone_map, time_obs))),
        [pltpu.VMEM((2, 1, 2, ny, nz), F32), pltpu.VMEM((2, 2, ny, nz), jnp.int32),
         pltpu.VMEM((nx, ny, nz), F32), pltpu.VMEM((nx, ny, nz), F32), pltpu.SemaphoreType.DMA((4 + nx // 4,))],
    )
    xa, xb = exchange("gx", xa, xb)
    low, high, t = call(
        functools.partial(bounds_kernel, g, zones), [block] * 3,
        [SMEM, SMEM] + [VMEM] * 2, (zone_low, zone_high, zone_map, time_obs),
    )
    q, p, table, ztable = call(
        functools.partial(spread_kernel, g),
        [block] * 2 + [((2 * nz, 2 * nz), BF16), ((2 * nz, nz), BF16)], [VMEM], (pressure_obs,),
    )
    as_rows = lambda v: v.reshape(nx * ny, nz)
    ya, yb = call(
        functools.partial(sides_kernel, g, 3), [ymsg(3)] * 2,
        [SMEM] + [VMEM] * 4, (flags, own, as_rows(density), as_rows(slowness), as_rows(zone_map)),
    )
    ya, yb = exchange("gy", ya, yb)
    ca, cb, pair = call(
        functools.partial(corners_kernel, g, 3), [((8, nz), F32)] * 2 + [own_shape],
        [SMEM] + [VMEM] * 3, (flags, xa, xb, own),
    )
    ca, cb = exchange("gy", ca, cb)
    others = pair_totals(pair, px)
    ends = [flat, flat, ((16, nz), F32), own_shape, xa_shape(2), xb_shape(2), ymsg(2), ymsg(2)]
    chunks = ((px * py * CHUNK, nz), F32)
    outs = call(
        functools.partial(opening_step, g, zones),
        [ext, ext, trs_shape, xbound, xbound, ybound, ybound] + ends,
        [SMEM] * 3 + [VMEM] * (14 + len(others)),
        (flags, zone_low, zone_high, xa, xb, ya, yb, ca, cb, own, density, slowness, p, q, t, table, ztable, *others),
        core_scratch, 24,
    )
    rho_e, sig_e, trs, xlow, xhigh, ylow, yhigh, grho, gsig, head, own, xa, xb, ya, yb = outs
    history = []
    for iteration in range(1, ITERS):
        last = iteration == ITERS - 1
        xa, xb = exchange("gx", xa, xb)
        ya, yb = exchange("gy", ya, yb)
        pair, sums = call(
            functools.partial(join_kernel, g), [own_shape, chunks], [SMEM] + [VMEM] * 3,
            (flags, xa, own, head),
        )
        others = pair_totals(pair, px)
        sums = lax.all_to_all(sums, both, 0, 0, tiled=True)
        history.append(sums)
        outs = call(
            functools.partial(later_step, g, last), [ext, ext, trs_shape] + ([flat, flat, sums_shape] if last else ends),
            [SMEM] + [VMEM] * (22 + len(others)),
            (flags, xa, xb, ya, yb, sums, own, grho, gsig, rho_e, sig_e, low, high, xlow, xhigh, ylow, yhigh, trs,
             p, q, t, table, ztable, *others),
            core_scratch, 24,
        )
        rho_e, sig_e, trs, grho, gsig, head = outs[:6]
        if not last:
            own, xa, xb, ya, yb = outs[6:]
    history.append(lax.all_to_all(head, both, 0, 0, tiled=True))
    rho, sigma, obj = call(
        functools.partial(closing_kernel, g), [block, block, ((ITERS,), F32)],
        [VMEM] * 9, (*history, grho, gsig, rho_e, sig_e, low, high), outs=[VMEM, VMEM, SMEM],
    )
    return rho, sigma, obj


def solution(mesh):
    placed = (P("gx", "gy", None),) * 5 + (P(), P())
    return jax.shard_map(
        local,
        mesh=mesh,
        in_specs=placed,
        out_specs=(P("gx", "gy", None), P("gx", "gy", None), P()),
        check_vma=False,
    )
```

```python
import functools
import math

import jax
import jax.numpy as jnp
from jax import lax
from jax.experimental import pallas as pl
from jax.experimental.pallas import tpu as pltpu
from jax.sharding import PartitionSpec as P


ITERS = 3
BETA = 1.0
ETA = 0.5
EPSILON = 1e-06

XO = 2
YO = 8
CHUNK = 4
STEP = 16
UNROLL_FIELDS = 4
UNROLL_MAIN = 2
SCALE = 16.0 / BETA
DIAGONALS = ((-1, -1), (-1, 1), (1, -1), (1, 1))
F32 = jnp.float32
BF16 = jnp.bfloat16


class Geo:
    def __init__(self, nx, ny, nz, px, py):
        self.nx, self.ny, self.nz, self.px, self.py = nx, ny, nz, px, py
        self.pl = ny + YO + 1
        self.gp = ny + 1
        self.ext = (nx + 9) * self.pl
        self.xp = nx + 8
        self.cells = float(nx * px * ny * py * nz)
        self.zs = 1.0 / math.sqrt(nz)
        self.xs = 1.0 / math.sqrt(nx * px)
        self.win = (nx + 2) * ny
        self.pairs = px // 2

    def own(self, x):
        return (x + XO) * self.pl + YO


def fold8(v):
    total = v[0:8]
    for i in range(8, v.shape[0], 8):
        total = total + v[i : i + 8]
    return total


def pick_sides(even, first, last, a, b):
    low = jnp.where(even, b, a)
    high = jnp.where(even, a, b)
    return jnp.where(first, 0.0, low), jnp.where(last, 0.0, high)


def put_pair(even, low, high, a_ref, b_ref, at):
    n = low.shape[0]
    a_ref[at : at + n, :] = jnp.where(even, high, low)
    b_ref[at : at + n, :] = jnp.where(even, low, high)


def flags_of(g, flags):
    ix, iy = flags[0], flags[1]
    return ((ix % 2) == 0, ix == 0, ix == g.px - 1), ((iy % 2) == 0, iy == 0, iy == g.py - 1)


def split2(v):
    high = v.astype(BF16)
    low = (v - high.astype(F32)).astype(BF16)
    return jnp.concatenate([high, low], axis=1)


def bounds_of(zones, z, zlow, zhigh):
    low = jnp.full(z.shape, zlow[0], F32)
    high = jnp.full(z.shape, zhigh[0], F32)
    for i in range(1, zones):
        hit = z == i
        low = jnp.where(hit, zlow[i], low)
        high = jnp.where(hit, zhigh[i], high)
    return low, high


def first_kernel(g, flags, rho, sigma, zone, t, own, xa, xb, sig_v, t_v, rims, zrims, sems):
    (even, _, _), _ = flags_of(g, flags)
    step = 8
    small = []
    for k, at in enumerate((0, g.nx - 2)):
        small.append(pltpu.make_async_copy(rho.at[pl.ds(at, 2)], rims.at[k, 0], sems.at[2 * k]))
        small.append(pltpu.make_async_copy(zone.at[pl.ds(at, 2)], zrims.at[k], sems.at[2 * k + 1]))
    big = []
    for c in range(g.nx // step):
        at = pl.ds(c * step, step)
        big.append((
            pltpu.make_async_copy(sigma.at[at], sig_v.at[at], sems.at[4 + 2 * c]),
            pltpu.make_async_copy(t.at[at], t_v.at[at], sems.at[5 + 2 * c]),
        ))
    for a, b in big:
        a.start()
        b.start()
    for copy in small:
        copy.start()
    zero = jnp.zeros((g.ny, g.nz), F32)
    run, total, seen = zero, zero, zero
    for c, (a, b) in enumerate(big):
        a.wait()
        b.wait()
        for k in range(step):
            run = run + sig_v[c * step + k]
            total = total + run
            scaled = t_v[c * step + k] * (1.0 / g.xs)
            t_v[c * step + k] = scaled
            seen = seen + scaled
    own[0 : g.ny, :] = run
    own[g.ny : 2 * g.ny, :] = total - seen
    for copy in small:
        copy.wait()
    at = 0
    for r in range(2):
        put_pair(even, rims[0, 0, r], rims[1, 0, r], xa, xb, at)
        at += g.ny
    for r in range(2):
        put_pair(even, sig_v[r], sig_v[g.nx - 2 + r], xa, xb, at)
        at += g.ny
    for r in range(2):
        put_pair(even, zrims[0, r].astype(F32), zrims[1, r].astype(F32), xa, xb, at)
        at += g.ny
    xa[at : at + g.ny, :] = run
    xa[at + g.ny : at + 2 * g.ny, :] = total - seen


def bounds_kernel(g, zones, zlow, zhigh, zone, low_o, high_o):
    def body(x, carry):
        low_o[x], high_o[x] = bounds_of(zones, zone[x], zlow, zhigh)
        return carry

    lax.fori_loop(0, g.nx, body, 0, unroll=8)


def spread_kernel(g, p, q, p_o, table, ztable):
    nz = g.nz
    row = lax.broadcasted_iota(jnp.int32, (2 * nz, 2 * nz), 0) % nz
    col = lax.broadcasted_iota(jnp.int32, (2 * nz, 2 * nz), 1)
    first = (row <= col).astype(F32)
    second = (nz - jnp.maximum(row, col - nz)).astype(F32) * (SCALE / nz)
    table[...] = jnp.where(col < nz, first, second).astype(BF16)
    r2 = lax.broadcasted_iota(jnp.int32, (2 * nz, nz), 0) % nz
    c2 = lax.broadcasted_iota(jnp.int32, (2 * nz, nz), 1)
    back = (r2 >= c2).astype(F32).astype(BF16)
    ztable[...] = ((r2 == c2 + 1).astype(F32) - (r2 == c2 - 1).astype(F32)).astype(BF16)
    step = 16

    def body(c, carry):
        here = pl.ds(c * step, step)
        values = p[here]
        p_o[here] = values * (1.0 / g.zs)
        out = jnp.dot(split2(values.reshape(step * g.ny, nz)), back, preferred_element_type=F32) * (g.zs * SCALE)
        q[here] = out.reshape(step, g.ny, nz)
        return carry

    lax.fori_loop(0, g.nx // step, body, 0, unroll=True)


def join_kernel(g, flags, xa, own, head, pair, sums):
    (even, _, _), _ = flags_of(g, flags)
    ny = g.ny
    at = 4 * ny
    join_pair(g, even, own, xa, at, pair)
    n = sums.shape[0] // CHUNK
    sums[...] = jnp.zeros(sums.shape, F32)
    sums[pl.ds(0, n, stride=CHUNK), :] = jnp.broadcast_to(head[0:1, :], (n, g.nz))
    for k, (dx, dy) in enumerate(DIAGONALS):
        ok, there = diagonal(g, flags, dx, dy)

        @pl.when(ok)
        def _():
            for f in range(2):
                sums[pl.ds(there * CHUNK + 1 + f, 1), :] = head[8 + 2 * k + f : 9 + 2 * k + f, :]


def diagonal(g, flags, dx, dy):
    ix, iy = flags[0] + dx, flags[1] + dy
    ok = jnp.logical_and(jnp.logical_and(ix >= 0, ix < g.px), jnp.logical_and(iy >= 0, iy < g.py))
    return ok, jnp.where(ok, ix * g.py + iy, 0)


def join_pair(g, even, own, xa, at, pair):
    ny = g.ny
    mine_t, mine_s = own[0:ny, :], own[ny : 2 * ny, :]
    other_t, other_s = xa[at : at + ny, :], xa[at + ny : at + 2 * ny, :]
    pair[0:ny, :] = mine_t + other_t
    pair[ny : 2 * ny, :] = mine_s + other_s + jnp.where(even, mine_t, other_t) * float(g.nx)


def sides_kernel(g, fields, flags, order, *refs):
    blocks, (ya, yb) = refs[:fields], refs[fields:]
    _, (even, _, _) = flags_of(g, flags)
    for f in range(fields):
        for r in range(2):
            low = blocks[f][pl.ds(r, g.nx, stride=g.ny), :].astype(F32)
            high = blocks[f][pl.ds(g.ny - 2 + r, g.nx, stride=g.ny), :].astype(F32)
            put_pair(even, low, high, ya, yb, (f * 2 + r) * g.nx)


def corners_kernel(g, fields, flags, xa, xb, own, ca, cb, pair):
    (even, first, last), (yeven, _, _) = flags_of(g, flags)
    ca[...] = jnp.zeros(ca.shape, F32)
    cb[...] = jnp.zeros(cb.shape, F32)
    for f in range(fields):
        for side, px in ((0, 1), (1, 0)):
            at = (f * 2 + px) * g.ny
            value = pick_sides(even, first, last, xa[at : at + g.ny, :], xb[at : at + g.ny, :])[side]
            put_pair(yeven, value[0:1], value[g.ny - 1 : g.ny], ca, cb, 2 * f + side)
    join_pair(g, even, own, xa, fields * 2 * g.ny, pair)


def halo_slots(g, n, off):
    xs = []
    for r in range(2):
        xs.append((r * g.ny, pl.ds(r * g.pl + YO, g.ny), pl.ds((XO + g.nx + r) * g.pl + YO, g.ny)))
    ys = []
    for r in range(2):
        first = off * g.pl + r
        ys.append((r * n, pl.ds(first + YO - 2, n, stride=g.pl), pl.ds(first + YO + g.ny, n, stride=g.pl)))
    return xs, ys


def halo_values(g, flags, field, xa, xb, ya, yb, yn, off):
    (xeven, xfirst, xlast), (yeven, yfirst, ylast) = flags_of(g, flags)
    xs, ys = halo_slots(g, yn, off)
    for axis, slots, n, a, b, even, first, last in (
        (0, xs, g.ny, xa, xb, xeven, xfirst, xlast),
        (1, ys, yn, ya, yb, yeven, yfirst, ylast),
    ):
        for at, low_rows, high_rows in slots:
            here = pl.ds(field * 2 * n + at, n)
            low, high = pick_sides(even, first, last, a[here, :], b[here, :])
            yield axis, 0, at, low_rows, low
            yield axis, 1, at, high_rows, high


def lane_value(row, lane):
    ids = lax.broadcasted_iota(jnp.int32, row.shape, 1)
    return jnp.sum(jnp.where(ids == lane, row, 0.0), axis=1, keepdims=True)


def sum_row(g, sums):
    n = g.px * g.py
    return jnp.sum(sums[pl.ds(0, n, stride=sums.shape[0] // n), :], axis=0, keepdims=True)


def alphas(g, sums):
    row = sum_row(g, sums)
    return tuple(
        ETA / SCALE * lax.rsqrt(lane_value(row, k) * (1.0 / (g.cells * SCALE * SCALE)) + EPSILON) for k in range(2)
    )


def ray_offsets(g, flags, trs):
    ix = flags[0]
    q = ix // 2
    even = (ix % 2) == 0
    ny = g.ny
    mine, other = trs[0, 0:ny, :], trs[1, 0:ny, :]
    reach = float(g.nx)
    before = jnp.where(even, 0.0, other)
    sums = jnp.zeros_like(mine)
    spread = (mine + other) * (g.pairs - 1 - q).astype(F32)
    for m in range(1, g.pairs):
        p = q ^ m
        total = trs[1 + m, 0:ny, :]
        before = before + jnp.where(p < q, total, 0.0)
        sums = sums + jnp.where(p > q, trs[1 + m, ny : 2 * ny, :], 0.0)
        spread = spread + total * (g.pairs - 1 - jnp.maximum(p, q)).astype(F32)
    near = jnp.where(even, trs[1, ny : 2 * ny, :] + (before + mine) * reach, 0.0)
    return before, near + sums + spread * (2.0 * reach)


def cross(a, b):
    return a[1] * b[2] - a[2] * b[1], a[2] * b[0] - a[0] * b[2], a[0] * b[1] - a[1] * b[0]


def step_core(g, flags, update, rho_e, sig_e, trs, p, q, t, table, ztable, outs, scratch):
    grho, gsig, sums, own, xa, xb, ya, yb = outs
    vxr, vxs, vyr, vys, vzr, vzs, rt_s, az, bz, yu, ym = scratch
    nx, ny, nz, w = g.nx, g.ny, g.nz, g.pl
    (even, _, _), (yeven, _, _) = flags_of(g, flags)
    zero = jnp.zeros((ny, nz), F32)
    zero8 = jnp.zeros((8, nz), F32)
    before, after = ray_offsets(g, flags, trs)
    step = STEP
    rows = step * ny
    ext = ((rho_e, az), (sig_e, bz))

    def span(start, size, tile=8):
        return pl.ds(start if isinstance(start, int) or tile == 1 else pl.multiple_of(start, tile), size)

    def plane(x):
        return span((x + 1) * ny, ny)

    def zdiff(v):
        return jnp.dot(split2(v), ztable[...], preferred_element_type=F32)

    def slopes(ref, z, x):
        at = g.own(x)
        sx = ref[pl.ds(at + w, ny), :] - ref[pl.ds(at - w, ny), :]
        sy = ref[pl.ds(at + 1, ny), :] - ref[pl.ds(at - 1, ny), :]
        return sx, sy, z[plane(x), :]

    def cross_plane(x, acc, inside):
        a = slopes(*ext[0], x)
        b = slopes(*ext[1], x)
        c = cross(a, b)
        vxr[plane(x), :] = b[1] * c[2] - b[2] * c[1]
        vxs[plane(x), :] = c[1] * a[2] - c[2] * a[1]
        if not inside:
            return acc
        at = pl.ds(g.own(x), ny)
        vyr[at, :] = b[2] * c[0] - b[0] * c[2]
        vys[at, :] = c[2] * a[0] - c[0] * a[2]
        vzr[plane(x), :] = b[0] * c[1] - b[1] * c[0]
        vzs[plane(x), :] = c[0] * a[1] - c[1] * a[0]
        return acc + fold8(c[0] * c[0] + c[1] * c[1] + c[2] * c[2])

    def fields_chunk(c, carry):
        run, acc = carry
        values = ([], [])
        for k in range(step):
            x = c * step + k
            at = pl.ds(g.own(x), ny)
            rho, sig = update(x, at)
            rho_e[at, :] = rho
            sig_e[at, :] = sig
            values[0].append(rho)
            values[1].append(sig)
            run = run + sig
            miss = run - t[x]
            rt_s[span(x * ny, ny), :] = miss
            acc = acc + fold8(miss * miss)
        at = span(c * rows + ny, rows)
        pieces = split2(jnp.concatenate(values[0] + values[1], axis=0))
        y = jnp.dot(pieces[:rows], table[...], preferred_element_type=F32)
        yu[at, :] = y[:, :nz]
        ym[at, :] = y[:, nz:]
        z = jnp.dot(pieces, ztable[...], preferred_element_type=F32)
        az[at, :] = z[:rows]
        bz[at, :] = z[rows:]
        return run, acc

    chunks = nx // step
    _, acc_t = lax.fori_loop(0, chunks, fields_chunk, (before, zero8), unroll=UNROLL_FIELDS)

    lines = (-1, ny)
    line = lambda ref, x, y: ref[pl.ds((XO + x) * w + YO + y, nx, stride=w), :]
    flat = lambda ref, x: ref[g.own(x) : g.own(x) + ny, :]
    pieces = [line(ref, 0, y) for ref, _ in ext for y in lines] + [flat(ref, x) for ref, _ in ext for x in (-1, nx)]
    deep = zdiff(jnp.concatenate(pieces, axis=0))
    for k, y in enumerate(lines):
        fields = []
        for f, (ref, _) in enumerate(ext):
            at = (2 * f + k) * nx
            fields.append((line(ref, 1, y) - line(ref, -1, y), line(ref, 0, y + 1) - line(ref, 0, y - 1), deep[at : at + nx]))
        a, b = fields
        c = cross(a, b)
        spot = pl.ds(XO * w + YO + y, nx, stride=w)
        vyr[spot, :] = b[2] * c[0] - b[0] * c[2]
        vys[spot, :] = c[2] * a[0] - c[0] * a[2]
    base = 4 * nx
    for k, x in enumerate((-1, nx)):
        for f, (_, z) in enumerate(ext):
            at = base + (2 * f + k) * ny
            z[plane(x), :] = deep[at : at + ny]

    def gradient_plane(x, carry):
        back, sum_t, sum_r, nr, ns, acc = carry
        at = g.own(x)
        here = plane(x)
        flat_at = span(x * ny, ny)

        def term(vx, vy, vz):
            along_x = vx[plane(x - 1), :] - vx[plane(x + 1), :]
            along_y = vy[pl.ds(at - 1, ny), :] - vy[pl.ds(at + 1, ny), :]
            return along_x + along_y - vz[here, :]

        back = back + rt_s[flat_at, :]
        miss = yu[here, :] - p[x]
        gr = ym[here, :] - q[x] + term(vxr, vyr, vzr)
        gs = back * (SCALE * g.xs * g.xs) + term(vxs, vys, vzs)
        out = pl.ds(x * g.gp, ny)
        grho[out, :] = gr
        gsig[out, :] = gs
        sum_t = sum_t + gs
        return back, sum_t, sum_r + sum_t, nr + fold8(gr * gr), ns + fold8(gs * gs), acc + fold8(miss * miss)

    def crosses(c, acc):
        for k in range(step):
            acc = cross_plane(c * step + step - 1 - k, acc, True)
        return acc

    def adjoint(c):
        at = span(c * rows + ny, rows)
        z = zdiff(jnp.concatenate([vzr[at, :], vzs[at, :]], axis=0))
        vzr[at, :] = z[:rows]
        vzs[at, :] = z[rows:]

    def gradients(c, carry):
        for k in range(step):
            carry = gradient_plane(c * step + step - 1 - k, carry)
        return carry

    carry = (after, zero, zero, zero8, zero8, zero8)
    cross_plane(-1, None, False)
    cross_plane(nx, None, False)
    acc_c = crosses(chunks - 1, zero8)
    acc_c = crosses(chunks - 2, acc_c)
    adjoint(chunks - 1)

    def main(i, carry):
        c = chunks - 3 - i
        acc = crosses(c, carry[0])
        adjoint(c + 1)
        return acc, gradients(c + 2, carry[1])

    acc_c, carry = lax.fori_loop(0, chunks - 2, main, (acc_c, carry), unroll=UNROLL_MAIN)
    adjoint(0)
    carry = gradients(1, carry)
    _, sum_t, sum_r, nr, ns, acc_p = gradients(0, carry)

    total = lambda v: jnp.sum(jnp.sum(v, axis=0, keepdims=True), axis=1, keepdims=True)
    spread = sums.shape[0] if own is None else 8
    lane = lax.broadcasted_iota(jnp.int32, (spread, nz), 1)
    obj = acc_t * (g.xs * g.xs) + acc_p * (g.zs * g.zs) + acc_c * (BETA / 16.0)
    sums[0:spread, :] = jnp.where(lane == 0, total(nr), jnp.where(lane == 1, total(ns), jnp.where(lane == 2, total(obj), 0.0)))
    if own is not None:
        rest = sum_t * (nx + 1.0) - sum_r
        pos = 0
        for block in (grho, gsig):
            for r in range(2):
                put_pair(even, block[pl.ds(r * g.gp, ny), :], block[pl.ds((nx - 2 + r) * g.gp, ny), :], xa, xb, pos)
                pos += ny
        for ref, at in ((own, 0), (xa, pos)):
            ref[at : at + ny, :] = sum_t
            ref[at + ny : at + 2 * ny, :] = rest
        for f, block in enumerate((grho, gsig)):
            for r in range(2):
                rows_low = block[pl.ds(r, nx, stride=g.gp), :]
                rows_high = block[pl.ds(ny - 2 + r, nx, stride=g.gp), :]
                put_pair(yeven, rows_low, rows_high, ya, yb, (f * 2 + r) * nx)
            for k, (dx, dy) in enumerate(DIAGONALS):
                cell = (0 if dx < 0 else nx - 1) * g.gp + (0 if dy < 0 else ny - 1)
                sums[8 + 2 * k + f : 9 + 2 * k + f, :] = block[cell : cell + 1, :]


def opening_step(g, zones, flags, zlow, zhigh, xa, xb, ya, yb, ca, cb, own, rho, sig, p, q, t, table, ztable, *refs):
    others, rest = refs[: g.pairs - 1], refs[g.pairs - 1 :]
    rho_e, sig_e, trs, xlow, xhigh, ylow, yhigh = rest[:7]
    ny = g.ny
    _, (yeven, yfirst, ylast) = flags_of(g, flags)
    for f, ext in ((0, rho_e), (1, sig_e)):
        for axis, side, at, spot, value in halo_values(g, flags, f, xa, xb, ya, yb, g.nx, XO):
            ext[spot, :] = value
    for axis, side, at, spot, value in halo_values(g, flags, 2, xa, xb, ya, yb, g.nx, XO):
        low, high = bounds_of(zones, value, zlow, zhigh)
        lows, highs = ((xlow, xhigh), (ylow, yhigh))[axis]
        if axis == 1:
            at = at // g.nx * g.xp + XO
        lows[side, pl.ds(at, value.shape[0]), :] = low
        highs[side, pl.ds(at, value.shape[0]), :] = high
    cells = pick_sides(yeven, yfirst, ylast, ca[...], cb[...])
    limits = [bounds_of(zones, values, zlow, zhigh) for values in cells]
    for side, row in ((0, YO - 1), (1, YO + ny)):
        for k, plane in enumerate((XO - 1, XO + g.nx)):
            at = plane * g.pl + row
            rho_e[at : at + 1, :] = cells[side][k : k + 1]
            sig_e[at : at + 1, :] = cells[side][2 + k : 3 + k]
            at = (1 - side) * g.xp + plane
            ylow[side, at : at + 1, :] = limits[side][0][4 + k : 5 + k]
            yhigh[side, at : at + 1, :] = limits[side][1][4 + k : 5 + k]
    pos = 6 * ny
    trs[0] = own[...]
    trs[1] = xa[pos : pos + 2 * ny, :]
    for m, other in enumerate(others):
        trs[2 + m] = other[...]
    step_core(g, flags, lambda x, at: (rho[x], sig[x]), rho_e, sig_e, trs, p, q, t, table, ztable, rest[7:15], rest[15:])


def later_step(g, last, flags, xa, xb, ya, yb, sums_i, own_i, grho_i, gsig_i, rho_i, sig_i, low, high,
               xlow, xhigh, ylow, yhigh, trs_i, p, q, t, table, ztable, *refs):
    others, rest = refs[: g.pairs - 1], refs[g.pairs - 1 :]
    rest = (*rest[:2], rest[-1], *rest[2:-1]) if last else rest
    rho_e, sig_e, trs = rest[:3]
    ny = g.ny
    ar, asig = alphas(g, sums_i)
    clip = lambda v, lows, highs: jnp.minimum(jnp.maximum(v, lows), highs)
    for axis, side, at, spot, value in halo_values(g, flags, 0, xa, xb, ya, yb, g.nx, XO):
        lows, highs = ((xlow, xhigh), (ylow, yhigh))[axis]
        if axis == 1:
            at = at // g.nx * g.xp + XO
        here = pl.ds(at, value.shape[0])
        rho_e[spot, :] = clip(rho_i[spot, :] - ar * value, lows[side, here, :], highs[side, here, :])
    for axis, side, at, spot, value in halo_values(g, flags, 1, xa, xb, ya, yb, g.nx, XO):
        sig_e[spot, :] = sig_i[spot, :] - asig * value
    for dx, dy in DIAGONALS:
        ok, there = diagonal(g, flags, dx, dy)
        plane = XO - 1 if dx < 0 else XO + g.nx
        side = 0 if dy < 0 else 1
        here = pl.ds((1 - side) * g.xp + plane, 1)
        spot = pl.ds(plane * g.pl + (YO - 1 if dy < 0 else YO + ny), 1)
        value = jnp.where(ok, sums_i[pl.ds(there * CHUNK + 1, 1), :], 0.0)
        rho_e[spot, :] = clip(rho_i[spot, :] - ar * value, ylow[side, here, :], yhigh[side, here, :])
        value = jnp.where(ok, sums_i[pl.ds(there * CHUNK + 2, 1), :], 0.0)
        sig_e[spot, :] = sig_i[spot, :] - asig * value
    pos = 4 * ny
    trs[0] = trs_i[0] - asig * own_i[...]
    trs[1] = trs_i[1] - asig * xa[pos : pos + 2 * ny, :]
    for m, other in enumerate(others):
        trs[2 + m] = trs_i[2 + m] - asig * other[...]

    def update(x, at):
        here = pl.ds(x * g.gp, ny)
        moved = rho_i[at, :] - ar * grho_i[here, :]
        return clip(moved, low[x], high[x]), sig_i[at, :] - asig * gsig_i[here, :]

    if last:
        outs, scratch = (*rest[3:6], None, None, None, None, None), rest[6:]
    else:
        outs, scratch = rest[3:11], rest[11:]
    step_core(g, flags, update, rho_e, sig_e, trs, p, q, t, table, ztable, outs, scratch)


def closing_kernel(g, sums0, sums1, sums2, grho, gsig, rho_e, sig_e, low, high, rho_o, sig_o, obj):
    ar, asig = alphas(g, sums2)

    def body(x, carry):
        at = pl.ds(g.own(x), g.ny)
        here = pl.ds(x * g.gp, g.ny)
        rho_o[x] = jnp.minimum(jnp.maximum(rho_e[at, :] - ar * grho[here, :], low[x]), high[x])
        sig_o[x] = sig_e[at, :] - asig * gsig[here, :]
        return carry

    lax.fori_loop(0, g.nx, body, 0, unroll=8)
    for k, sums in enumerate((sums0, sums1, sums2)):
        row = sum_row(g, sums)
        lane = lax.broadcasted_iota(jnp.int32, row.shape, 1)
        obj[k] = jnp.sum(jnp.where(lane == 2, row, 0.0)) * (0.5 / g.cells)


def pairs_of(size):
    a = [(i, i ^ 1) for i in range(size)]
    b = [(i, i if i in (0, size - 1) else ((i + 1) ^ 1) - 1) for i in range(size)]
    return a, b


def exchange(axis, a, b):
    pa, pb = pairs_of(lax.axis_size(axis))
    a = lax.ppermute(a, axis, pa)
    b = lax.ppermute(b, axis, pb)
    return a, b


def pair_totals(pair, size):
    out = []
    for m in range(1, size // 2):
        out.append(lax.ppermute(pair, "gx", [(i, i ^ (2 * m)) for i in range(size)]))
    return out


SMEM = pl.BlockSpec(memory_space=pltpu.SMEM)
VMEM = pl.BlockSpec(memory_space=pltpu.VMEM)
HBM = pl.BlockSpec(memory_space=pltpu.HBM)


def call(body, shapes, specs, args, scratch=(), limit=12, outs=None):
    return pl.pallas_call(
        body,
        out_shape=[jax.ShapeDtypeStruct(s, d) for s, d in shapes],
        in_specs=specs,
        out_specs=outs or [VMEM] * len(shapes),
        scratch_shapes=list(scratch),
        compiler_params=pltpu.CompilerParams(vmem_limit_bytes=limit * 1024 * 1024),
    )(*args)


def local(density, slowness, pressure_obs, time_obs, zone_map, zone_low, zone_high):
    nx, ny, nz = density.shape
    px, py = lax.axis_size("gx"), lax.axis_size("gy")
    g = Geo(nx, ny, nz, px, py)
    zones = zone_low.shape[0]
    both = ("gx", "gy")
    flags = jnp.stack([lax.axis_index("gx"), lax.axis_index("gy")]).astype(jnp.int32)

    ext = ((g.ext, nz), F32)
    own_shape = ((2 * ny, nz), F32)
    trs_shape = ((g.pairs + 1, 2 * ny, nz), F32)
    sums_shape = ((px * py, nz), F32)
    block = ((nx, ny, nz), F32)
    flat = ((nx * g.gp, nz), F32)
    xa_shape = lambda f: (((f + 1) * 2 * ny, nz), F32)
    xb_shape = lambda f: ((f * 2 * ny, nz), F32)
    ymsg = lambda f: ((f * 2 * nx, nz), F32)
    xbound = ((2, 2 * ny, nz), F32)
    ybound = ((2, 2 * g.xp, nz), F32)
    win = pltpu.VMEM((g.win, nz), F32)
    ext_v = pltpu.VMEM((g.ext, nz), F32)
    core_scratch = [win] * 2 + [ext_v] * 2 + [win] * 2 + [pltpu.VMEM((nx * ny, nz), F32)] + [win] * 4

    own, xa, xb, sig, t = call(
        functools.partial(first_kernel, g), [own_shape, xa_shape(3), xb_shape(3), block, block],
        [SMEM] + [HBM] * 4, (flags, *(pltpu.with_memory_space_constraint(v, pltpu.HBM) for v in (density, slowness, zone_map, time_obs))),
        [pltpu.VMEM((2, 1, 2, ny, nz), F32), pltpu.VMEM((2, 2, ny, nz), jnp.int32),
         pltpu.SemaphoreType.DMA((4 + nx // 4,))],
    )
    xa, xb = exchange("gx", xa, xb)
    low, high = call(
        functools.partial(bounds_kernel, g, zones), [block] * 2,
        [SMEM, SMEM, VMEM], (zone_low, zone_high, zone_map),
    )
    q, p, table, ztable = call(
        functools.partial(spread_kernel, g),
        [block] * 2 + [((2 * nz, 2 * nz), BF16), ((2 * nz, nz), BF16)], [VMEM], (pressure_obs,),
    )
    as_rows = lambda v: v.reshape(nx * ny, nz)
    ya, yb = call(
        functools.partial(sides_kernel, g, 3), [ymsg(3)] * 2,
        [SMEM] + [VMEM] * 4, (flags, own, as_rows(density), as_rows(sig), as_rows(zone_map)),
    )
    ya, yb = exchange("gy", ya, yb)
    ca, cb, pair = call(
        functools.partial(corners_kernel, g, 3), [((8, nz), F32)] * 2 + [own_shape],
        [SMEM] + [VMEM] * 3, (flags, xa, xb, own),
    )
    ca, cb = exchange("gy", ca, cb)
    others = pair_totals(pair, px)
    ends = [flat, flat, ((16, nz), F32), own_shape, xa_shape(2), xb_shape(2), ymsg(2), ymsg(2)]
    chunks = ((px * py * CHUNK, nz), F32)
    outs = call(
        functools.partial(opening_step, g, zones),
        [ext, ext, trs_shape, xbound, xbound, ybound, ybound] + ends,
        [SMEM] * 3 + [VMEM] * (14 + len(others)),
        (flags, zone_low, zone_high, xa, xb, ya, yb, ca, cb, own, density, sig, p, q, t, table, ztable, *others),
        core_scratch, 24,
    )
    rho_e, sig_e, trs, xlow, xhigh, ylow, yhigh, grho, gsig, head, own, xa, xb, ya, yb = outs
    history = []
    for iteration in range(1, ITERS):
        last = iteration == ITERS - 1
        xa, xb = exchange("gx", xa, xb)
        ya, yb = exchange("gy", ya, yb)
        pair, sums = call(
            functools.partial(join_kernel, g), [own_shape, chunks], [SMEM] + [VMEM] * 3,
            (flags, xa, own, head),
        )
        others = pair_totals(pair, px)
        sums = lax.all_to_all(sums, both, 0, 0, tiled=True)
        history.append(sums)
        outs = call(
            functools.partial(later_step, g, last),
            [ext, ext] + ([flat, flat, sums_shape] if last else [trs_shape] + ends),
            [SMEM] + [VMEM] * (22 + len(others)),
            (flags, xa, xb, ya, yb, sums, own, grho, gsig, rho_e, sig_e, low, high, xlow, xhigh, ylow, yhigh, trs,
             p, q, t, table, ztable, *others),
            core_scratch + ([pltpu.VMEM(*trs_shape)] if last else []), 24,
        )
        if last:
            rho_e, sig_e, grho, gsig, head = outs
        else:
            rho_e, sig_e, trs, grho, gsig, head, own, xa, xb, ya, yb = outs
    history.append(lax.all_to_all(head, both, 0, 0, tiled=True))
    rho, sigma, obj = call(
        functools.partial(closing_kernel, g), [block, block, ((ITERS,), F32)],
        [VMEM] * 9, (*history, grho, gsig, rho_e, sig_e, low, high), outs=[VMEM, VMEM, SMEM],
    )
    return rho, sigma, obj


def solution(mesh):
    placed = (P("gx", "gy", None),) * 5 + (P(), P())
    return jax.shard_map(
        local,
        mesh=mesh,
        in_specs=placed,
        out_specs=(P("gx", "gy", None), P("gx", "gy", None), P()),
        check_vma=False,
    )
```

```python
import functools
import math

import jax
import jax.numpy as jnp
from jax import lax
from jax.experimental import pallas as pl
from jax.experimental.pallas import tpu as pltpu
from jax.sharding import PartitionSpec as P


ITERS = 3
BETA = 1.0
ETA = 0.5
EPSILON = 1e-06

XO = 2
YO = 8
CHUNK = 4
STEP = 16
UNROLL_FIELDS = 4
UNROLL_MAIN = 2
SCALE = 16.0 / BETA
DIAGONALS = ((-1, -1), (-1, 1), (1, -1), (1, 1))
F32 = jnp.float32
BF16 = jnp.bfloat16


class Geo:
    def __init__(self, nx, ny, nz, px, py):
        self.nx, self.ny, self.nz, self.px, self.py = nx, ny, nz, px, py
        self.pl = ny + YO + 1
        self.gp = ny + 1
        self.ext = (nx + 9) * self.pl
        self.xp = nx + 8
        self.cells = float(nx * px * ny * py * nz)
        self.zs = 1.0 / math.sqrt(nz)
        self.xs = 1.0 / math.sqrt(nx * px)
        self.win = (nx + 2) * ny
        self.pairs = px // 2

    def own(self, x):
        return (x + XO) * self.pl + YO


def fold8(v):
    total = v[0:8]
    for i in range(8, v.shape[0], 8):
        total = total + v[i : i + 8]
    return total


def pick_sides(even, first, last, a, b):
    low = jnp.where(even, b, a)
    high = jnp.where(even, a, b)
    return jnp.where(first, 0.0, low), jnp.where(last, 0.0, high)


def put_pair(even, low, high, a_ref, b_ref, at):
    n = low.shape[0]
    a_ref[at : at + n, :] = jnp.where(even, high, low)
    b_ref[at : at + n, :] = jnp.where(even, low, high)


def flags_of(g, flags):
    ix, iy = flags[0], flags[1]
    return ((ix % 2) == 0, ix == 0, ix == g.px - 1), ((iy % 2) == 0, iy == 0, iy == g.py - 1)


def split2(v):
    high = v.astype(BF16)
    low = (v - high.astype(F32)).astype(BF16)
    return jnp.concatenate([high, low], axis=1)


def bounds_of(zones, z, zlow, zhigh):
    low = jnp.full(z.shape, zlow[0], F32)
    high = jnp.full(z.shape, zhigh[0], F32)
    for i in range(1, zones):
        hit = z == i
        low = jnp.where(hit, zlow[i], low)
        high = jnp.where(hit, zhigh[i], high)
    return low, high


def first_kernel(g, flags, rho, sigma, zone, t, own, xa, xb, sig_v, t_v, rims, zrims, sems):
    (even, _, _), _ = flags_of(g, flags)
    step = 8
    small = []
    for k, at in enumerate((0, g.nx - 2)):
        small.append(pltpu.make_async_copy(rho.at[pl.ds(at, 2)], rims.at[k, 0], sems.at[2 * k]))
        small.append(pltpu.make_async_copy(zone.at[pl.ds(at, 2)], zrims.at[k], sems.at[2 * k + 1]))
    big = []
    for c in range(g.nx // step):
        at = pl.ds(c * step, step)
        big.append((
            pltpu.make_async_copy(sigma.at[at], sig_v.at[at], sems.at[4 + 2 * c]),
            pltpu.make_async_copy(t.at[at], t_v.at[at], sems.at[5 + 2 * c]),
        ))
    for a, b in big:
        a.start()
        b.start()
    for copy in small:
        copy.start()
    zero = jnp.zeros((g.ny, g.nz), F32)
    run, total, seen = zero, zero, zero
    for c, (a, b) in enumerate(big):
        a.wait()
        b.wait()
        for k in range(step):
            run = run + sig_v[c * step + k]
            total = total + run
            scaled = t_v[c * step + k] * (1.0 / g.xs)
            t_v[c * step + k] = scaled
            seen = seen + scaled
    own[0 : g.ny, :] = run
    own[g.ny : 2 * g.ny, :] = total - seen
    for copy in small:
        copy.wait()
    at = 0
    for r in range(2):
        put_pair(even, rims[0, 0, r], rims[1, 0, r], xa, xb, at)
        at += g.ny
    for r in range(2):
        put_pair(even, sig_v[r], sig_v[g.nx - 2 + r], xa, xb, at)
        at += g.ny
    for r in range(2):
        put_pair(even, zrims[0, r].astype(F32), zrims[1, r].astype(F32), xa, xb, at)
        at += g.ny
    xa[at : at + g.ny, :] = run
    xa[at + g.ny : at + 2 * g.ny, :] = total - seen


def bounds_kernel(g, zones, zlow, zhigh, zone, low_o, high_o):
    lows = [jnp.full((8, g.nz), zlow[i], F32) for i in range(zones)]
    highs = [jnp.full((8, g.nz), zhigh[i], F32) for i in range(zones)]

    def body(x, carry):
        for k in range(0, g.ny, 8):
            here = pl.ds(k, 8)
            z = zone[x, here, :]
            low, high = lows[0], highs[0]
            for i in range(1, zones):
                hit = z == i
                low = jnp.where(hit, lows[i], low)
                high = jnp.where(hit, highs[i], high)
            low_o[x, here, :] = low
            high_o[x, here, :] = high
        return carry

    lax.fori_loop(0, g.nx, body, 0, unroll=8)


def spread_kernel(g, p, q, p_o, table, ztable):
    nz = g.nz
    row = lax.broadcasted_iota(jnp.int32, (2 * nz, 2 * nz), 0) % nz
    col = lax.broadcasted_iota(jnp.int32, (2 * nz, 2 * nz), 1)
    first = (row <= col).astype(F32)
    second = (nz - jnp.maximum(row, col - nz)).astype(F32) * (SCALE / nz)
    table[...] = jnp.where(col < nz, first, second).astype(BF16)
    r2 = lax.broadcasted_iota(jnp.int32, (2 * nz, nz), 0) % nz
    c2 = lax.broadcasted_iota(jnp.int32, (2 * nz, nz), 1)
    back = (r2 >= c2).astype(F32).astype(BF16)
    ztable[...] = ((r2 == c2 + 1).astype(F32) - (r2 == c2 - 1).astype(F32)).astype(BF16)
    step = 16

    def body(c, carry):
        here = pl.ds(c * step, step)
        values = p[here]
        p_o[here] = values * (1.0 / g.zs)
        out = jnp.dot(split2(values.reshape(step * g.ny, nz)), back, preferred_element_type=F32) * (g.zs * SCALE)
        q[here] = out.reshape(step, g.ny, nz)
        return carry

    lax.fori_loop(0, g.nx // step, body, 0, unroll=True)


def join_kernel(g, flags, xa, own, head, pair, sums):
    (even, _, _), _ = flags_of(g, flags)
    ny = g.ny
    at = 4 * ny
    join_pair(g, even, own, xa, at, pair)
    n = sums.shape[0] // CHUNK
    sums[...] = jnp.zeros(sums.shape, F32)
    sums[pl.ds(0, n, stride=CHUNK), :] = jnp.broadcast_to(head[0:1, :], (n, g.nz))
    for k, (dx, dy) in enumerate(DIAGONALS):
        ok, there = diagonal(g, flags, dx, dy)

        @pl.when(ok)
        def _():
            for f in range(2):
                sums[pl.ds(there * CHUNK + 1 + f, 1), :] = head[8 + 2 * k + f : 9 + 2 * k + f, :]


def diagonal(g, flags, dx, dy):
    ix, iy = flags[0] + dx, flags[1] + dy
    ok = jnp.logical_and(jnp.logical_and(ix >= 0, ix < g.px), jnp.logical_and(iy >= 0, iy < g.py))
    return ok, jnp.where(ok, ix * g.py + iy, 0)


def join_pair(g, even, own, xa, at, pair):
    ny = g.ny
    mine_t, mine_s = own[0:ny, :], own[ny : 2 * ny, :]
    other_t, other_s = xa[at : at + ny, :], xa[at + ny : at + 2 * ny, :]
    pair[0:ny, :] = mine_t + other_t
    pair[ny : 2 * ny, :] = mine_s + other_s + jnp.where(even, mine_t, other_t) * float(g.nx)


def sides_kernel(g, fields, flags, order, *refs):
    blocks, (ya, yb) = refs[:fields], refs[fields:]
    _, (even, _, _) = flags_of(g, flags)
    for f in range(fields):
        for r in range(2):
            low = blocks[f][pl.ds(r, g.nx, stride=g.ny), :].astype(F32)
            high = blocks[f][pl.ds(g.ny - 2 + r, g.nx, stride=g.ny), :].astype(F32)
            put_pair(even, low, high, ya, yb, (f * 2 + r) * g.nx)


def corners_kernel(g, fields, flags, xa, xb, own, ca, cb, pair):
    (even, first, last), (yeven, _, _) = flags_of(g, flags)
    ca[...] = jnp.zeros(ca.shape, F32)
    cb[...] = jnp.zeros(cb.shape, F32)
    for f in range(fields):
        for side, px in ((0, 1), (1, 0)):
            at = (f * 2 + px) * g.ny
            value = pick_sides(even, first, last, xa[at : at + g.ny, :], xb[at : at + g.ny, :])[side]
            put_pair(yeven, value[0:1], value[g.ny - 1 : g.ny], ca, cb, 2 * f + side)
    join_pair(g, even, own, xa, fields * 2 * g.ny, pair)


def halo_slots(g, n, off):
    xs = []
    for r in range(2):
        xs.append((r * g.ny, pl.ds(r * g.pl + YO, g.ny), pl.ds((XO + g.nx + r) * g.pl + YO, g.ny)))
    ys = []
    for r in range(2):
        first = off * g.pl + r
        ys.append((r * n, pl.ds(first + YO - 2, n, stride=g.pl), pl.ds(first + YO + g.ny, n, stride=g.pl)))
    return xs, ys


def halo_values(g, flags, field, xa, xb, ya, yb, yn, off):
    (xeven, xfirst, xlast), (yeven, yfirst, ylast) = flags_of(g, flags)
    xs, ys = halo_slots(g, yn, off)
    for axis, slots, n, a, b, even, first, last in (
        (0, xs, g.ny, xa, xb, xeven, xfirst, xlast),
        (1, ys, yn, ya, yb, yeven, yfirst, ylast),
    ):
        for at, low_rows, high_rows in slots:
            here = pl.ds(field * 2 * n + at, n)
            low, high = pick_sides(even, first, last, a[here, :], b[here, :])
            yield axis, 0, at, low_rows, low
            yield axis, 1, at, high_rows, high


def lane_value(row, lane):
    ids = lax.broadcasted_iota(jnp.int32, row.shape, 1)
    return jnp.sum(jnp.where(ids == lane, row, 0.0), axis=1, keepdims=True)


def sum_row(g, sums):
    n = g.px * g.py
    return jnp.sum(sums[pl.ds(0, n, stride=sums.shape[0] // n), :], axis=0, keepdims=True)


def alphas(g, sums):
    row = sum_row(g, sums)
    return tuple(
        ETA / SCALE * lax.rsqrt(lane_value(row, k) * (1.0 / (g.cells * SCALE * SCALE)) + EPSILON) for k in range(2)
    )


def ray_offsets(g, flags, trs):
    ix = flags[0]
    q = ix // 2
    even = (ix % 2) == 0
    ny = g.ny
    mine, other = trs[0, 0:ny, :], trs[1, 0:ny, :]
    reach = float(g.nx)
    before = jnp.where(even, 0.0, other)
    sums = jnp.zeros_like(mine)
    spread = (mine + other) * (g.pairs - 1 - q).astype(F32)
    for m in range(1, g.pairs):
        p = q ^ m
        total = trs[1 + m, 0:ny, :]
        before = before + jnp.where(p < q, total, 0.0)
        sums = sums + jnp.where(p > q, trs[1 + m, ny : 2 * ny, :], 0.0)
        spread = spread + total * (g.pairs - 1 - jnp.maximum(p, q)).astype(F32)
    near = jnp.where(even, trs[1, ny : 2 * ny, :] + (before + mine) * reach, 0.0)
    return before, near + sums + spread * (2.0 * reach)


def cross(a, b):
    return a[1] * b[2] - a[2] * b[1], a[2] * b[0] - a[0] * b[2], a[0] * b[1] - a[1] * b[0]


def step_core(g, flags, update, rho_e, sig_e, trs, p, q, t, table, ztable, outs, scratch):
    grho, gsig, sums, own, xa, xb, ya, yb = outs
    vxr, vxs, vyr, vys, vzr, vzs, rt_s, az, bz, yu, ym = scratch
    nx, ny, nz, w = g.nx, g.ny, g.nz, g.pl
    (even, _, _), (yeven, _, _) = flags_of(g, flags)
    zero = jnp.zeros((ny, nz), F32)
    zero8 = jnp.zeros((8, nz), F32)
    before, after = ray_offsets(g, flags, trs)
    step = STEP
    rows = step * ny
    ext = ((rho_e, az), (sig_e, bz))

    def span(start, size, tile=8):
        return pl.ds(start if isinstance(start, int) or tile == 1 else pl.multiple_of(start, tile), size)

    def plane(x):
        return span((x + 1) * ny, ny)

    def zdiff(v):
        return jnp.dot(split2(v), ztable[...], preferred_element_type=F32)

    def slopes(ref, z, x):
        at = g.own(x)
        sx = ref[pl.ds(at + w, ny), :] - ref[pl.ds(at - w, ny), :]
        sy = ref[pl.ds(at + 1, ny), :] - ref[pl.ds(at - 1, ny), :]
        return sx, sy, z[plane(x), :]

    def cross_plane(x, acc, inside):
        a = slopes(*ext[0], x)
        b = slopes(*ext[1], x)
        c = cross(a, b)
        vxr[plane(x), :] = b[1] * c[2] - b[2] * c[1]
        vxs[plane(x), :] = c[1] * a[2] - c[2] * a[1]
        if not inside:
            return acc
        at = pl.ds(g.own(x), ny)
        vyr[at, :] = b[2] * c[0] - b[0] * c[2]
        vys[at, :] = c[2] * a[0] - c[0] * a[2]
        vzr[plane(x), :] = b[0] * c[1] - b[1] * c[0]
        vzs[plane(x), :] = c[0] * a[1] - c[1] * a[0]
        return acc + fold8(c[0] * c[0] + c[1] * c[1] + c[2] * c[2])

    def fields_chunk(c, carry):
        run, acc = carry
        values = ([], [])
        for k in range(step):
            x = c * step + k
            at = pl.ds(g.own(x), ny)
            rho, sig = update(x, at)
            rho_e[at, :] = rho
            sig_e[at, :] = sig
            values[0].append(rho)
            values[1].append(sig)
            run = run + sig
            miss = run - t[x]
            rt_s[span(x * ny, ny), :] = miss
            acc = acc + fold8(miss * miss)
        at = span(c * rows + ny, rows)
        pieces = split2(jnp.concatenate(values[0] + values[1], axis=0))
        y = jnp.dot(pieces[:rows], table[...], preferred_element_type=F32)
        yu[at, :] = y[:, :nz]
        ym[at, :] = y[:, nz:]
        z = jnp.dot(pieces, ztable[...], preferred_element_type=F32)
        az[at, :] = z[:rows]
        bz[at, :] = z[rows:]
        return run, acc

    chunks = nx // step
    _, acc_t = lax.fori_loop(0, chunks, fields_chunk, (before, zero8), unroll=UNROLL_FIELDS)

    lines = (-1, ny)
    line = lambda ref, x, y: ref[pl.ds((XO + x) * w + YO + y, nx, stride=w), :]
    flat = lambda ref, x: ref[g.own(x) : g.own(x) + ny, :]
    pieces = [line(ref, 0, y) for ref, _ in ext for y in lines] + [flat(ref, x) for ref, _ in ext for x in (-1, nx)]
    deep = zdiff(jnp.concatenate(pieces, axis=0))
    for k, y in enumerate(lines):
        fields = []
        for f, (ref, _) in enumerate(ext):
            at = (2 * f + k) * nx
            fields.append((line(ref, 1, y) - line(ref, -1, y), line(ref, 0, y + 1) - line(ref, 0, y - 1), deep[at : at + nx]))
        a, b = fields
        c = cross(a, b)
        spot = pl.ds(XO * w + YO + y, nx, stride=w)
        vyr[spot, :] = b[2] * c[0] - b[0] * c[2]
        vys[spot, :] = c[2] * a[0] - c[0] * a[2]
    base = 4 * nx
    for k, x in enumerate((-1, nx)):
        for f, (_, z) in enumerate(ext):
            at = base + (2 * f + k) * ny
            z[plane(x), :] = deep[at : at + ny]

    def gradient_plane(x, carry):
        back, sum_t, sum_r, nr, ns, acc = carry
        at = g.own(x)
        here = plane(x)
        flat_at = span(x * ny, ny)

        def term(vx, vy, vz):
            along_x = vx[plane(x - 1), :] - vx[plane(x + 1), :]
            along_y = vy[pl.ds(at - 1, ny), :] - vy[pl.ds(at + 1, ny), :]
            return along_x + along_y - vz[here, :]

        back = back + rt_s[flat_at, :]
        miss = yu[here, :] - p[x]
        gr = ym[here, :] - q[x] + term(vxr, vyr, vzr)
        gs = back * (SCALE * g.xs * g.xs) + term(vxs, vys, vzs)
        out = pl.ds(x * g.gp, ny)
        grho[out, :] = gr
        gsig[out, :] = gs
        sum_t = sum_t + gs
        return back, sum_t, sum_r + sum_t, nr + fold8(gr * gr), ns + fold8(gs * gs), acc + fold8(miss * miss)

    def crosses(c, acc):
        for k in range(step):
            acc = cross_plane(c * step + step - 1 - k, acc, True)
        return acc

    def adjoint(c):
        at = span(c * rows + ny, rows)
        z = zdiff(jnp.concatenate([vzr[at, :], vzs[at, :]], axis=0))
        vzr[at, :] = z[:rows]
        vzs[at, :] = z[rows:]

    def gradients(c, carry):
        for k in range(step):
            carry = gradient_plane(c * step + step - 1 - k, carry)
        return carry

    carry = (after, zero, zero, zero8, zero8, zero8)
    cross_plane(-1, None, False)
    cross_plane(nx, None, False)
    acc_c = crosses(chunks - 1, zero8)
    acc_c = crosses(chunks - 2, acc_c)
    adjoint(chunks - 1)

    def main(i, carry):
        c = chunks - 3 - i
        acc = crosses(c, carry[0])
        adjoint(c + 1)
        return acc, gradients(c + 2, carry[1])

    acc_c, carry = lax.fori_loop(0, chunks - 2, main, (acc_c, carry), unroll=UNROLL_MAIN)
    adjoint(0)
    carry = gradients(1, carry)
    _, sum_t, sum_r, nr, ns, acc_p = gradients(0, carry)

    total = lambda v: jnp.sum(jnp.sum(v, axis=0, keepdims=True), axis=1, keepdims=True)
    spread = sums.shape[0] if own is None else 8
    lane = lax.broadcasted_iota(jnp.int32, (spread, nz), 1)
    obj = acc_t * (g.xs * g.xs) + acc_p * (g.zs * g.zs) + acc_c * (BETA / 16.0)
    sums[0:spread, :] = jnp.where(lane == 0, total(nr), jnp.where(lane == 1, total(ns), jnp.where(lane == 2, total(obj), 0.0)))
    if own is not None:
        rest = sum_t * (nx + 1.0) - sum_r
        pos = 0
        for block in (grho, gsig):
            for r in range(2):
                put_pair(even, block[pl.ds(r * g.gp, ny), :], block[pl.ds((nx - 2 + r) * g.gp, ny), :], xa, xb, pos)
                pos += ny
        for ref, at in ((own, 0), (xa, pos)):
            ref[at : at + ny, :] = sum_t
            ref[at + ny : at + 2 * ny, :] = rest
        for f, block in enumerate((grho, gsig)):
            for r in range(2):
                rows_low = block[pl.ds(r, nx, stride=g.gp), :]
                rows_high = block[pl.ds(ny - 2 + r, nx, stride=g.gp), :]
                put_pair(yeven, rows_low, rows_high, ya, yb, (f * 2 + r) * nx)
            for k, (dx, dy) in enumerate(DIAGONALS):
                cell = (0 if dx < 0 else nx - 1) * g.gp + (0 if dy < 0 else ny - 1)
                sums[8 + 2 * k + f : 9 + 2 * k + f, :] = block[cell : cell + 1, :]


def opening_step(g, zones, flags, zlow, zhigh, xa, xb, ya, yb, ca, cb, own, rho, sig, p, q, t, table, ztable, *refs):
    others, rest = refs[: g.pairs - 1], refs[g.pairs - 1 :]
    rho_e, sig_e, trs, xlow, xhigh, ylow, yhigh = rest[:7]
    ny = g.ny
    _, (yeven, yfirst, ylast) = flags_of(g, flags)
    for f, ext in ((0, rho_e), (1, sig_e)):
        for axis, side, at, spot, value in halo_values(g, flags, f, xa, xb, ya, yb, g.nx, XO):
            ext[spot, :] = value
    for axis, side, at, spot, value in halo_values(g, flags, 2, xa, xb, ya, yb, g.nx, XO):
        low, high = bounds_of(zones, value, zlow, zhigh)
        lows, highs = ((xlow, xhigh), (ylow, yhigh))[axis]
        if axis == 1:
            at = at // g.nx * g.xp + XO
        lows[side, pl.ds(at, value.shape[0]), :] = low
        highs[side, pl.ds(at, value.shape[0]), :] = high
    cells = pick_sides(yeven, yfirst, ylast, ca[...], cb[...])
    limits = [bounds_of(zones, values, zlow, zhigh) for values in cells]
    for side, row in ((0, YO - 1), (1, YO + ny)):
        for k, plane in enumerate((XO - 1, XO + g.nx)):
            at = plane * g.pl + row
            rho_e[at : at + 1, :] = cells[side][k : k + 1]
            sig_e[at : at + 1, :] = cells[side][2 + k : 3 + k]
            at = (1 - side) * g.xp + plane
            ylow[side, at : at + 1, :] = limits[side][0][4 + k : 5 + k]
            yhigh[side, at : at + 1, :] = limits[side][1][4 + k : 5 + k]
    pos = 6 * ny
    trs[0] = own[...]
    trs[1] = xa[pos : pos + 2 * ny, :]
    for m, other in enumerate(others):
        trs[2 + m] = other[...]
    step_core(g, flags, lambda x, at: (rho[x], sig[x]), rho_e, sig_e, trs, p, q, t, table, ztable, rest[7:15], rest[15:])


def later_step(g, last, flags, xa, xb, ya, yb, sums_i, own_i, grho_i, gsig_i, rho_i, sig_i, low, high,
               xlow, xhigh, ylow, yhigh, trs_i, p, q, t, table, ztable, *refs):
    others, rest = refs[: g.pairs - 1], refs[g.pairs - 1 :]
    rest = (*rest[:2], rest[-1], *rest[2:-1]) if last else rest
    rho_e, sig_e, trs = rest[:3]
    ny = g.ny
    ar, asig = alphas(g, sums_i)
    clip = lambda v, lows, highs: jnp.minimum(jnp.maximum(v, lows), highs)
    for axis, side, at, spot, value in halo_values(g, flags, 0, xa, xb, ya, yb, g.nx, XO):
        lows, highs = ((xlow, xhigh), (ylow, yhigh))[axis]
        if axis == 1:
            at = at // g.nx * g.xp + XO
        here = pl.ds(at, value.shape[0])
        rho_e[spot, :] = clip(rho_i[spot, :] - ar * value, lows[side, here, :], highs[side, here, :])
    for axis, side, at, spot, value in halo_values(g, flags, 1, xa, xb, ya, yb, g.nx, XO):
        sig_e[spot, :] = sig_i[spot, :] - asig * value
    for dx, dy in DIAGONALS:
        ok, there = diagonal(g, flags, dx, dy)
        plane = XO - 1 if dx < 0 else XO + g.nx
        side = 0 if dy < 0 else 1
        here = pl.ds((1 - side) * g.xp + plane, 1)
        spot = pl.ds(plane * g.pl + (YO - 1 if dy < 0 else YO + ny), 1)
        value = jnp.where(ok, sums_i[pl.ds(there * CHUNK + 1, 1), :], 0.0)
        rho_e[spot, :] = clip(rho_i[spot, :] - ar * value, ylow[side, here, :], yhigh[side, here, :])
        value = jnp.where(ok, sums_i[pl.ds(there * CHUNK + 2, 1), :], 0.0)
        sig_e[spot, :] = sig_i[spot, :] - asig * value
    pos = 4 * ny
    trs[0] = trs_i[0] - asig * own_i[...]
    trs[1] = trs_i[1] - asig * xa[pos : pos + 2 * ny, :]
    for m, other in enumerate(others):
        trs[2 + m] = trs_i[2 + m] - asig * other[...]

    def update(x, at):
        here = pl.ds(x * g.gp, ny)
        moved = rho_i[at, :] - ar * grho_i[here, :]
        return clip(moved, low[x], high[x]), sig_i[at, :] - asig * gsig_i[here, :]

    if last:
        outs, scratch = (*rest[3:6], None, None, None, None, None), rest[6:]
    else:
        outs, scratch = rest[3:11], rest[11:]
    step_core(g, flags, update, rho_e, sig_e, trs, p, q, t, table, ztable, outs, scratch)


def closing_kernel(g, sums0, sums1, sums2, grho, gsig, rho_e, sig_e, low, high, rho_o, sig_o, obj):
    ar, asig = alphas(g, sums2)

    def body(x, carry):
        at = pl.ds(g.own(x), g.ny)
        here = pl.ds(x * g.gp, g.ny)
        rho_o[x] = jnp.minimum(jnp.maximum(rho_e[at, :] - ar * grho[here, :], low[x]), high[x])
        sig_o[x] = sig_e[at, :] - asig * gsig[here, :]
        return carry

    lax.fori_loop(0, g.nx, body, 0, unroll=8)
    for k, sums in enumerate((sums0, sums1, sums2)):
        row = sum_row(g, sums)
        lane = lax.broadcasted_iota(jnp.int32, row.shape, 1)
        obj[k] = jnp.sum(jnp.where(lane == 2, row, 0.0)) * (0.5 / g.cells)


def pairs_of(size):
    a = [(i, i ^ 1) for i in range(size)]
    b = [(i, i if i in (0, size - 1) else ((i + 1) ^ 1) - 1) for i in range(size)]
    return a, b


def exchange(axis, a, b):
    pa, pb = pairs_of(lax.axis_size(axis))
    a = lax.ppermute(a, axis, pa)
    b = lax.ppermute(b, axis, pb)
    return a, b


def pair_totals(pair, size):
    out = []
    for m in range(1, size // 2):
        out.append(lax.ppermute(pair, "gx", [(i, i ^ (2 * m)) for i in range(size)]))
    return out


SMEM = pl.BlockSpec(memory_space=pltpu.SMEM)
VMEM = pl.BlockSpec(memory_space=pltpu.VMEM)
HBM = pl.BlockSpec(memory_space=pltpu.HBM)


def call(body, shapes, specs, args, scratch=(), limit=12, outs=None):
    return pl.pallas_call(
        body,
        out_shape=[jax.ShapeDtypeStruct(s, d) for s, d in shapes],
        in_specs=specs,
        out_specs=outs or [VMEM] * len(shapes),
        scratch_shapes=list(scratch),
        compiler_params=pltpu.CompilerParams(vmem_limit_bytes=limit * 1024 * 1024),
    )(*args)


def local(density, slowness, pressure_obs, time_obs, zone_map, zone_low, zone_high):
    nx, ny, nz = density.shape
    px, py = lax.axis_size("gx"), lax.axis_size("gy")
    g = Geo(nx, ny, nz, px, py)
    zones = zone_low.shape[0]
    both = ("gx", "gy")
    flags = jnp.stack([lax.axis_index("gx"), lax.axis_index("gy")]).astype(jnp.int32)

    ext = ((g.ext, nz), F32)
    own_shape = ((2 * ny, nz), F32)
    trs_shape = ((g.pairs + 1, 2 * ny, nz), F32)
    sums_shape = ((px * py, nz), F32)
    block = ((nx, ny, nz), F32)
    flat = ((nx * g.gp, nz), F32)
    xa_shape = lambda f: (((f + 1) * 2 * ny, nz), F32)
    xb_shape = lambda f: ((f * 2 * ny, nz), F32)
    ymsg = lambda f: ((f * 2 * nx, nz), F32)
    xbound = ((2, 2 * ny, nz), F32)
    ybound = ((2, 2 * g.xp, nz), F32)
    win = pltpu.VMEM((g.win, nz), F32)
    ext_v = pltpu.VMEM((g.ext, nz), F32)
    core_scratch = [win] * 2 + [ext_v] * 2 + [win] * 2 + [pltpu.VMEM((nx * ny, nz), F32)] + [win] * 4

    own, xa, xb, sig, t = call(
        functools.partial(first_kernel, g), [own_shape, xa_shape(3), xb_shape(3), block, block],
        [SMEM] + [HBM] * 4, (flags, *(pltpu.with_memory_space_constraint(v, pltpu.HBM) for v in (density, slowness, zone_map, time_obs))),
        [pltpu.VMEM((2, 1, 2, ny, nz), F32), pltpu.VMEM((2, 2, ny, nz), jnp.int32),
         pltpu.SemaphoreType.DMA((4 + nx // 4,))],
    )
    xa, xb = exchange("gx", xa, xb)
    low, high = call(
        functools.partial(bounds_kernel, g, zones), [block] * 2,
        [SMEM, SMEM, VMEM], (zone_low, zone_high, zone_map),
    )
    q, p, table, ztable = call(
        functools.partial(spread_kernel, g),
        [block] * 2 + [((2 * nz, 2 * nz), BF16), ((2 * nz, nz), BF16)], [VMEM], (pressure_obs,),
    )
    as_rows = lambda v: v.reshape(nx * ny, nz)
    ya, yb = call(
        functools.partial(sides_kernel, g, 3), [ymsg(3)] * 2,
        [SMEM] + [VMEM] * 4, (flags, own, as_rows(density), as_rows(sig), as_rows(zone_map)),
    )
    ya, yb = exchange("gy", ya, yb)
    ca, cb, pair = call(
        functools.partial(corners_kernel, g, 3), [((8, nz), F32)] * 2 + [own_shape],
        [SMEM] + [VMEM] * 3, (flags, xa, xb, own),
    )
    ca, cb = exchange("gy", ca, cb)
    others = pair_totals(pair, px)
    ends = [flat, flat, ((16, nz), F32), own_shape, xa_shape(2), xb_shape(2), ymsg(2), ymsg(2)]
    chunks = ((px * py * CHUNK, nz), F32)
    outs = call(
        functools.partial(opening_step, g, zones),
        [ext, ext, trs_shape, xbound, xbound, ybound, ybound] + ends,
        [SMEM] * 3 + [VMEM] * (14 + len(others)),
        (flags, zone_low, zone_high, xa, xb, ya, yb, ca, cb, own, density, sig, p, q, t, table, ztable, *others),
        core_scratch, 24,
    )
    rho_e, sig_e, trs, xlow, xhigh, ylow, yhigh, grho, gsig, head, own, xa, xb, ya, yb = outs
    history = []
    for iteration in range(1, ITERS):
        last = iteration == ITERS - 1
        xa, xb = exchange("gx", xa, xb)
        ya, yb = exchange("gy", ya, yb)
        pair, sums = call(
            functools.partial(join_kernel, g), [own_shape, chunks], [SMEM] + [VMEM] * 3,
            (flags, xa, own, head),
        )
        others = pair_totals(pair, px)
        sums = lax.all_to_all(sums, both, 0, 0, tiled=True)
        history.append(sums)
        outs = call(
            functools.partial(later_step, g, last),
            [ext, ext] + ([flat, flat, sums_shape] if last else [trs_shape] + ends),
            [SMEM] + [VMEM] * (22 + len(others)),
            (flags, xa, xb, ya, yb, sums, own, grho, gsig, rho_e, sig_e, low, high, xlow, xhigh, ylow, yhigh, trs,
             p, q, t, table, ztable, *others),
            core_scratch + ([pltpu.VMEM(*trs_shape)] if last else []), 24,
        )
        if last:
            rho_e, sig_e, grho, gsig, head = outs
        else:
            rho_e, sig_e, trs, grho, gsig, head, own, xa, xb, ya, yb = outs
    history.append(lax.all_to_all(head, both, 0, 0, tiled=True))
    rho, sigma, obj = call(
        functools.partial(closing_kernel, g), [block, block, ((ITERS,), F32)],
        [VMEM] * 9, (*history, grho, gsig, rho_e, sig_e, low, high), outs=[VMEM, VMEM, SMEM],
    )
    return rho, sigma, obj


def solution(mesh):
    placed = (P("gx", "gy", None),) * 5 + (P(), P())
    return jax.shard_map(
        local,
        mesh=mesh,
        in_specs=placed,
        out_specs=(P("gx", "gy", None), P("gx", "gy", None), P()),
        check_vma=False,
    )
```
